16 devices in a mesh: dp: 2 (over y, z), tp: 8 (over x, core).
Axes of the slice: x: 4, y: 2, z: 1, core: 2. Of those that a mesh axis runs over, the one named last changes fastest.
The devices are a block of a 4x4x8 slice.
Arguments:
- x_rows: bfloat16 [16384, 2304], P(('dp', 'tp')), parts along dimension 0
- norm_gain: float32 [2304], replicated
- w_q: bfloat16 [2304, 8, 256], P(None, 'tp')
- w_k: bfloat16 [2304, 1024], P(None, 'tp')
- w_v: bfloat16 [2304, 1024], P(None, 'tp')
Outputs:
- output 1: bfloat16 [16384, 8, 256], P('dp', 'tp'), parts along dimension 0
- output 2: bfloat16 [16384, 8, 256], P('dp', 'tp'), parts along dimension 0
- output 3: bfloat16 [16384, 8, 256], P('dp', 'tp'), parts along dimension 0
There are 2 independent parts. The reference program is written for one: setup_inputs(seed, part) draws one part's arguments, and reference() takes and returns one part's arrays. A program takes and returns all parts, laid end to end along the dimension named above; an argument that names none is the same for every part.
All inputs are finite; a program needn't handle non-finite values.
Results may differ from the reference program's by a relative error of at most 0.001.
Values are sent between devices in bfloat16 or wider.
A program may use at most 768 MiB of HBM per device.

```python
import jax
import jax.numpy as jnp
from jax import lax

TOKENS = 8192
D_MODEL = 2304
Q_HEADS = 8
KV_COUNT = 4
HEAD_DIM = 256
GROUP_SIZE = 8
EPSILON = 1e-6


def setup_inputs(seed: int = 0, part: int = 0) -> dict:
    key = jax.random.key(seed)
    shared_key, rows_key = jax.random.split(key)
    part_key = jax.random.fold_in(rows_key, part)
    x_rows = jax.random.normal(part_key, (TOKENS, D_MODEL), jnp.float32).astype(jnp.bfloat16)
    gain_key, q_key, k_key, v_key = jax.random.split(shared_key, 4)
    norm_gain = jax.random.uniform(gain_key, (D_MODEL,), jnp.float32, 0.4, 1.6)
    weight_scale = D_MODEL ** -0.5
    w_q = (jax.random.normal(q_key, (D_MODEL, Q_HEADS, HEAD_DIM), jnp.float32) * weight_scale).astype(jnp.bfloat16)
    w_k = (jax.random.normal(k_key, (D_MODEL, KV_COUNT * HEAD_DIM), jnp.float32) * weight_scale).astype(jnp.bfloat16)
    w_v = (jax.random.normal(v_key, (D_MODEL, KV_COUNT * HEAD_DIM), jnp.float32) * weight_scale).astype(jnp.bfloat16)
    return {"x_rows": x_rows, "norm_gain": norm_gain, "w_q": w_q, "w_k": w_k, "w_v": w_v}


def reference(x_rows, norm_gain, w_q, w_k, w_v):
    x_wide = x_rows.astype(jnp.float32)
    mean_sq = jnp.mean(x_wide * x_wide, axis=-1, keepdims=True)
    normed = (x_wide * lax.rsqrt(mean_sq + EPSILON) * norm_gain).astype(jnp.bfloat16)
    q_flat = jnp.dot(normed, w_q.reshape(D_MODEL, Q_HEADS * HEAD_DIM), preferred_element_type=jnp.float32)
    q_out = q_flat.astype(jnp.bfloat16).reshape(TOKENS, Q_HEADS, HEAD_DIM)
    head_share = GROUP_SIZE // KV_COUNT
    k_flat = jnp.dot(normed, w_k, preferred_element_type=jnp.float32).astype(jnp.bfloat16)
    v_flat = jnp.dot(normed, w_v, preferred_element_type=jnp.float32).astype(jnp.bfloat16)
    k_out = jnp.repeat(k_flat.reshape(TOKENS, KV_COUNT, HEAD_DIM), head_share, axis=1)
    v_out = jnp.repeat(v_flat.reshape(TOKENS, KV_COUNT, HEAD_DIM), head_share, axis=1)
    return (q_out, k_out, v_out)
```

```python
import functools

import jax
import jax.numpy as jnp
from jax import lax
from jax.experimental import pallas as pl
from jax.experimental.pallas import tpu as pltpu
from jax.sharding import PartitionSpec as P

EPSILON = 1e-6
LANES = 128
NORM_ROWS = 32
CHUNK = 128
OWN_ROWS = 256
MESH = pl.DeviceIdType.MESH


def exchange(chips, x, gain, wq, wk, wv, oq, okv, n, w, slq, srq, srkv, x_sem, wl_sem, wl_s, wl_r, wx_s, wx_r, wg_s, wg_r, wd_s, wd_r, n_s, n_r,
             oq_s, oq_r, okv_s, okv_r, rq_s, rq_r, rkv_s, rkv_r, lq_s, lq_r, lkv_s, lkv_r, fk_s, fk_r):
    rows, depth = x.shape
    chunks = rows // CHUNK
    group = lax.axis_index("dp")
    device = lax.axis_index("tp")
    half = lax.rem(group, 2)
    core = lax.rem(device, 2)
    chip = lax.div(device, 2)
    token_chip = chip + 1 - 2 * lax.rem(chip, 2)
    weight_chip = chips - 1 - chip
    far_chip = weight_chip + 1 - 2 * lax.rem(weight_chip, 2)
    other_core = 1 - core
    partner = {"tp": 2 * chip + other_core}
    token_peer = {"tp": 2 * token_chip + core}
    weight_peer = {"tp": 2 * weight_chip + core}
    group_peer = {"dp": group + 1 - 2 * half}

    def weight_core(c):
        return {"tp": 2 * weight_chip + c}

    def remote(src, dst, send, recv, to):
        return pltpu.make_async_remote_copy(src_ref=src, dst_ref=dst, send_sem=send, recv_sem=recv, device_id=to, device_id_type=MESH)

    def block(c, on_chip):
        return pl.multiple_of((2 * on_chip + c) * rows, rows)

    def chunk_of(j):
        return pl.ds(pl.multiple_of(j * CHUNK, CHUNK), CHUNK)

    def load_x(j):
        return pltpu.make_async_copy(x.at[chunk_of(j)], n.at[0, chunk_of(j)], x_sem.at[j])

    for j in range(chunks):
        load_x(j).start()

    q_half = [wq.at[:, pl.ds(h * LANES, LANES)] for h in range(2)]
    kv = [wk, wv]

    barrier = pltpu.get_barrier_semaphore()
    for peer in (partner, token_peer, weight_peer, weight_core(other_core), group_peer):
        pl.semaphore_signal(barrier, inc=1, device_id=peer, device_id_type=MESH)
    pl.semaphore_wait(barrier, 5)

    w_first = w.at[1, half, core, :, pl.ds(0, LANES)]
    w_second = w.at[1, half, core, :, pl.ds(LANES, LANES)]
    remote(wq.at[:, pl.ds(pl.multiple_of(half * LANES, LANES), LANES)], w_first, wx_s, wx_r.at[0], weight_peer).start()
    for h in range(2):
        @pl.when(half == h)
        def _():
            remote(kv[h], w_second, wx_s, wx_r.at[1], weight_peer).start()
    for h in range(2):
        for part, src in enumerate((q_half[h], kv[h])):
            dst = w.at[0, h, core, :, pl.ds(part * LANES, LANES)]
            remote(src, dst, wl_s, wl_r, partner).start()
            pltpu.make_async_copy(src, dst, wl_sem).start()

    def send_n(j):
        return remote(n.at[0, chunk_of(j)], n.at[1, chunk_of(j)], n_s, n_r.at[j], token_peer)

    @pl.loop(0, chunks)
    def _(j):
        load_x(j).wait()

        @pl.loop(0, CHUNK // NORM_ROWS)
        def _(i):
            at = pl.ds(pl.multiple_of(j * CHUNK + i * NORM_ROWS, NORM_ROWS), NORM_ROWS)
            wide = n[0, at, :].astype(jnp.float32)
            mean_sq = jnp.mean(wide * wide, axis=-1, keepdims=True)
            n[0, at, :] = (wide * lax.rsqrt(mean_sq + EPSILON) * gain[...]).astype(jnp.bfloat16)

        send_n(j).start()

    def product(blk, at, side, h, c):
        return jnp.dot(n[blk, at, :], w[side, h, c], preferred_element_type=jnp.float32).astype(jnp.bfloat16)

    def local_products(blk, base, start, size):
        at = pl.ds(start, size)
        out = pl.ds(pl.multiple_of(base + start, size), size)

        @pl.loop(0, 2)
        def _(h):
            for b in range(2):
                c = lax.rem(core + b, 2)
                both = product(blk, at, 0, h, c)
                if b == 0:
                    oq[h, out, :] = both[:, :LANES]
                else:
                    slq[blk, h, at, :] = both[:, :LANES]
                okv[h, c, out, :] = both[:, LANES:]
        remote(slq.at[blk, :, at], oq.at[:, out], lq_s.at[blk], lq_r.at[blk], partner).start()
        remote(okv.at[:, :, out], okv.at[:, :, out], lkv_s.at[blk], lkv_r.at[blk], partner).start()

    own = block(core, chip)
    near = block(core, token_chip)

    own_w = w.at[0, :, core]
    pltpu.make_async_copy(own_w, own_w, wl_sem).wait()
    other_w = w.at[0, :, other_core]
    remote(other_w, other_w, wl_s, wl_r, partner).wait_recv()

    @pl.loop(0, rows // OWN_ROWS)
    def _(i):
        local_products(0, own, pl.multiple_of(i * OWN_ROWS, OWN_ROWS), OWN_ROWS)

    for part, piece in enumerate((w_first, w_second)):
        remote(piece, piece, wx_s, wx_r.at[part], weight_peer).wait_recv()
        remote(piece, piece, wg_s, wg_r, group_peer).start()
        remote(piece, piece, wd_s.at[0], wd_r.at[0], partner).start()

    def own_products(h, c):
        @pl.loop(0, rows // OWN_ROWS)
        def _(i):
            at = pl.ds(pl.multiple_of(i * OWN_ROWS, OWN_ROWS), OWN_ROWS)
            both = product(0, at, 1, h, c)
            srq[0, c, h, at, :] = both[:, :LANES]
            srkv[0, h, c, at, :] = both[:, LANES:]
        out = pl.ds(own, rows)
        remote(srq.at[0, c, h], oq.at[h, out], oq_s, oq_r.at[core], weight_core(c)).start()
        remote(srkv.at[0, h, c], okv.at[h, c, out], okv_s, okv_r, weight_peer).start()

    other_half = 1 - half
    own_products(half, core)
    from_partner = w.at[1, half, other_core]
    remote(from_partner, from_partner, wd_s.at[0], wd_r.at[0], partner).wait_recv()
    own_products(half, other_core)
    from_group = w.at[1, other_half, core]
    remote(from_group, from_group, wg_s, wg_r, group_peer).wait_recv()
    remote(from_group, from_group, wd_s.at[1], wd_r.at[1], partner).start()
    own_products(other_half, core)
    from_both = w.at[1, other_half, other_core]
    remote(from_both, from_both, wd_s.at[1], wd_r.at[1], partner).wait_recv()
    own_products(other_half, other_core)

    @pl.loop(0, chunks)
    def _(j):
        send_n(j).wait_recv()
        start = pl.multiple_of(j * CHUNK, CHUNK)
        at = pl.ds(start, CHUNK)
        out = pl.ds(pl.multiple_of(near + start, CHUNK), CHUNK)

        @pl.loop(0, 2)
        def _(h):
            for c in range(2):
                both = product(1, at, 1, h, c)
                srq[1, c, h, at, :] = both[:, :LANES]
                srkv[1, h, c, at, :] = both[:, LANES:]
        remote(srkv.at[1, :, :, at], okv.at[:, :, out], rkv_s, rkv_r.at[j], weight_peer).start()
        for c in range(2):
            remote(srq.at[1, c, :, at], oq.at[:, out], rq_s, rq_r.at[core], weight_core(c)).start()
        local_products(1, near, start, CHUNK)

    beside = pl.ds(block(core, weight_chip), rows)
    arrived = okv.at[:, :, beside]
    remote(arrived, arrived, okv_s, okv_r, weight_peer).wait_recv()
    remote(arrived, arrived, fk_s.at[0], fk_r.at[0], partner).start()
    far = block(core, far_chip)

    @pl.loop(0, chunks)
    def _(j):
        piece = okv.at[:, :, pl.ds(pl.multiple_of(far + j * CHUNK, CHUNK), CHUNK)]
        remote(piece, piece, rkv_s, rkv_r.at[j], weight_peer).wait_recv()
        remote(piece, piece, fk_s.at[1], fk_r.at[1], partner).start()

    def all_q(c, on_chip):
        return oq.at[:, pl.ds(block(c, on_chip), rows)]

    def all_kv(c, on_chip):
        return okv.at[:, :, pl.ds(block(c, on_chip), rows)]

    for c in range(2):
        remote(all_q(c, weight_chip), all_q(c, weight_chip), oq_s, oq_r.at[c], weight_peer).wait_recv()
        remote(all_q(c, far_chip), all_q(c, far_chip), rq_s, rq_r.at[c], weight_peer).wait_recv()
    for i, on_chip in enumerate((chip, token_chip)):
        remote(all_q(other_core, on_chip), all_q(other_core, on_chip), lq_s.at[i], lq_r.at[i], partner).wait_recv()
        remote(all_kv(other_core, on_chip), all_kv(other_core, on_chip), lkv_s.at[i], lkv_r.at[i], partner).wait_recv()
    for i, on_chip in enumerate((weight_chip, far_chip)):
        remote(all_kv(other_core, on_chip), all_kv(other_core, on_chip), fk_s.at[i], fk_r.at[i], partner).wait_recv()

    def sent(ref, sem):
        remote(ref, ref, sem, n_r.at[0], partner).wait_send()

    sent(own_w, wl_s)
    sent(w.at[1, 0, 0], wx_s)
    sent(w.at[1, 0, 0], wg_s)
    for i in range(2):
        sent(w.at[1, 0, 0], wd_s.at[i])
        sent(slq.at[i], lq_s.at[i])
        sent(srkv.at[0], lkv_s.at[i])
        sent(srkv.at[0], fk_s.at[i])
    sent(n.at[0], n_s)
    sent(srq.at[0], oq_s)
    sent(srkv.at[0], okv_s)
    sent(srq.at[1], rq_s)
    sent(srkv.at[1], rkv_s)


def place(oq, okv, q, k, v, sems):
    copies = []
    for h in range(2):
        cols = pl.ds(h * LANES, LANES)
        copies.append(pltpu.make_async_copy(oq.at[h], q.at[:, cols], sems.at[h]))
        copies.append(pltpu.make_async_copy(okv.at[0, h], k.at[:, cols], sems.at[2 + h]))
        copies.append(pltpu.make_async_copy(okv.at[1, h], v.at[:, cols], sems.at[4 + h]))
    for copy in copies:
        copy.start()
    for copy in copies:
        copy.wait()


def solution(mesh):
    group_size = mesh.shape["tp"]
    chips = group_size // 2

    def local_step(x_rows, norm_gain, w_q, w_k, w_v):
        rows, depth = x_rows.shape
        head = w_q.shape[2]
        tokens = rows * group_size
        dtype = x_rows.dtype
        any_space = pl.BlockSpec(memory_space=pl.ANY)
        vmem = pl.BlockSpec(memory_space=pltpu.VMEM)
        dma = pltpu.SemaphoreType.DMA
        chunks = rows // CHUNK
        oq, okv = pl.pallas_call(
            functools.partial(exchange, chips),
            out_shape=(pltpu.VMEM((2, tokens, LANES), dtype), pltpu.VMEM((2, 2, tokens, LANES), dtype)),
            in_specs=[any_space, vmem, any_space, any_space, any_space],
            out_specs=(vmem, vmem),
            scratch_shapes=[
                pltpu.VMEM((2, rows, depth), dtype),
                pltpu.VMEM((2, 2, 2, depth, 2 * LANES), dtype),
                pltpu.VMEM((2, 2, rows, LANES), dtype),
                pltpu.VMEM((2, 2, 2, rows, LANES), dtype),
                pltpu.VMEM((2, 2, 2, rows, LANES), dtype),
                dma((chunks,)),
                dma, dma, dma,
                dma, dma((2,)),
                dma, dma,
                dma((2,)), dma((2,)),
                dma, dma((chunks,)),
                dma, dma((2,)), dma, dma,
                dma, dma((2,)), dma, dma((chunks,)),
                dma((2,)), dma((2,)), dma((2,)), dma((2,)),
                dma((2,)), dma((2,)),
            ],
            compiler_params=pltpu.CompilerParams(collective_id=0, has_side_effects=True, vmem_limit_bytes=46 * 1024 * 1024),
        )(x_rows, norm_gain.reshape(1, depth), w_q.reshape(depth, head), w_k, w_v)
        out = jax.ShapeDtypeStruct((tokens, head), dtype)
        q, k, v = pl.pallas_call(
            place,
            out_shape=(out, out, out),
            in_specs=[vmem, vmem],
            out_specs=(any_space, any_space, any_space),
            scratch_shapes=[dma((6,))],
            compiler_params=pltpu.CompilerParams(vmem_limit_bytes=1024 * 1024),
        )(pltpu.with_memory_space_constraint(oq, pltpu.VMEM), pltpu.with_memory_space_constraint(okv, pltpu.VMEM))
        return q[:, None, :], k[:, None, :], v[:, None, :]

    return jax.shard_map(local_step, mesh=mesh, in_specs=(P(("dp", "tp"), None), P(None), P(None, "tp", None), P(None, "tp"), P(None, "tp")), out_specs=(P("dp", "tp", None), P("dp", "tp", None), P("dp", "tp", None)), check_vma=False)
```

```python
import functools

import jax
import jax.numpy as jnp
from jax import lax
from jax.experimental import pallas as pl
from jax.experimental.pallas import tpu as pltpu
from jax.sharding import PartitionSpec as P

EPSILON = 1e-6
LANES = 128
NORM_ROWS = 32
CHUNK = 128
OWN_ROWS = 256
MESH = pl.DeviceIdType.MESH


def exchange(chips, x, gain, wq, wk, wv, oq, okv, gain_row, n, w, slq, srq, srkv, x_sem, wl_sem, wl_s, wl_r, wx_s, wx_r, wg_s, wg_r, wd_s, wd_r, n_s, n_r,
             oq_s, oq_r, okv_s, okv_r, rq_s, rq_r, rkv_s, rkv_r, lq_s, lq_r, lkv_s, lkv_r, fk_s, fk_r):
    rows, depth = x.shape
    chunks = rows // CHUNK
    group = lax.axis_index("dp")
    device = lax.axis_index("tp")
    half = lax.rem(group, 2)
    core = lax.rem(device, 2)
    chip = lax.div(device, 2)
    token_chip = chip + 1 - 2 * lax.rem(chip, 2)
    weight_chip = chips - 1 - chip
    far_chip = weight_chip + 1 - 2 * lax.rem(weight_chip, 2)
    other_core = 1 - core
    partner = {"tp": 2 * chip + other_core}
    token_peer = {"tp": 2 * token_chip + core}
    weight_peer = {"tp": 2 * weight_chip + core}
    group_peer = {"dp": group + 1 - 2 * half}

    def weight_core(c):
        return {"tp": 2 * weight_chip + c}

    def remote(src, dst, send, recv, to):
        return pltpu.make_async_remote_copy(src_ref=src, dst_ref=dst, send_sem=send, recv_sem=recv, device_id=to, device_id_type=MESH)

    def block(c, on_chip):
        return pl.multiple_of((2 * on_chip + c) * rows, rows)

    def chunk_of(j):
        return pl.ds(pl.multiple_of(j * CHUNK, CHUNK), CHUNK)

    def load_x(j):
        return pltpu.make_async_copy(x.at[chunk_of(j)], n.at[0, chunk_of(j)], x_sem.at[j])

    for j in range(chunks):
        load_x(j).start()

    gain_row[...] = gain[...].reshape(1, depth)
    q_half = [wq.at[:, pl.ds(h * LANES, LANES)] for h in range(2)]
    kv = [wk, wv]

    barrier = pltpu.get_barrier_semaphore()
    for peer in (partner, token_peer, weight_peer, weight_core(other_core), group_peer):
        pl.semaphore_signal(barrier, inc=1, device_id=peer, device_id_type=MESH)
    pl.semaphore_wait(barrier, 5)

    w_first = w.at[1, half, core, :, pl.ds(0, LANES)]
    w_second = w.at[1, half, core, :, pl.ds(LANES, LANES)]
    remote(wq.at[:, pl.ds(pl.multiple_of(half * LANES, LANES), LANES)], w_first, wx_s, wx_r.at[0], weight_peer).start()
    for h in range(2):
        @pl.when(half == h)
        def _():
            remote(kv[h], w_second, wx_s, wx_r.at[1], weight_peer).start()
    for h in range(2):
        for part, src in enumerate((q_half[h], kv[h])):
            dst = w.at[0, h, core, :, pl.ds(part * LANES, LANES)]
            remote(src, dst, wl_s, wl_r, partner).start()
            pltpu.make_async_copy(src, dst, wl_sem).start()

    def send_n(j):
        return remote(n.at[0, chunk_of(j)], n.at[1, chunk_of(j)], n_s, n_r.at[j], token_peer)

    @pl.loop(0, chunks)
    def _(j):
        load_x(j).wait()

        @pl.loop(0, CHUNK // NORM_ROWS)
        def _(i):
            at = pl.ds(pl.multiple_of(j * CHUNK + i * NORM_ROWS, NORM_ROWS), NORM_ROWS)
            wide = n[0, at, :].astype(jnp.float32)
            mean_sq = jnp.mean(wide * wide, axis=-1, keepdims=True)
            n[0, at, :] = (wide * lax.rsqrt(mean_sq + EPSILON) * gain_row[...]).astype(jnp.bfloat16)

        send_n(j).start()

    def product(blk, at, side, h, c):
        return jnp.dot(n[blk, at, :], w[side, h, c], preferred_element_type=jnp.float32).astype(jnp.bfloat16)

    def local_products(blk, base, start, size):
        at = pl.ds(start, size)
        out = pl.ds(pl.multiple_of(base + start, size), size)

        @pl.loop(0, 2)
        def _(h):
            for b in range(2):
                c = lax.rem(core + b, 2)
                both = product(blk, at, 0, h, c)
                if b == 0:
                    oq[h, out, :] = both[:, :LANES]
                else:
                    slq[blk, h, at, :] = both[:, :LANES]
                okv[h, c, out, :] = both[:, LANES:]
        remote(slq.at[blk, :, at], oq.at[:, out], lq_s.at[blk], lq_r.at[blk], partner).start()
        remote(okv.at[:, :, out], okv.at[:, :, out], lkv_s.at[blk], lkv_r.at[blk], partner).start()

    own = block(core, chip)
    near = block(core, token_chip)

    own_w = w.at[0, :, core]
    pltpu.make_async_copy(own_w, own_w, wl_sem).wait()
    other_w = w.at[0, :, other_core]
    remote(other_w, other_w, wl_s, wl_r, partner).wait_recv()

    @pl.loop(0, rows // OWN_ROWS)
    def _(i):
        local_products(0, own, pl.multiple_of(i * OWN_ROWS, OWN_ROWS), OWN_ROWS)

    def own_part(h, c, part):
        @pl.loop(0, rows // OWN_ROWS)
        def _(i):
            at = pl.ds(pl.multiple_of(i * OWN_ROWS, OWN_ROWS), OWN_ROWS)
            piece = w[1, h, c, :, part * LANES:(part + 1) * LANES]
            value = jnp.dot(n[0, at, :], piece, preferred_element_type=jnp.float32).astype(jnp.bfloat16)
            if part == 0:
                srq[0, c, h, at, :] = value
            else:
                srkv[0, h, c, at, :] = value

    def send_own(h, c, part):
        out = pl.ds(own, rows)
        if part == 0:
            remote(srq.at[0, c, h], oq.at[h, out], oq_s, oq_r.at[core], weight_core(c)).start()
        else:
            remote(srkv.at[0, h, c], okv.at[h, c, out], okv_s, okv_r, weight_peer).start()

    for part, piece in enumerate((w_first, w_second)):
        remote(piece, piece, wx_s, wx_r.at[part], weight_peer).wait_recv()
        remote(piece, piece, wg_s, wg_r, group_peer).start()
        remote(piece, piece, wd_s.at[0], wd_r.at[0], partner).start()
        own_part(half, core, part)
        send_own(half, core, part)

    def own_products(h, c):
        @pl.loop(0, rows // OWN_ROWS)
        def _(i):
            at = pl.ds(pl.multiple_of(i * OWN_ROWS, OWN_ROWS), OWN_ROWS)
            both = product(0, at, 1, h, c)
            srq[0, c, h, at, :] = both[:, :LANES]
            srkv[0, h, c, at, :] = both[:, LANES:]
        for part in range(2):
            send_own(h, c, part)

    other_half = 1 - half
    from_partner = w.at[1, half, other_core]
    remote(from_partner, from_partner, wd_s.at[0], wd_r.at[0], partner).wait_recv()
    own_products(half, other_core)
    from_group = w.at[1, other_half, core]
    remote(from_group, from_group, wg_s, wg_r, group_peer).wait_recv()
    remote(from_group, from_group, wd_s.at[1], wd_r.at[1], partner).start()
    own_products(other_half, core)
    from_both = w.at[1, other_half, other_core]
    remote(from_both, from_both, wd_s.at[1], wd_r.at[1], partner).wait_recv()
    own_products(other_half, other_core)

    @pl.loop(0, chunks)
    def _(j):
        send_n(j).wait_recv()
        start = pl.multiple_of(j * CHUNK, CHUNK)
        at = pl.ds(start, CHUNK)
        out = pl.ds(pl.multiple_of(near + start, CHUNK), CHUNK)

        @pl.loop(0, 2)
        def _(h):
            for c in range(2):
                both = product(1, at, 1, h, c)
                srq[1, c, h, at, :] = both[:, :LANES]
                srkv[1, h, c, at, :] = both[:, LANES:]
        remote(srkv.at[1, :, :, at], okv.at[:, :, out], rkv_s, rkv_r.at[j], weight_peer).start()
        for c in range(2):
            remote(srq.at[1, c, :, at], oq.at[:, out], rq_s, rq_r.at[core], weight_core(c)).start()
        local_products(1, near, start, CHUNK)

    beside = pl.ds(block(core, weight_chip), rows)
    arrived = okv.at[:, :, beside]
    remote(arrived, arrived, okv_s, okv_r, weight_peer).wait_recv()
    remote(arrived, arrived, fk_s.at[0], fk_r.at[0], partner).start()
    far = block(core, far_chip)

    @pl.loop(0, chunks)
    def _(j):
        piece = okv.at[:, :, pl.ds(pl.multiple_of(far + j * CHUNK, CHUNK), CHUNK)]
        remote(piece, piece, rkv_s, rkv_r.at[j], weight_peer).wait_recv()
        remote(piece, piece, fk_s.at[1], fk_r.at[1], partner).start()

    def all_q(c, on_chip):
        return oq.at[:, pl.ds(block(c, on_chip), rows)]

    def all_kv(c, on_chip):
        return okv.at[:, :, pl.ds(block(c, on_chip), rows)]

    for c in range(2):
        remote(all_q(c, weight_chip), all_q(c, weight_chip), oq_s, oq_r.at[c], weight_peer).wait_recv()
        remote(all_q(c, far_chip), all_q(c, far_chip), rq_s, rq_r.at[c], weight_peer).wait_recv()
    for i, on_chip in enumerate((chip, token_chip)):
        remote(all_q(other_core, on_chip), all_q(other_core, on_chip), lq_s.at[i], lq_r.at[i], partner).wait_recv()
        remote(all_kv(other_core, on_chip), all_kv(other_core, on_chip), lkv_s.at[i], lkv_r.at[i], partner).wait_recv()
    for i, on_chip in enumerate((weight_chip, far_chip)):
        remote(all_kv(other_core, on_chip), all_kv(other_core, on_chip), fk_s.at[i], fk_r.at[i], partner).wait_recv()

    def sent(ref, sem):
        remote(ref, ref, sem, n_r.at[0], partner).wait_send()

    sent(own_w, wl_s)
    sent(w.at[1, 0, 0], wx_s)
    sent(w.at[1, 0, 0], wg_s)
    for i in range(2):
        sent(w.at[1, 0, 0], wd_s.at[i])
        sent(slq.at[i], lq_s.at[i])
        sent(srkv.at[0], lkv_s.at[i])
        sent(srkv.at[0], fk_s.at[i])
    sent(n.at[0], n_s)
    sent(srq.at[0], oq_s)
    sent(srkv.at[0], okv_s)
    sent(srq.at[1], rq_s)
    sent(srkv.at[1], rkv_s)


def place(oq, okv, q, k, v, sems):
    copies = []
    for h in range(2):
        cols = pl.ds(h * LANES, LANES)
        copies.append(pltpu.make_async_copy(oq.at[h], q.at[:, cols], sems.at[h]))
        copies.append(pltpu.make_async_copy(okv.at[0, h], k.at[:, cols], sems.at[2 + h]))
        copies.append(pltpu.make_async_copy(okv.at[1, h], v.at[:, cols], sems.at[4 + h]))
    for copy in copies:
        copy.start()
    for copy in copies:
        copy.wait()


def solution(mesh):
    group_size = mesh.shape["tp"]
    chips = group_size // 2

    def local_step(x_rows, norm_gain, w_q, w_k, w_v):
        rows, depth = x_rows.shape
        head = w_q.shape[2]
        tokens = rows * group_size
        dtype = x_rows.dtype
        any_space = pl.BlockSpec(memory_space=pl.ANY)
        vmem = pl.BlockSpec(memory_space=pltpu.VMEM)
        dma = pltpu.SemaphoreType.DMA
        chunks = rows // CHUNK
        oq, okv = pl.pallas_call(
            functools.partial(exchange, chips),
            out_shape=(pltpu.VMEM((2, tokens, LANES), dtype), pltpu.VMEM((2, 2, tokens, LANES), dtype)),
            in_specs=[any_space, vmem, any_space, any_space, any_space],
            out_specs=(vmem, vmem),
            scratch_shapes=[
                pltpu.VMEM((1, depth), norm_gain.dtype),
                pltpu.VMEM((2, rows, depth), dtype),
                pltpu.VMEM((2, 2, 2, depth, 2 * LANES), dtype),
                pltpu.VMEM((2, 2, rows, LANES), dtype),
                pltpu.VMEM((2, 2, 2, rows, LANES), dtype),
                pltpu.VMEM((2, 2, 2, rows, LANES), dtype),
                dma((chunks,)),
                dma, dma, dma,
                dma, dma((2,)),
                dma, dma,
                dma((2,)), dma((2,)),
                dma, dma((chunks,)),
                dma, dma((2,)), dma, dma,
                dma, dma((2,)), dma, dma((chunks,)),
                dma((2,)), dma((2,)), dma((2,)), dma((2,)),
                dma((2,)), dma((2,)),
            ],
            compiler_params=pltpu.CompilerParams(collective_id=0, has_side_effects=True, vmem_limit_bytes=46 * 1024 * 1024),
        )(x_rows, norm_gain, w_q.reshape(depth, head), w_k, w_v)
        out = jax.ShapeDtypeStruct((tokens, head), dtype)
        q, k, v = pl.pallas_call(
            place,
            out_shape=(out, out, out),
            in_specs=[vmem, vmem],
            out_specs=(any_space, any_space, any_space),
            scratch_shapes=[dma((6,))],
            compiler_params=pltpu.CompilerParams(vmem_limit_bytes=1024 * 1024),
        )(pltpu.with_memory_space_constraint(oq, pltpu.VMEM), pltpu.with_memory_space_constraint(okv, pltpu.VMEM))
        return q[:, None, :], k[:, None, :], v[:, None, :]

    return jax.shard_map(local_step, mesh=mesh, in_specs=(P(("dp", "tp"), None), P(None), P(None, "tp", None), P(None, "tp"), P(None, "tp")), out_specs=(P("dp", "tp", None), P("dp", "tp", None), P("dp", "tp", None)), check_vma=False)
```

```python
import functools

import jax
import jax.numpy as jnp
from jax import lax
from jax.experimental import pallas as pl
from jax.experimental.pallas import tpu as pltpu
from jax.sharding import PartitionSpec as P

EPSILON = 1e-6
LANES = 128
NORM_ROWS = 32
CHUNK = 128
OWN_ROWS = 256
PLACE_BLOCKS = 4
MESH = pl.DeviceIdType.MESH


def exchange(chips, x, gain, wq, wk, wv, oq, okv, gain_copy, gain_row, n, w, slq, srq, srkv, g_sem, x_sem, wl_sem, wl_s, wl_r, wx_s, wx_r, wg_s, wg_r, wd_s, wd_r, n_s, n_r,
             oq_s, oq_r, okv_s, okv_r, rq_s, rq_r, rkv_s, rkv_r, lq_s, lq_r, lkv_s, lkv_r, fk_s, fk_r):
    rows, depth = x.shape
    chunks = rows // CHUNK
    group = lax.axis_index("dp")
    device = lax.axis_index("tp")
    half = lax.rem(group, 2)
    core = lax.rem(device, 2)
    chip = lax.div(device, 2)
    token_chip = chip + 1 - 2 * lax.rem(chip, 2)
    weight_chip = chips - 1 - chip
    far_chip = weight_chip + 1 - 2 * lax.rem(weight_chip, 2)
    other_core = 1 - core
    partner = {"tp": 2 * chip + other_core}
    token_peer = {"tp": 2 * token_chip + core}
    weight_peer = {"tp": 2 * weight_chip + core}
    group_peer = {"dp": group + 1 - 2 * half}

    def weight_core(c):
        return {"tp": 2 * weight_chip + c}

    def remote(src, dst, send, recv, to):
        return pltpu.make_async_remote_copy(src_ref=src, dst_ref=dst, send_sem=send, recv_sem=recv, device_id=to, device_id_type=MESH)

    def block(c, on_chip):
        return pl.multiple_of((2 * on_chip + c) * rows, rows)

    def chunk_of(j):
        return pl.ds(pl.multiple_of(j * CHUNK, CHUNK), CHUNK)

    def load_x(j):
        return pltpu.make_async_copy(x.at[chunk_of(j)], n.at[0, chunk_of(j)], x_sem.at[j])

    q_half = [wq.at[:, pl.ds(h * LANES, LANES)] for h in range(2)]
    kv = [wk, wv]

    def own_w_part(h, part):
        return w.at[0, h, core, :, pl.ds(part * LANES, LANES)]

    barrier = pltpu.get_barrier_semaphore()
    for peer in (partner, token_peer, weight_peer, weight_core(other_core), group_peer):
        pl.semaphore_signal(barrier, inc=1, device_id=peer, device_id_type=MESH)
    first = own_w_part(half, 0)
    pltpu.make_async_copy(wq.at[:, pl.ds(pl.multiple_of(half * LANES, LANES), LANES)], first, wl_sem.at[0]).start()
    second = own_w_part(1 - half, 0)
    pltpu.make_async_copy(wq.at[:, pl.ds(pl.multiple_of((1 - half) * LANES, LANES), LANES)], second, wl_sem.at[1]).start()
    for h in range(2):
        pltpu.make_async_copy(kv[h], own_w_part(h, 1), wl_sem.at[2 + h]).start()
    gain_load = pltpu.make_async_copy(gain, gain_copy, g_sem)
    gain_load.start()
    for j in range(chunks):
        load_x(j).start()
    pltpu.make_async_copy(first, first, wl_sem.at[0]).wait()
    pl.semaphore_wait(barrier, 5)

    w_first = w.at[1, half, core, :, pl.ds(0, LANES)]
    w_second = w.at[1, half, core, :, pl.ds(LANES, LANES)]
    remote(first, w_first, wx_s, wx_r.at[0], weight_peer).start()
    for h in range(2):
        @pl.when(half == h)
        def _():
            remote(kv[h], w_second, wx_s, wx_r.at[1], weight_peer).start()
    for h in range(2):
        for part, src in enumerate((q_half[h], kv[h])):
            remote(src, own_w_part(h, part), wl_s, wl_r, partner).start()
    gain_load.wait()
    gain_row[...] = gain_copy[...].reshape(1, depth)

    def send_n(j):
        return remote(n.at[0, chunk_of(j)], n.at[1, chunk_of(j)], n_s, n_r.at[j], token_peer)

    @pl.loop(0, chunks)
    def _(j):
        load_x(j).wait()

        @pl.loop(0, CHUNK // NORM_ROWS)
        def _(i):
            at = pl.ds(pl.multiple_of(j * CHUNK + i * NORM_ROWS, NORM_ROWS), NORM_ROWS)
            wide = n[0, at, :].astype(jnp.float32)
            mean_sq = jnp.mean(wide * wide, axis=-1, keepdims=True)
            n[0, at, :] = (wide * lax.rsqrt(mean_sq + EPSILON) * gain_row[...]).astype(jnp.bfloat16)

        send_n(j).start()

    def product(blk, at, side, h, c):
        return jnp.dot(n[blk, at, :], w[side, h, c], preferred_element_type=jnp.float32).astype(jnp.bfloat16)

    def local_products(blk, base, start, size):
        at = pl.ds(start, size)
        out = pl.ds(pl.multiple_of(base + start, size), size)

        @pl.loop(0, 2)
        def _(h):
            for b in range(2):
                c = lax.rem(core + b, 2)
                both = product(blk, at, 0, h, c)
                if b == 0:
                    oq[h, out, :] = both[:, :LANES]
                else:
                    slq[blk, h, at, :] = both[:, :LANES]
                okv[h, c, out, :] = both[:, LANES:]
        remote(slq.at[blk, :, at], oq.at[:, out], lq_s.at[blk], lq_r.at[blk], partner).start()
        remote(okv.at[:, :, out], okv.at[:, :, out], lkv_s.at[blk], lkv_r.at[blk], partner).start()

    own = block(core, chip)
    near = block(core, token_chip)

    own_w = w.at[0, :, core]
    pltpu.make_async_copy(second, second, wl_sem.at[1]).wait()
    for h in range(2):
        pltpu.make_async_copy(kv[h], own_w_part(h, 1), wl_sem.at[2 + h]).wait()
    other_w = w.at[0, :, other_core]
    remote(other_w, other_w, wl_s, wl_r, partner).wait_recv()

    @pl.loop(0, rows // OWN_ROWS)
    def _(i):
        local_products(0, own, pl.multiple_of(i * OWN_ROWS, OWN_ROWS), OWN_ROWS)

    def own_part(h, c, part):
        @pl.loop(0, rows // OWN_ROWS)
        def _(i):
            at = pl.ds(pl.multiple_of(i * OWN_ROWS, OWN_ROWS), OWN_ROWS)
            piece = w[1, h, c, :, part * LANES:(part + 1) * LANES]
            value = jnp.dot(n[0, at, :], piece, preferred_element_type=jnp.float32).astype(jnp.bfloat16)
            if part == 0:
                srq[0, c, h, at, :] = value
            else:
                srkv[0, h, c, at, :] = value

    def send_own(h, c, part):
        out = pl.ds(own, rows)
        if part == 0:
            remote(srq.at[0, c, h], oq.at[h, out], oq_s, oq_r.at[core], weight_core(c)).start()
        else:
            remote(srkv.at[0, h, c], okv.at[h, c, out], okv_s, okv_r, weight_peer).start()

    for part, piece in enumerate((w_first, w_second)):
        remote(piece, piece, wx_s, wx_r.at[part], weight_peer).wait_recv()
        remote(piece, piece, wg_s, wg_r, group_peer).start()
        remote(piece, piece, wd_s.at[0], wd_r.at[0], partner).start()
        own_part(half, core, part)
        send_own(half, core, part)

    def own_products(h, c):
        @pl.loop(0, rows // OWN_ROWS)
        def _(i):
            at = pl.ds(pl.multiple_of(i * OWN_ROWS, OWN_ROWS), OWN_ROWS)
            both = product(0, at, 1, h, c)
            srq[0, c, h, at, :] = both[:, :LANES]
            srkv[0, h, c, at, :] = both[:, LANES:]
        for part in range(2):
            send_own(h, c, part)

    other_half = 1 - half
    from_partner = w.at[1, half, other_core]
    remote(from_partner, from_partner, wd_s.at[0], wd_r.at[0], partner).wait_recv()
    own_products(half, other_core)
    from_group = w.at[1, other_half, core]
    remote(from_group, from_group, wg_s, wg_r, group_peer).wait_recv()
    remote(from_group, from_group, wd_s.at[1], wd_r.at[1], partner).start()
    own_products(other_half, core)
    from_both = w.at[1, other_half, other_core]
    remote(from_both, from_both, wd_s.at[1], wd_r.at[1], partner).wait_recv()
    own_products(other_half, other_core)

    @pl.loop(0, chunks)
    def _(j):
        send_n(j).wait_recv()
        start = pl.multiple_of(j * CHUNK, CHUNK)
        at = pl.ds(start, CHUNK)
        out = pl.ds(pl.multiple_of(near + start, CHUNK), CHUNK)

        @pl.loop(0, 2)
        def _(h):
            for c in range(2):
                both = product(1, at, 1, h, c)
                srq[1, c, h, at, :] = both[:, :LANES]
                srkv[1, h, c, at, :] = both[:, LANES:]
        remote(srkv.at[1, :, :, at], okv.at[:, :, out], rkv_s, rkv_r.at[j], weight_peer).start()
        for c in range(2):
            remote(srq.at[1, c, :, at], oq.at[:, out], rq_s, rq_r.at[core], weight_core(c)).start()
        local_products(1, near, start, CHUNK)

    beside = pl.ds(block(core, weight_chip), rows)
    arrived = okv.at[:, :, beside]
    remote(arrived, arrived, okv_s, okv_r, weight_peer).wait_recv()
    remote(arrived, arrived, fk_s.at[0], fk_r.at[0], partner).start()
    far = block(core, far_chip)

    @pl.loop(0, chunks)
    def _(j):
        piece = okv.at[:, :, pl.ds(pl.multiple_of(far + j * CHUNK, CHUNK), CHUNK)]
        remote(piece, piece, rkv_s, rkv_r.at[j], weight_peer).wait_recv()
        remote(piece, piece, fk_s.at[1], fk_r.at[1], partner).start()

    def all_q(c, on_chip):
        return oq.at[:, pl.ds(block(c, on_chip), rows)]

    def all_kv(c, on_chip):
        return okv.at[:, :, pl.ds(block(c, on_chip), rows)]

    for c in range(2):
        remote(all_q(c, weight_chip), all_q(c, weight_chip), oq_s, oq_r.at[c], weight_peer).wait_recv()
        remote(all_q(c, far_chip), all_q(c, far_chip), rq_s, rq_r.at[c], weight_peer).wait_recv()
    for i, on_chip in enumerate((chip, token_chip)):
        remote(all_q(other_core, on_chip), all_q(other_core, on_chip), lq_s.at[i], lq_r.at[i], partner).wait_recv()
        remote(all_kv(other_core, on_chip), all_kv(other_core, on_chip), lkv_s.at[i], lkv_r.at[i], partner).wait_recv()
    for i, on_chip in enumerate((weight_chip, far_chip)):
        remote(all_kv(other_core, on_chip), all_kv(other_core, on_chip), fk_s.at[i], fk_r.at[i], partner).wait_recv()

    def sent(ref, sem):
        remote(ref, ref, sem, n_r.at[0], partner).wait_send()

    sent(own_w, wl_s)
    sent(w.at[1, 0, 0], wx_s)
    sent(w.at[1, 0, 0], wg_s)
    for i in range(2):
        sent(w.at[1, 0, 0], wd_s.at[i])
        sent(slq.at[i], lq_s.at[i])
        sent(srkv.at[0], lkv_s.at[i])
        sent(srkv.at[0], fk_s.at[i])
    sent(n.at[0], n_s)
    sent(srq.at[0], oq_s)
    sent(srkv.at[0], okv_s)
    sent(srq.at[1], rq_s)
    sent(srkv.at[1], rkv_s)


def place(oq, okv, q, k, v, sems):
    rows = oq.shape[1] // PLACE_BLOCKS
    copies = []
    for i in range(PLACE_BLOCKS):
        at = pl.ds(i * rows, rows)
        for h in range(2):
            cols = pl.ds(h * LANES, LANES)
            for a, (src, dst) in enumerate(((oq, q), (okv.at[0], k), (okv.at[1], v))):
                copies.append(pltpu.make_async_copy(src.at[h, at], dst.at[at, cols], sems.at[i, h, a]))
    for copy in copies:
        copy.start()
    for copy in copies:
        copy.wait()


def solution(mesh):
    group_size = mesh.shape["tp"]
    chips = group_size // 2

    def local_step(x_rows, norm_gain, w_q, w_k, w_v):
        rows, depth = x_rows.shape
        head = w_q.shape[2]
        tokens = rows * group_size
        dtype = x_rows.dtype
        any_space = pl.BlockSpec(memory_space=pl.ANY)
        vmem = pl.BlockSpec(memory_space=pltpu.VMEM)
        dma = pltpu.SemaphoreType.DMA
        chunks = rows // CHUNK
        oq, okv = pl.pallas_call(
            functools.partial(exchange, chips),
            out_shape=(pltpu.VMEM((2, tokens, LANES), dtype), pltpu.VMEM((2, 2, tokens, LANES), dtype)),
            in_specs=[any_space] * 5,
            out_specs=(vmem, vmem),
            scratch_shapes=[
                pltpu.VMEM((depth,), norm_gain.dtype),
                pltpu.VMEM((1, depth), norm_gain.dtype),
                pltpu.VMEM((2, rows, depth), dtype),
                pltpu.VMEM((2, 2, 2, depth, 2 * LANES), dtype),
                pltpu.VMEM((2, 2, rows, LANES), dtype),
                pltpu.VMEM((2, 2, 2, rows, LANES), dtype),
                pltpu.VMEM((2, 2, 2, rows, LANES), dtype),
                dma, dma((chunks,)),
                dma((4,)), dma, dma,
                dma, dma((2,)),
                dma, dma,
                dma((2,)), dma((2,)),
                dma, dma((chunks,)),
                dma, dma((2,)), dma, dma,
                dma, dma((2,)), dma, dma((chunks,)),
                dma((2,)), dma((2,)), dma((2,)), dma((2,)),
                dma((2,)), dma((2,)),
            ],
            compiler_params=pltpu.CompilerParams(collective_id=0, has_side_effects=True, vmem_limit_bytes=46 * 1024 * 1024),
        )(x_rows, norm_gain, w_q.reshape(depth, head), w_k, w_v)
        out = jax.ShapeDtypeStruct((tokens, head), dtype)
        q, k, v = pl.pallas_call(
            place,
            out_shape=(out, out, out),
            in_specs=[vmem, vmem],
            out_specs=(any_space, any_space, any_space),
            scratch_shapes=[dma((PLACE_BLOCKS, 2, 3))],
            compiler_params=pltpu.CompilerParams(vmem_limit_bytes=1024 * 1024),
        )(pltpu.with_memory_space_constraint(oq, pltpu.VMEM), pltpu.with_memory_space_constraint(okv, pltpu.VMEM))
        return q[:, None, :], k[:, None, :], v[:, None, :]

    return jax.shard_map(local_step, mesh=mesh, in_specs=(P(("dp", "tp"), None), P(None), P(None, "tp", None), P(None, "tp"), P(None, "tp")), out_specs=(P("dp", "tp", None), P("dp", "tp", None), P("dp", "tp", None)), check_vma=False)
```

```python
import functools

import jax
import jax.numpy as jnp
from jax import lax
from jax.experimental import pallas as pl
from jax.experimental.pallas import tpu as pltpu
from jax.sharding import PartitionSpec as P

EPSILON = 1e-6
LANES = 128
NORM_ROWS = 32
CHUNK = 128
OWN_ROWS = 256
PLACE_BLOCKS = 1
MESH = pl.DeviceIdType.MESH


def exchange(chips, x, gain, wq, wk, wv, oq, okv, gain_copy, gain_row, n, w, slq, srq, srkv, g_sem, x_sem, wl_sem, wl_s, wl_r, wx_s, wx_r, wg_s, wg_r, wd_s, wd_r, n_s, n_r,
             oq_s, oq_r, okv_s, okv_r, rq_s, rq_r, rkv_s, rkv_r, lq_s, lq_r, lkv_s, lkv_r, fk_s, fk_r):
    rows, depth = x.shape
    chunks = rows // CHUNK
    group = lax.axis_index("dp")
    device = lax.axis_index("tp")
    half = lax.rem(group, 2)
    core = lax.rem(device, 2)
    chip = lax.div(device, 2)
    token_chip = chips - 1 - chip
    weight_chip = chip + 1 - 2 * lax.rem(chip, 2)
    far_chip = chips - 1 - weight_chip
    other_core = 1 - core
    partner = {"tp": 2 * chip + other_core}
    token_peer = {"tp": 2 * token_chip + core}
    weight_peer = {"tp": 2 * weight_chip + core}
    group_peer = {"dp": group + 1 - 2 * half}

    def weight_core(c):
        return {"tp": 2 * weight_chip + c}

    def remote(src, dst, send, recv, to):
        return pltpu.make_async_remote_copy(src_ref=src, dst_ref=dst, send_sem=send, recv_sem=recv, device_id=to, device_id_type=MESH)

    def block(c, on_chip):
        return pl.multiple_of((2 * on_chip + c) * rows, rows)

    def chunk_of(j):
        return pl.ds(pl.multiple_of(j * CHUNK, CHUNK), CHUNK)

    def load_x(j):
        return pltpu.make_async_copy(x.at[chunk_of(j)], n.at[0, chunk_of(j)], x_sem.at[j])

    q_half = [wq.at[:, pl.ds(h * LANES, LANES)] for h in range(2)]
    kv = [wk, wv]

    def own_w_part(h, part):
        return w.at[0, h, core, :, pl.ds(part * LANES, LANES)]

    barrier = pltpu.get_barrier_semaphore()
    for peer in (partner, token_peer, weight_peer, weight_core(other_core), group_peer):
        pl.semaphore_signal(barrier, inc=1, device_id=peer, device_id_type=MESH)
    first = own_w_part(half, 0)
    pltpu.make_async_copy(wq.at[:, pl.ds(pl.multiple_of(half * LANES, LANES), LANES)], first, wl_sem.at[0]).start()
    second = own_w_part(1 - half, 0)
    pltpu.make_async_copy(wq.at[:, pl.ds(pl.multiple_of((1 - half) * LANES, LANES), LANES)], second, wl_sem.at[1]).start()
    for h in range(2):
        pltpu.make_async_copy(kv[h], own_w_part(h, 1), wl_sem.at[2 + h]).start()
    gain_load = pltpu.make_async_copy(gain, gain_copy, g_sem)
    gain_load.start()
    for j in range(chunks):
        load_x(j).start()
    pltpu.make_async_copy(first, first, wl_sem.at[0]).wait()
    pl.semaphore_wait(barrier, 5)

    w_first = w.at[1, half, core, :, pl.ds(0, LANES)]
    w_second = w.at[1, half, core, :, pl.ds(LANES, LANES)]
    remote(first, w_first, wx_s, wx_r.at[0], weight_peer).start()
    for h in range(2):
        @pl.when(half == h)
        def _():
            remote(kv[h], w_second, wx_s, wx_r.at[1], weight_peer).start()
    for h in range(2):
        for part, src in enumerate((q_half[h], kv[h])):
            remote(src, own_w_part(h, part), wl_s, wl_r, partner).start()
    gain_load.wait()
    gain_row[...] = gain_copy[...].reshape(1, depth)

    def send_n(j):
        return remote(n.at[0, chunk_of(j)], n.at[1, chunk_of(j)], n_s, n_r.at[j], token_peer)

    @pl.loop(0, chunks)
    def _(j):
        load_x(j).wait()

        @pl.loop(0, CHUNK // NORM_ROWS)
        def _(i):
            at = pl.ds(pl.multiple_of(j * CHUNK + i * NORM_ROWS, NORM_ROWS), NORM_ROWS)
            wide = n[0, at, :].astype(jnp.float32)
            mean_sq = jnp.mean(wide * wide, axis=-1, keepdims=True)
            n[0, at, :] = (wide * lax.rsqrt(mean_sq + EPSILON) * gain_row[...]).astype(jnp.bfloat16)

        send_n(j).start()

    def product(blk, at, side, h, c):
        return jnp.dot(n[blk, at, :], w[side, h, c], preferred_element_type=jnp.float32).astype(jnp.bfloat16)

    def local_products(blk, base, start, size):
        at = pl.ds(start, size)
        out = pl.ds(pl.multiple_of(base + start, size), size)

        @pl.loop(0, 2)
        def _(h):
            for b in range(2):
                c = lax.rem(core + b, 2)
                both = product(blk, at, 0, h, c)
                if b == 0:
                    oq[h, out, :] = both[:, :LANES]
                else:
                    slq[blk, h, at, :] = both[:, :LANES]
                okv[h, c, out, :] = both[:, LANES:]
        remote(slq.at[blk, :, at], oq.at[:, out], lq_s.at[blk], lq_r.at[blk], partner).start()
        remote(okv.at[:, :, out], okv.at[:, :, out], lkv_s.at[blk], lkv_r.at[blk], partner).start()

    own = block(core, chip)
    near = block(core, token_chip)

    own_w = w.at[0, :, core]
    pltpu.make_async_copy(second, second, wl_sem.at[1]).wait()
    for h in range(2):
        pltpu.make_async_copy(kv[h], own_w_part(h, 1), wl_sem.at[2 + h]).wait()
    other_w = w.at[0, :, other_core]
    remote(other_w, other_w, wl_s, wl_r, partner).wait_recv()

    @pl.loop(0, rows // OWN_ROWS)
    def _(i):
        local_products(0, own, pl.multiple_of(i * OWN_ROWS, OWN_ROWS), OWN_ROWS)

    def own_part(h, c, part):
        @pl.loop(0, rows // OWN_ROWS)
        def _(i):
            at = pl.ds(pl.multiple_of(i * OWN_ROWS, OWN_ROWS), OWN_ROWS)
            piece = w[1, h, c, :, part * LANES:(part + 1) * LANES]
            value = jnp.dot(n[0, at, :], piece, preferred_element_type=jnp.float32).astype(jnp.bfloat16)
            if part == 0:
                srq[0, c, h, at, :] = value
            else:
                srkv[0, h, c, at, :] = value

    def send_own(h, c, part):
        out = pl.ds(own, rows)
        if part == 0:
            remote(srq.at[0, c, h], oq.at[h, out], oq_s, oq_r.at[core], weight_core(c)).start()
        else:
            remote(srkv.at[0, h, c], okv.at[h, c, out], okv_s, okv_r, weight_peer).start()

    for part, piece in enumerate((w_first, w_second)):
        remote(piece, piece, wx_s, wx_r.at[part], weight_peer).wait_recv()
        remote(piece, piece, wg_s, wg_r, group_peer).start()
        remote(piece, piece, wd_s.at[0], wd_r.at[0], partner).start()
        own_part(half, core, part)
        send_own(half, core, part)

    def own_products(h, c):
        @pl.loop(0, rows // OWN_ROWS)
        def _(i):
            at = pl.ds(pl.multiple_of(i * OWN_ROWS, OWN_ROWS), OWN_ROWS)
            both = product(0, at, 1, h, c)
            srq[0, c, h, at, :] = both[:, :LANES]
            srkv[0, h, c, at, :] = both[:, LANES:]
        for part in range(2):
            send_own(h, c, part)

    other_half = 1 - half
    from_partner = w.at[1, half, other_core]
    remote(from_partner, from_partner, wd_s.at[0], wd_r.at[0], partner).wait_recv()
    own_products(half, other_core)
    from_group = w.at[1, other_half, core]
    remote(from_group, from_group, wg_s, wg_r, group_peer).wait_recv()
    remote(from_group, from_group, wd_s.at[1], wd_r.at[1], partner).start()
    own_products(other_half, core)
    from_both = w.at[1, other_half, other_core]
    remote(from_both, from_both, wd_s.at[1], wd_r.at[1], partner).wait_recv()
    own_products(other_half, other_core)

    @pl.loop(0, chunks)
    def _(j):
        send_n(j).wait_recv()
        start = pl.multiple_of(j * CHUNK, CHUNK)
        at = pl.ds(start, CHUNK)
        out = pl.ds(pl.multiple_of(near + start, CHUNK), CHUNK)

        @pl.loop(0, 2)
        def _(h):
            for c in range(2):
                both = product(1, at, 1, h, c)
                srq[1, c, h, at, :] = both[:, :LANES]
                srkv[1, h, c, at, :] = both[:, LANES:]
        remote(srkv.at[1, :, :, at], okv.at[:, :, out], rkv_s, rkv_r.at[j], weight_peer).start()
        for c in range(2):
            remote(srq.at[1, c, :, at], oq.at[:, out], rq_s, rq_r.at[core], weight_core(c)).start()
        local_products(1, near, start, CHUNK)

    beside = pl.ds(block(core, weight_chip), rows)
    arrived = okv.at[:, :, beside]
    remote(arrived, arrived, okv_s, okv_r, weight_peer).wait_recv()
    remote(arrived, arrived, fk_s.at[0], fk_r.at[0], partner).start()
    far = block(core, far_chip)

    @pl.loop(0, chunks)
    def _(j):
        piece = okv.at[:, :, pl.ds(pl.multiple_of(far + j * CHUNK, CHUNK), CHUNK)]
        remote(piece, piece, rkv_s, rkv_r.at[j], weight_peer).wait_recv()
        remote(piece, piece, fk_s.at[1], fk_r.at[1], partner).start()

    def all_q(c, on_chip):
        return oq.at[:, pl.ds(block(c, on_chip), rows)]

    def all_kv(c, on_chip):
        return okv.at[:, :, pl.ds(block(c, on_chip), rows)]

    for c in range(2):
        remote(all_q(c, weight_chip), all_q(c, weight_chip), oq_s, oq_r.at[c], weight_peer).wait_recv()
        remote(all_q(c, far_chip), all_q(c, far_chip), rq_s, rq_r.at[c], weight_peer).wait_recv()
    for i, on_chip in enumerate((chip, token_chip)):
        remote(all_q(other_core, on_chip), all_q(other_core, on_chip), lq_s.at[i], lq_r.at[i], partner).wait_recv()
        remote(all_kv(other_core, on_chip), all_kv(other_core, on_chip), lkv_s.at[i], lkv_r.at[i], partner).wait_recv()
    for i, on_chip in enumerate((weight_chip, far_chip)):
        remote(all_kv(other_core, on_chip), all_kv(other_core, on_chip), fk_s.at[i], fk_r.at[i], partner).wait_recv()

    def sent(ref, sem):
        remote(ref, ref, sem, n_r.at[0], partner).wait_send()

    sent(own_w, wl_s)
    sent(w.at[1, 0, 0], wx_s)
    sent(w.at[1, 0, 0], wg_s)
    for i in range(2):
        sent(w.at[1, 0, 0], wd_s.at[i])
        sent(slq.at[i], lq_s.at[i])
        sent(srkv.at[0], lkv_s.at[i])
        sent(srkv.at[0], fk_s.at[i])
    sent(n.at[0], n_s)
    sent(srq.at[0], oq_s)
    sent(srkv.at[0], okv_s)
    sent(srq.at[1], rq_s)
    sent(srkv.at[1], rkv_s)


def place(oq, okv, q, k, v, sems):
    rows = oq.shape[1] // PLACE_BLOCKS
    copies = []
    for i in range(PLACE_BLOCKS):
        at = pl.ds(i * rows, rows)
        for h in range(2):
            cols = pl.ds(h * LANES, LANES)
            for a, (src, dst) in enumerate(((oq, q), (okv.at[0], k), (okv.at[1], v))):
                copies.append(pltpu.make_async_copy(src.at[h, at], dst.at[at, cols], sems.at[i, h, a]))
    for copy in copies:
        copy.start()
    for copy in copies:
        copy.wait()


def solution(mesh):
    group_size = mesh.shape["tp"]
    chips = group_size // 2

    def local_step(x_rows, norm_gain, w_q, w_k, w_v):
        rows, depth = x_rows.shape
        head = w_q.shape[2]
        tokens = rows * group_size
        dtype = x_rows.dtype
        any_space = pl.BlockSpec(memory_space=pl.ANY)
        vmem = pl.BlockSpec(memory_space=pltpu.VMEM)
        dma = pltpu.SemaphoreType.DMA
        chunks = rows // CHUNK
        oq, okv = pl.pallas_call(
            functools.partial(exchange, chips),
            out_shape=(pltpu.VMEM((2, tokens, LANES), dtype), pltpu.VMEM((2, 2, tokens, LANES), dtype)),
            in_specs=[any_space] * 5,
            out_specs=(vmem, vmem),
            scratch_shapes=[
                pltpu.VMEM((depth,), norm_gain.dtype),
                pltpu.VMEM((1, depth), norm_gain.dtype),
                pltpu.VMEM((2, rows, depth), dtype),
                pltpu.VMEM((2, 2, 2, depth, 2 * LANES), dtype),
                pltpu.VMEM((2, 2, rows, LANES), dtype),
                pltpu.VMEM((2, 2, 2, rows, LANES), dtype),
                pltpu.VMEM((2, 2, 2, rows, LANES), dtype),
                dma, dma((chunks,)),
                dma((4,)), dma, dma,
                dma, dma((2,)),
                dma, dma,
                dma((2,)), dma((2,)),
                dma, dma((chunks,)),
                dma, dma((2,)), dma, dma,
                dma, dma((2,)), dma, dma((chunks,)),
                dma((2,)), dma((2,)), dma((2,)), dma((2,)),
                dma((2,)), dma((2,)),
            ],
            compiler_params=pltpu.CompilerParams(collective_id=0, has_side_effects=True, vmem_limit_bytes=46 * 1024 * 1024),
        )(x_rows, norm_gain, w_q.reshape(depth, head), w_k, w_v)
        out = jax.ShapeDtypeStruct((tokens, head), dtype)
        q, k, v = pl.pallas_call(
            place,
            out_shape=(out, out, out),
            in_specs=[vmem, vmem],
            out_specs=(any_space, any_space, any_space),
            scratch_shapes=[dma((PLACE_BLOCKS, 2, 3))],
            compiler_params=pltpu.CompilerParams(vmem_limit_bytes=1024 * 1024),
        )(pltpu.with_memory_space_constraint(oq, pltpu.VMEM), pltpu.with_memory_space_constraint(okv, pltpu.VMEM))
        return q[:, None, :], k[:, None, :], v[:, None, :]

    return jax.shard_map(local_step, mesh=mesh, in_specs=(P(("dp", "tp"), None), P(None), P(None, "tp", None), P(None, "tp"), P(None, "tp")), out_specs=(P("dp", "tp", None), P("dp", "tp", None), P("dp", "tp", None)), check_vma=False)
```

```python
import functools

import jax
import jax.numpy as jnp
from jax import lax
from jax.experimental import pallas as pl
from jax.experimental.pallas import tpu as pltpu
from jax.sharding import PartitionSpec as P

EPSILON = 1e-6
LANES = 128
NORM_ROWS = 32
CHUNK = 128
OWN_ROWS = 256
PLACE_BLOCKS = 1
W_BLOCKS = 4
MESH = pl.DeviceIdType.MESH


def exchange(chips, x, gain, wq, wk, wv, oq, okv, gain_copy, gain_row, n, w, slq, srq, srkv, g_sem, x_sem, w0_sem, wl_sem, wl_s, wl_r, wx_s, wx_r, wg_s, wg_r, wd_s, wd_r, n_s, n_r,
             oq_s, oq_r, okv_s, okv_r, rq_s, rq_r, rkv_s, rkv_r, lq_s, lq_r, lkv_s, lkv_r, fk_s, fk_r):
    rows, depth = x.shape
    chunks = rows // CHUNK
    group = lax.axis_index("dp")
    device = lax.axis_index("tp")
    half = lax.rem(group, 2)
    core = lax.rem(device, 2)
    chip = lax.div(device, 2)
    token_chip = chips - 1 - chip
    weight_chip = chip + 1 - 2 * lax.rem(chip, 2)
    far_chip = chips - 1 - weight_chip
    other_core = 1 - core
    partner = {"tp": 2 * chip + other_core}
    token_peer = {"tp": 2 * token_chip + core}
    weight_peer = {"tp": 2 * weight_chip + core}
    group_peer = {"dp": group + 1 - 2 * half}

    def weight_core(c):
        return {"tp": 2 * weight_chip + c}

    def remote(src, dst, send, recv, to):
        return pltpu.make_async_remote_copy(src_ref=src, dst_ref=dst, send_sem=send, recv_sem=recv, device_id=to, device_id_type=MESH)

    def block(c, on_chip):
        return pl.multiple_of((2 * on_chip + c) * rows, rows)

    def chunk_of(j):
        return pl.ds(pl.multiple_of(j * CHUNK, CHUNK), CHUNK)

    def load_x(j):
        return pltpu.make_async_copy(x.at[chunk_of(j)], n.at[0, chunk_of(j)], x_sem.at[j])

    q_half = [wq.at[:, pl.ds(h * LANES, LANES)] for h in range(2)]
    kv = [wk, wv]

    def own_w_part(h, part):
        return w.at[0, h, core, :, pl.ds(part * LANES, LANES)]

    w_rows = depth // W_BLOCKS

    def at_rows(ref, r):
        return ref.at[pl.ds(r * w_rows, w_rows)]

    barrier = pltpu.get_barrier_semaphore()
    for peer in (partner, token_peer, weight_peer, weight_core(other_core), group_peer):
        pl.semaphore_signal(barrier, inc=1, device_id=peer, device_id_type=MESH)
    first = own_w_part(half, 0)
    first_src = wq.at[:, pl.ds(pl.multiple_of(half * LANES, LANES), LANES)]
    for r in range(W_BLOCKS):
        pltpu.make_async_copy(at_rows(first_src, r), at_rows(first, r), w0_sem.at[r]).start()
    second = own_w_part(1 - half, 0)
    pltpu.make_async_copy(wq.at[:, pl.ds(pl.multiple_of((1 - half) * LANES, LANES), LANES)], second, wl_sem.at[0]).start()
    for h in range(2):
        pltpu.make_async_copy(kv[h], own_w_part(h, 1), wl_sem.at[1 + h]).start()
    gain_load = pltpu.make_async_copy(gain, gain_copy, g_sem)
    gain_load.start()
    for j in range(chunks):
        load_x(j).start()
    pl.semaphore_wait(barrier, 5)

    w_parts = [w.at[1, half, core, :, pl.ds(part * LANES, LANES)] for part in range(2)]
    for r in range(W_BLOCKS):
        pltpu.make_async_copy(at_rows(first, r), at_rows(first, r), w0_sem.at[r]).wait()
        remote(at_rows(first, r), at_rows(w_parts[0], r), wx_s, wx_r.at[0, r], weight_peer).start()
    for h in range(2):
        @pl.when(half == h)
        def _():
            for r in range(W_BLOCKS):
                remote(at_rows(kv[h], r), at_rows(w_parts[1], r), wx_s, wx_r.at[1, r], weight_peer).start()
    for h in range(2):
        for part, src in enumerate((q_half[h], kv[h])):
            remote(src, own_w_part(h, part), wl_s, wl_r, partner).start()
    gain_load.wait()
    gain_row[...] = gain_copy[...].reshape(1, depth)

    def send_n(j):
        return remote(n.at[0, chunk_of(j)], n.at[1, chunk_of(j)], n_s, n_r.at[j], token_peer)

    @pl.loop(0, chunks)
    def _(j):
        load_x(j).wait()

        @pl.loop(0, CHUNK // NORM_ROWS)
        def _(i):
            at = pl.ds(pl.multiple_of(j * CHUNK + i * NORM_ROWS, NORM_ROWS), NORM_ROWS)
            wide = n[0, at, :].astype(jnp.float32)
            mean_sq = jnp.mean(wide * wide, axis=-1, keepdims=True)
            n[0, at, :] = (wide * lax.rsqrt(mean_sq + EPSILON) * gain_row[...]).astype(jnp.bfloat16)

        send_n(j).start()

    def product(blk, at, side, h, c):
        return jnp.dot(n[blk, at, :], w[side, h, c], preferred_element_type=jnp.float32).astype(jnp.bfloat16)

    def local_products(blk, base, start, size):
        at = pl.ds(start, size)
        out = pl.ds(pl.multiple_of(base + start, size), size)

        @pl.loop(0, 2)
        def _(h):
            for b in range(2):
                c = lax.rem(core + b, 2)
                both = product(blk, at, 0, h, c)
                if b == 0:
                    oq[h, out, :] = both[:, :LANES]
                else:
                    slq[blk, h, at, :] = both[:, :LANES]
                okv[h, c, out, :] = both[:, LANES:]
        remote(slq.at[blk, :, at], oq.at[:, out], lq_s.at[blk], lq_r.at[blk], partner).start()
        remote(okv.at[:, :, out], okv.at[:, :, out], lkv_s.at[blk], lkv_r.at[blk], partner).start()

    own = block(core, chip)
    near = block(core, token_chip)

    own_w = w.at[0, :, core]
    pltpu.make_async_copy(second, second, wl_sem.at[0]).wait()
    for h in range(2):
        pltpu.make_async_copy(kv[h], own_w_part(h, 1), wl_sem.at[1 + h]).wait()
    other_w = w.at[0, :, other_core]
    remote(other_w, other_w, wl_s, wl_r, partner).wait_recv()

    def own_part(h, c, part):
        @pl.loop(0, rows // OWN_ROWS)
        def _(i):
            at = pl.ds(pl.multiple_of(i * OWN_ROWS, OWN_ROWS), OWN_ROWS)
            piece = w[1, h, c, :, part * LANES:(part + 1) * LANES]
            value = jnp.dot(n[0, at, :], piece, preferred_element_type=jnp.float32).astype(jnp.bfloat16)
            if part == 0:
                srq[0, c, h, at, :] = value
            else:
                srkv[0, h, c, at, :] = value

    def send_own(h, c, part):
        out = pl.ds(own, rows)
        if part == 0:
            remote(srq.at[0, c, h], oq.at[h, out], oq_s, oq_r.at[core], weight_core(c)).start()
        else:
            remote(srkv.at[0, h, c], okv.at[h, c, out], okv_s, okv_r, weight_peer).start()

    local_chunks = rows // OWN_ROWS
    steps = 2 * W_BLOCKS
    for step in range(steps):
        part, r = divmod(step, W_BLOCKS)
        piece = at_rows(w_parts[part], r)
        remote(piece, piece, wx_s, wx_r.at[part, r], weight_peer).wait_recv()
        remote(piece, piece, wg_s, wg_r, group_peer).start()
        remote(piece, piece, wd_s.at[0], wd_r.at[0], partner).start()
        if r == W_BLOCKS - 1:
            own_part(half, core, part)
            send_own(half, core, part)
        for i in range(step * local_chunks // steps, (step + 1) * local_chunks // steps):
            local_products(0, own, i * OWN_ROWS, OWN_ROWS)

    def own_products(h, c):
        @pl.loop(0, rows // OWN_ROWS)
        def _(i):
            at = pl.ds(pl.multiple_of(i * OWN_ROWS, OWN_ROWS), OWN_ROWS)
            both = product(0, at, 1, h, c)
            srq[0, c, h, at, :] = both[:, :LANES]
            srkv[0, h, c, at, :] = both[:, LANES:]
        for part in range(2):
            send_own(h, c, part)

    other_half = 1 - half
    from_partner = w.at[1, half, other_core]
    remote(from_partner, from_partner, wd_s.at[0], wd_r.at[0], partner).wait_recv()
    own_products(half, other_core)
    from_group = w.at[1, other_half, core]
    remote(from_group, from_group, wg_s, wg_r, group_peer).wait_recv()
    remote(from_group, from_group, wd_s.at[1], wd_r.at[1], partner).start()
    own_products(other_half, core)
    from_both = w.at[1, other_half, other_core]
    remote(from_both, from_both, wd_s.at[1], wd_r.at[1], partner).wait_recv()
    own_products(other_half, other_core)

    @pl.loop(0, chunks)
    def _(j):
        send_n(j).wait_recv()
        start = pl.multiple_of(j * CHUNK, CHUNK)
        at = pl.ds(start, CHUNK)
        out = pl.ds(pl.multiple_of(near + start, CHUNK), CHUNK)

        @pl.loop(0, 2)
        def _(h):
            for c in range(2):
                both = product(1, at, 1, h, c)
                srq[1, c, h, at, :] = both[:, :LANES]
                srkv[1, h, c, at, :] = both[:, LANES:]
        remote(srkv.at[1, :, :, at], okv.at[:, :, out], rkv_s, rkv_r.at[j], weight_peer).start()
        for c in range(2):
            remote(srq.at[1, c, :, at], oq.at[:, out], rq_s, rq_r.at[core], weight_core(c)).start()
        local_products(1, near, start, CHUNK)

    beside = pl.ds(block(core, weight_chip), rows)
    arrived = okv.at[:, :, beside]
    remote(arrived, arrived, okv_s, okv_r, weight_peer).wait_recv()
    remote(arrived, arrived, fk_s.at[0], fk_r.at[0], partner).start()
    far = block(core, far_chip)

    @pl.loop(0, chunks)
    def _(j):
        piece = okv.at[:, :, pl.ds(pl.multiple_of(far + j * CHUNK, CHUNK), CHUNK)]
        remote(piece, piece, rkv_s, rkv_r.at[j], weight_peer).wait_recv()
        remote(piece, piece, fk_s.at[1], fk_r.at[1], partner).start()

    def all_q(c, on_chip):
        return oq.at[:, pl.ds(block(c, on_chip), rows)]

    def all_kv(c, on_chip):
        return okv.at[:, :, pl.ds(block(c, on_chip), rows)]

    for c in range(2):
        remote(all_q(c, weight_chip), all_q(c, weight_chip), oq_s, oq_r.at[c], weight_peer).wait_recv()
        remote(all_q(c, far_chip), all_q(c, far_chip), rq_s, rq_r.at[c], weight_peer).wait_recv()
    for i, on_chip in enumerate((chip, token_chip)):
        remote(all_q(other_core, on_chip), all_q(other_core, on_chip), lq_s.at[i], lq_r.at[i], partner).wait_recv()
        remote(all_kv(other_core, on_chip), all_kv(other_core, on_chip), lkv_s.at[i], lkv_r.at[i], partner).wait_recv()
    for i, on_chip in enumerate((weight_chip, far_chip)):
        remote(all_kv(other_core, on_chip), all_kv(other_core, on_chip), fk_s.at[i], fk_r.at[i], partner).wait_recv()

    def sent(ref, sem):
        remote(ref, ref, sem, n_r.at[0], partner).wait_send()

    sent(own_w, wl_s)
    sent(w.at[1, 0, 0], wx_s)
    sent(w.at[1, 0, 0], wg_s)
    for i in range(2):
        sent(w.at[1, 0, 0], wd_s.at[i])
        sent(slq.at[i], lq_s.at[i])
        sent(srkv.at[0], lkv_s.at[i])
        sent(srkv.at[0], fk_s.at[i])
    sent(n.at[0], n_s)
    sent(srq.at[0], oq_s)
    sent(srkv.at[0], okv_s)
    sent(srq.at[1], rq_s)
    sent(srkv.at[1], rkv_s)


def place(oq, okv, q, k, v, sems):
    rows = oq.shape[1] // PLACE_BLOCKS
    copies = []
    for i in range(PLACE_BLOCKS):
        at = pl.ds(i * rows, rows)
        for h in range(2):
            cols = pl.ds(h * LANES, LANES)
            for a, (src, dst) in enumerate(((oq, q), (okv.at[0], k), (okv.at[1], v))):
                copies.append(pltpu.make_async_copy(src.at[h, at], dst.at[at, cols], sems.at[i, h, a]))
    for copy in copies:
        copy.start()
    for copy in copies:
        copy.wait()


def solution(mesh):
    group_size = mesh.shape["tp"]
    chips = group_size // 2

    def local_step(x_rows, norm_gain, w_q, w_k, w_v):
        rows, depth = x_rows.shape
        head = w_q.shape[2]
        tokens = rows * group_size
        dtype = x_rows.dtype
        any_space = pl.BlockSpec(memory_space=pl.ANY)
        vmem = pl.BlockSpec(memory_space=pltpu.VMEM)
        dma = pltpu.SemaphoreType.DMA
        chunks = rows // CHUNK
        oq, okv = pl.pallas_call(
            functools.partial(exchange, chips),
            out_shape=(pltpu.VMEM((2, tokens, LANES), dtype), pltpu.VMEM((2, 2, tokens, LANES), dtype)),
            in_specs=[any_space] * 5,
            out_specs=(vmem, vmem),
            scratch_shapes=[
                pltpu.VMEM((depth,), norm_gain.dtype),
                pltpu.VMEM((1, depth), norm_gain.dtype),
                pltpu.VMEM((2, rows, depth), dtype),
                pltpu.VMEM((2, 2, 2, depth, 2 * LANES), dtype),
                pltpu.VMEM((2, 2, rows, LANES), dtype),
                pltpu.VMEM((2, 2, 2, rows, LANES), dtype),
                pltpu.VMEM((2, 2, 2, rows, LANES), dtype),
                dma, dma((chunks,)),
                dma((W_BLOCKS,)), dma((3,)), dma, dma,
                dma, dma((2, W_BLOCKS)),
                dma, dma,
                dma((2,)), dma((2,)),
                dma, dma((chunks,)),
                dma, dma((2,)), dma, dma,
                dma, dma((2,)), dma, dma((chunks,)),
                dma((2,)), dma((2,)), dma((2,)), dma((2,)),
                dma((2,)), dma((2,)),
            ],
            compiler_params=pltpu.CompilerParams(collective_id=0, has_side_effects=True, vmem_limit_bytes=46 * 1024 * 1024),
        )(x_rows, norm_gain, w_q.reshape(depth, head), w_k, w_v)
        out = jax.ShapeDtypeStruct((tokens, head), dtype)
        q, k, v = pl.pallas_call(
            place,
            out_shape=(out, out, out),
            in_specs=[vmem, vmem],
            out_specs=(any_space, any_space, any_space),
            scratch_shapes=[dma((PLACE_BLOCKS, 2, 3))],
            compiler_params=pltpu.CompilerParams(vmem_limit_bytes=1024 * 1024),
        )(pltpu.with_memory_space_constraint(oq, pltpu.VMEM), pltpu.with_memory_space_constraint(okv, pltpu.VMEM))
        return q[:, None, :], k[:, None, :], v[:, None, :]

    return jax.shard_map(local_step, mesh=mesh, in_specs=(P(("dp", "tp"), None), P(None), P(None, "tp", None), P(None, "tp"), P(None, "tp")), out_specs=(P("dp", "tp", None), P("dp", "tp", None), P("dp", "tp", None)), check_vma=False)
```

```python
import functools

import jax
import jax.numpy as jnp
from jax import lax
from jax.experimental import pallas as pl
from jax.experimental.pallas import tpu as pltpu
from jax.sharding import PartitionSpec as P

EPSILON = 1e-6
LANES = 128
NORM_ROWS = 32
CHUNK = 128
OWN_ROWS = 256
PLACE_BLOCKS = 2
W_BLOCKS = 2
MESH = pl.DeviceIdType.MESH


def exchange(chips, x, gain, wq, wk, wv, oq, okv, gain_copy, gain_row, n, w, slq, srq, srkv, g_sem, x_sem, w0_sem, wl_sem, wl_s, wl_r, wx_s, wx_r, wg_s, wg_r, wd_s, wd_r, n_s, n_r,
             oq_s, oq_r, okv_s, okv_r, rq_s, rq_r, rkv_s, rkv_r, lq_s, lq_r, lkv_s, lkv_r, fk_s, fk_r):
    rows, depth = x.shape
    chunks = rows // CHUNK
    group = lax.axis_index("dp")
    device = lax.axis_index("tp")
    half = lax.rem(group, 2)
    core = lax.rem(device, 2)
    chip = lax.div(device, 2)
    token_chip = chips - 1 - chip
    weight_chip = chip + 1 - 2 * lax.rem(chip, 2)
    far_chip = chips - 1 - weight_chip
    other_core = 1 - core
    partner = {"tp": 2 * chip + other_core}
    token_peer = {"tp": 2 * token_chip + core}
    weight_peer = {"tp": 2 * weight_chip + core}
    group_peer = {"dp": group + 1 - 2 * half}

    def lanes(i):
        return pl.ds(pl.multiple_of(i * LANES, LANES), LANES)

    def weight_core(c):
        return {"tp": 2 * weight_chip + c}

    def remote(src, dst, send, recv, to):
        return pltpu.make_async_remote_copy(src_ref=src, dst_ref=dst, send_sem=send, recv_sem=recv, device_id=to, device_id_type=MESH)

    def block(c, on_chip):
        return pl.multiple_of((2 * on_chip + c) * rows, rows)

    def chunk_of(j):
        return pl.ds(pl.multiple_of(j * CHUNK, CHUNK), CHUNK)

    def load_x(j):
        return pltpu.make_async_copy(x.at[chunk_of(j)], n.at[0, chunk_of(j)], x_sem.at[j])

    q_half = [wq.at[:, pl.ds(h * LANES, LANES)] for h in range(2)]
    kv = [wk, wv]

    def own_w_part(h, part):
        return w.at[0, h, core, :, pl.ds(part * LANES, LANES)]

    w_rows = depth // W_BLOCKS

    def at_rows(ref, r):
        return ref.at[pl.ds(r * w_rows, w_rows)]

    barrier = pltpu.get_barrier_semaphore()
    for peer in (partner, token_peer, weight_peer, weight_core(other_core), group_peer):
        pl.semaphore_signal(barrier, inc=1, device_id=peer, device_id_type=MESH)
    first = own_w_part(half, 0)
    first_src = wq.at[:, pl.ds(pl.multiple_of(half * LANES, LANES), LANES)]
    for r in range(W_BLOCKS):
        pltpu.make_async_copy(at_rows(first_src, r), at_rows(first, r), w0_sem.at[r]).start()
    second = own_w_part(1 - half, 0)
    pltpu.make_async_copy(wq.at[:, pl.ds(pl.multiple_of((1 - half) * LANES, LANES), LANES)], second, wl_sem.at[0]).start()
    for h in range(2):
        pltpu.make_async_copy(kv[h], own_w_part(h, 1), wl_sem.at[1 + h]).start()
    gain_load = pltpu.make_async_copy(gain, gain_copy, g_sem)
    gain_load.start()
    for j in range(chunks):
        load_x(j).start()
    pl.semaphore_wait(barrier, 5)

    w_parts = [w.at[1, half, core, :, pl.ds(part * LANES, LANES)] for part in range(2)]
    for r in range(W_BLOCKS):
        pltpu.make_async_copy(at_rows(first, r), at_rows(first, r), w0_sem.at[r]).wait()
        remote(at_rows(first, r), at_rows(w_parts[0], r), wx_s, wx_r.at[0, r], weight_peer).start()
    for h in range(2):
        @pl.when(half == h)
        def _():
            for r in range(W_BLOCKS):
                remote(at_rows(kv[h], r), at_rows(w_parts[1], r), wx_s, wx_r.at[1, r], weight_peer).start()
    for h in range(2):
        for part, src in enumerate((q_half[h], kv[h])):
            remote(src, own_w_part(h, part), wl_s, wl_r, partner).start()
    gain_load.wait()
    gain_row[...] = gain_copy[...].reshape(1, depth)

    def send_n(j):
        return remote(n.at[0, chunk_of(j)], n.at[1, chunk_of(j)], n_s, n_r.at[j], token_peer)

    @pl.loop(0, chunks)
    def _(j):
        load_x(j).wait()

        @pl.loop(0, CHUNK // NORM_ROWS)
        def _(i):
            at = pl.ds(pl.multiple_of(j * CHUNK + i * NORM_ROWS, NORM_ROWS), NORM_ROWS)
            wide = n[0, at, :].astype(jnp.float32)
            mean_sq = jnp.mean(wide * wide, axis=-1, keepdims=True)
            n[0, at, :] = (wide * lax.rsqrt(mean_sq + EPSILON) * gain_row[...]).astype(jnp.bfloat16)

        send_n(j).start()

    def product(blk, at, side, h, c):
        return jnp.dot(n[blk, at, :], w[side, h, c], preferred_element_type=jnp.float32).astype(jnp.bfloat16)

    def local_products(blk, base, start, size):
        at = pl.ds(start, size)
        out = pl.ds(pl.multiple_of(base + start, size), size)

        @pl.loop(0, 2)
        def _(h):
            for b in range(2):
                c = lax.rem(core + b, 2)
                both = product(blk, at, 0, h, c)
                if b == 0:
                    oq[out, lanes(h)] = both[:, :LANES]
                else:
                    slq[blk, at, lanes(h)] = both[:, :LANES]
                okv[h, out, lanes(c)] = both[:, LANES:]
        remote(slq.at[blk, at], oq.at[out], lq_s.at[blk], lq_r.at[blk], partner).start()
        remote(okv.at[:, out], okv.at[:, out], lkv_s.at[blk], lkv_r.at[blk], partner).start()

    own = block(core, chip)
    near = block(core, token_chip)

    own_w = w.at[0, :, core]
    pltpu.make_async_copy(second, second, wl_sem.at[0]).wait()
    for h in range(2):
        pltpu.make_async_copy(kv[h], own_w_part(h, 1), wl_sem.at[1 + h]).wait()
    other_w = w.at[0, :, other_core]
    remote(other_w, other_w, wl_s, wl_r, partner).wait_recv()

    def own_part(h, c, part):
        @pl.loop(0, rows // OWN_ROWS)
        def _(i):
            at = pl.ds(pl.multiple_of(i * OWN_ROWS, OWN_ROWS), OWN_ROWS)
            piece = w[1, h, c, :, part * LANES:(part + 1) * LANES]
            value = jnp.dot(n[0, at, :], piece, preferred_element_type=jnp.float32).astype(jnp.bfloat16)
            if part == 0:
                srq[0, c, at, lanes(h)] = value
            else:
                srkv[0, h, at, lanes(c)] = value

    def send_own(h, c, part):
        out = pl.ds(own, rows)
        if part == 0:
            remote(srq.at[0, c, :, lanes(h)], oq.at[out, lanes(h)], oq_s, oq_r.at[core], weight_core(c)).start()
        else:
            remote(srkv.at[0, h, :, lanes(c)], okv.at[h, out, lanes(c)], okv_s, okv_r, weight_peer).start()

    local_chunks = rows // OWN_ROWS
    steps = 2 * W_BLOCKS
    for step in range(steps):
        part, r = divmod(step, W_BLOCKS)
        piece = at_rows(w_parts[part], r)
        remote(piece, piece, wx_s, wx_r.at[part, r], weight_peer).wait_recv()
        remote(piece, piece, wg_s, wg_r, group_peer).start()
        remote(piece, piece, wd_s.at[0], wd_r.at[0], partner).start()
        if r == W_BLOCKS - 1:
            own_part(half, core, part)
            send_own(half, core, part)
        for i in range(step * local_chunks // steps, (step + 1) * local_chunks // steps):
            local_products(0, own, i * OWN_ROWS, OWN_ROWS)

    def own_products(h, c):
        @pl.loop(0, rows // OWN_ROWS)
        def _(i):
            at = pl.ds(pl.multiple_of(i * OWN_ROWS, OWN_ROWS), OWN_ROWS)
            both = product(0, at, 1, h, c)
            srq[0, c, at, lanes(h)] = both[:, :LANES]
            srkv[0, h, at, lanes(c)] = both[:, LANES:]
        for part in range(2):
            send_own(h, c, part)

    other_half = 1 - half
    from_partner = w.at[1, half, other_core]
    remote(from_partner, from_partner, wd_s.at[0], wd_r.at[0], partner).wait_recv()
    own_products(half, other_core)
    from_group = w.at[1, other_half, core]
    remote(from_group, from_group, wg_s, wg_r, group_peer).wait_recv()
    remote(from_group, from_group, wd_s.at[1], wd_r.at[1], partner).start()
    own_products(other_half, core)
    from_both = w.at[1, other_half, other_core]
    remote(from_both, from_both, wd_s.at[1], wd_r.at[1], partner).wait_recv()
    own_products(other_half, other_core)

    @pl.loop(0, chunks)
    def _(j):
        send_n(j).wait_recv()
        start = pl.multiple_of(j * CHUNK, CHUNK)
        at = pl.ds(start, CHUNK)
        out = pl.ds(pl.multiple_of(near + start, CHUNK), CHUNK)

        @pl.loop(0, 2)
        def _(h):
            for c in range(2):
                both = product(1, at, 1, h, c)
                srq[1, c, at, lanes(h)] = both[:, :LANES]
                srkv[1, h, at, lanes(c)] = both[:, LANES:]
        remote(srkv.at[1, :, at], okv.at[:, out], rkv_s, rkv_r.at[j], weight_peer).start()
        for c in range(2):
            remote(srq.at[1, c, at], oq.at[out], rq_s, rq_r.at[core], weight_core(c)).start()
        local_products(1, near, start, CHUNK)

    beside = pl.ds(block(core, weight_chip), rows)
    arrived = okv.at[:, beside]
    remote(arrived, arrived, okv_s, okv_r, weight_peer).wait_recv()
    remote(arrived, arrived, fk_s.at[0], fk_r.at[0], partner).start()
    far = block(core, far_chip)

    @pl.loop(0, chunks)
    def _(j):
        piece = okv.at[:, pl.ds(pl.multiple_of(far + j * CHUNK, CHUNK), CHUNK)]
        remote(piece, piece, rkv_s, rkv_r.at[j], weight_peer).wait_recv()
        remote(piece, piece, fk_s.at[1], fk_r.at[1], partner).start()

    def all_q(c, on_chip):
        return oq.at[pl.ds(block(c, on_chip), rows)]

    def all_kv(c, on_chip):
        return okv.at[:, pl.ds(block(c, on_chip), rows)]

    for c in range(2):
        remote(all_q(c, weight_chip), all_q(c, weight_chip), oq_s, oq_r.at[c], weight_peer).wait_recv()
        remote(all_q(c, far_chip), all_q(c, far_chip), rq_s, rq_r.at[c], weight_peer).wait_recv()
    for i, on_chip in enumerate((chip, token_chip)):
        remote(all_q(other_core, on_chip), all_q(other_core, on_chip), lq_s.at[i], lq_r.at[i], partner).wait_recv()
        remote(all_kv(other_core, on_chip), all_kv(other_core, on_chip), lkv_s.at[i], lkv_r.at[i], partner).wait_recv()
    for i, on_chip in enumerate((weight_chip, far_chip)):
        remote(all_kv(other_core, on_chip), all_kv(other_core, on_chip), fk_s.at[i], fk_r.at[i], partner).wait_recv()

    def sent(ref, sem):
        remote(ref, ref, sem, n_r.at[0], partner).wait_send()

    sent(own_w, wl_s)
    sent(w.at[1, 0, 0], wx_s)
    sent(w.at[1, 0, 0], wg_s)
    for i in range(2):
        sent(w.at[1, 0, 0], wd_s.at[i])
        sent(slq.at[i], lq_s.at[i])
        sent(srkv.at[0], lkv_s.at[i])
        sent(srkv.at[0], fk_s.at[i])
    sent(n.at[0], n_s)
    sent(srq.at[0], oq_s)
    sent(srkv.at[0], okv_s)
    sent(srq.at[1], rq_s)
    sent(srkv.at[1], rkv_s)


def place(oq, okv, q, k, v, sems):
    rows = oq.shape[0] // PLACE_BLOCKS
    copies = []
    for i in range(PLACE_BLOCKS):
        at = pl.ds(i * rows, rows)
        for a, (src, dst) in enumerate(((oq, q), (okv.at[0], k), (okv.at[1], v))):
            copies.append(pltpu.make_async_copy(src.at[at], dst.at[at], sems.at[i, a]))
    for copy in copies:
        copy.start()
    for copy in copies:
        copy.wait()


def solution(mesh):
    group_size = mesh.shape["tp"]
    chips = group_size // 2

    def local_step(x_rows, norm_gain, w_q, w_k, w_v):
        rows, depth = x_rows.shape
        head = w_q.shape[2]
        tokens = rows * group_size
        dtype = x_rows.dtype
        any_space = pl.BlockSpec(memory_space=pl.ANY)
        vmem = pl.BlockSpec(memory_space=pltpu.VMEM)
        dma = pltpu.SemaphoreType.DMA
        chunks = rows // CHUNK
        oq, okv = pl.pallas_call(
            functools.partial(exchange, chips),
            out_shape=(pltpu.VMEM((tokens, head), dtype), pltpu.VMEM((2, tokens, head), dtype)),
            in_specs=[any_space] * 5,
            out_specs=(vmem, vmem),
            scratch_shapes=[
                pltpu.VMEM((depth,), norm_gain.dtype),
                pltpu.VMEM((1, depth), norm_gain.dtype),
                pltpu.VMEM((2, rows, depth), dtype),
                pltpu.VMEM((2, 2, 2, depth, 2 * LANES), dtype),
                pltpu.VMEM((2, rows, head), dtype),
                pltpu.VMEM((2, 2, rows, head), dtype),
                pltpu.VMEM((2, 2, rows, head), dtype),
                dma, dma((chunks,)),
                dma((W_BLOCKS,)), dma((3,)), dma, dma,
                dma, dma((2, W_BLOCKS)),
                dma, dma,
                dma((2,)), dma((2,)),
                dma, dma((chunks,)),
                dma, dma((2,)), dma, dma,
                dma, dma((2,)), dma, dma((chunks,)),
                dma((2,)), dma((2,)), dma((2,)), dma((2,)),
                dma((2,)), dma((2,)),
            ],
            compiler_params=pltpu.CompilerParams(collective_id=0, has_side_effects=True, vmem_limit_bytes=46 * 1024 * 1024),
        )(x_rows, norm_gain, w_q.reshape(depth, head), w_k, w_v)
        out = jax.ShapeDtypeStruct((tokens, head), dtype)
        q, k, v = pl.pallas_call(
            place,
            out_shape=(out, out, out),
            in_specs=[vmem, vmem],
            out_specs=(any_space, any_space, any_space),
            scratch_shapes=[dma((PLACE_BLOCKS, 3))],
            compiler_params=pltpu.CompilerParams(vmem_limit_bytes=1024 * 1024),
        )(pltpu.with_memory_space_constraint(oq, pltpu.VMEM), pltpu.with_memory_space_constraint(okv, pltpu.VMEM))
        return q[:, None, :], k[:, None, :], v[:, None, :]

    return jax.shard_map(local_step, mesh=mesh, in_specs=(P(("dp", "tp"), None), P(None), P(None, "tp", None), P(None, "tp"), P(None, "tp")), out_specs=(P("dp", "tp", None), P("dp", "tp", None), P("dp", "tp", None)), check_vma=False)
```

```python
import functools

import jax
import jax.numpy as jnp
from jax import lax
from jax.experimental import pallas as pl
from jax.experimental.pallas import tpu as pltpu
from jax.sharding import PartitionSpec as P

EPSILON = 1e-6
LANES = 128
NORM_ROWS = 32
CHUNK = 128
OWN_ROWS = 256
PLACE_BLOCKS = 2
W_BLOCKS = 2
W_FIRST = 256
MESH = pl.DeviceIdType.MESH


def exchange(chips, x, gain, wq, wk, wv, oq, okv, gain_copy, gain_row, n, w, slq, srq, srkv, g_sem, x_sem, w0_sem, wl_sem, wl_s, wl_r, wx_s, wx_r, wg_s, wg_r, wd_s, wd_r, n_s, n_r,
             oq_s, oq_r, okv_s, okv_r, rq_s, rq_r, rkv_s, rkv_r, lq_s, lq_r, lkv_s, lkv_r, fk_s, fk_r):
    rows, depth = x.shape
    chunks = rows // CHUNK
    group = lax.axis_index("dp")
    device = lax.axis_index("tp")
    half = lax.rem(group, 2)
    core = lax.rem(device, 2)
    chip = lax.div(device, 2)
    token_chip = chips - 1 - chip
    weight_chip = chip + 1 - 2 * lax.rem(chip, 2)
    far_chip = chips - 1 - weight_chip
    other_core = 1 - core
    partner = {"tp": 2 * chip + other_core}
    token_peer = {"tp": 2 * token_chip + core}
    weight_peer = {"tp": 2 * weight_chip + core}
    group_peer = {"dp": group + 1 - 2 * half}

    def lanes(i):
        return pl.ds(pl.multiple_of(i * LANES, LANES), LANES)

    def weight_core(c):
        return {"tp": 2 * weight_chip + c}

    def remote(src, dst, send, recv, to):
        return pltpu.make_async_remote_copy(src_ref=src, dst_ref=dst, send_sem=send, recv_sem=recv, device_id=to, device_id_type=MESH)

    def block(c, on_chip):
        return pl.multiple_of((2 * on_chip + c) * rows, rows)

    def chunk_of(j):
        return pl.ds(pl.multiple_of(j * CHUNK, CHUNK), CHUNK)

    def load_x(j):
        return pltpu.make_async_copy(x.at[chunk_of(j)], n.at[0, chunk_of(j)], x_sem.at[j])

    q_half = [wq.at[:, pl.ds(h * LANES, LANES)] for h in range(2)]
    kv = [wk, wv]

    def own_w_part(h, part):
        return w.at[0, h, core, :, pl.ds(part * LANES, LANES)]

    cuts = ((0, W_FIRST, depth), (0, depth // 2, depth))

    def at_rows(ref, part, r):
        return ref.at[pl.ds(cuts[part][r], cuts[part][r + 1] - cuts[part][r])]

    barrier = pltpu.get_barrier_semaphore()

    def greet(peers):
        for peer in peers:
            pl.semaphore_signal(barrier, inc=1, device_id=peer, device_id_type=MESH)

    greet((partner, weight_peer, weight_core(other_core)))
    follows = lax.div(2 * chip, chips) + half
    first = own_w_part(half, 0)
    first_src = wq.at[:, pl.ds(pl.multiple_of(half * LANES, LANES), LANES)]
    for r in range(W_BLOCKS):
        pltpu.make_async_copy(at_rows(first_src, 0, r), at_rows(first, 0, r), w0_sem.at[r]).start()
    second = own_w_part(1 - half, 0)
    pltpu.make_async_copy(wq.at[:, pl.ds(pl.multiple_of((1 - half) * LANES, LANES), LANES)], second, wl_sem.at[0]).start()
    for h in range(2):
        pltpu.make_async_copy(kv[h], own_w_part(h, 1), wl_sem.at[1 + h]).start()
    gain_load = pltpu.make_async_copy(gain, gain_copy, g_sem)
    gain_load.start()
    for j in range(chunks):
        load_x(j).start()
    pl.semaphore_wait(barrier, 3 + follows)
    greet((token_peer, group_peer))

    w_parts = [w.at[1, half, core, :, pl.ds(part * LANES, LANES)] for part in range(2)]
    for r in range(W_BLOCKS):
        pltpu.make_async_copy(at_rows(first, 0, r), at_rows(first, 0, r), w0_sem.at[r]).wait()
        remote(at_rows(first, 0, r), at_rows(w_parts[0], 0, r), wx_s, wx_r.at[0, r], weight_peer).start()
    for h in range(2):
        @pl.when(half == h)
        def _():
            for r in range(W_BLOCKS):
                remote(at_rows(kv[h], 1, r), at_rows(w_parts[1], 1, r), wx_s, wx_r.at[1, r], weight_peer).start()
    for h in range(2):
        for part, src in enumerate((q_half[h], kv[h])):
            remote(src, own_w_part(h, part), wl_s, wl_r, partner).start()
    gain_load.wait()
    gain_row[...] = gain_copy[...].reshape(1, depth)

    def send_n(j):
        return remote(n.at[0, chunk_of(j)], n.at[1, chunk_of(j)], n_s, n_r.at[j], token_peer)

    @pl.loop(0, chunks)
    def _(j):
        load_x(j).wait()

        @pl.loop(0, CHUNK // NORM_ROWS)
        def _(i):
            at = pl.ds(pl.multiple_of(j * CHUNK + i * NORM_ROWS, NORM_ROWS), NORM_ROWS)
            wide = n[0, at, :].astype(jnp.float32)
            mean_sq = jnp.mean(wide * wide, axis=-1, keepdims=True)
            n[0, at, :] = (wide * lax.rsqrt(mean_sq + EPSILON) * gain_row[...]).astype(jnp.bfloat16)

        @pl.when(jnp.logical_and(j == 0, follows < 2))
        def _():
            pl.semaphore_wait(barrier, 2 - follows)

        send_n(j).start()

    def product(blk, at, side, h, c):
        return jnp.dot(n[blk, at, :], w[side, h, c], preferred_element_type=jnp.float32).astype(jnp.bfloat16)

    def local_products(blk, base, start, size):
        at = pl.ds(start, size)
        out = pl.ds(pl.multiple_of(base + start, size), size)

        @pl.loop(0, 2)
        def _(h):
            for b in range(2):
                c = lax.rem(core + b, 2)
                both = product(blk, at, 0, h, c)
                if b == 0:
                    oq[out, lanes(h)] = both[:, :LANES]
                else:
                    slq[blk, at, lanes(h)] = both[:, :LANES]
                okv[h, out, lanes(c)] = both[:, LANES:]
        remote(slq.at[blk, at], oq.at[out], lq_s.at[blk], lq_r.at[blk], partner).start()
        remote(okv.at[:, out], okv.at[:, out], lkv_s.at[blk], lkv_r.at[blk], partner).start()

    own = block(core, chip)
    near = block(core, token_chip)

    own_w = w.at[0, :, core]
    pltpu.make_async_copy(second, second, wl_sem.at[0]).wait()
    for h in range(2):
        pltpu.make_async_copy(kv[h], own_w_part(h, 1), wl_sem.at[1 + h]).wait()
    other_w = w.at[0, :, other_core]
    remote(other_w, other_w, wl_s, wl_r, partner).wait_recv()

    def own_part(h, c, part):
        @pl.loop(0, rows // OWN_ROWS)
        def _(i):
            at = pl.ds(pl.multiple_of(i * OWN_ROWS, OWN_ROWS), OWN_ROWS)
            piece = w[1, h, c, :, part * LANES:(part + 1) * LANES]
            value = jnp.dot(n[0, at, :], piece, preferred_element_type=jnp.float32).astype(jnp.bfloat16)
            if part == 0:
                srq[0, c, at, lanes(h)] = value
            else:
                srkv[0, h, at, lanes(c)] = value

    def send_own(h, c, part):
        out = pl.ds(own, rows)
        if part == 0:
            remote(srq.at[0, c, :, lanes(h)], oq.at[out, lanes(h)], oq_s, oq_r.at[core], weight_core(c)).start()
        else:
            remote(srkv.at[0, h, :, lanes(c)], okv.at[h, out, lanes(c)], okv_s, okv_r, weight_peer).start()

    local_chunks = rows // OWN_ROWS
    steps = 2 * W_BLOCKS
    for step in range(steps):
        part, r = divmod(step, W_BLOCKS)
        piece = at_rows(w_parts[part], part, r)
        remote(piece, piece, wx_s, wx_r.at[part, r], weight_peer).wait_recv()
        remote(piece, piece, wg_s, wg_r, group_peer).start()
        remote(piece, piece, wd_s.at[0], wd_r.at[0], partner).start()
        if r == W_BLOCKS - 1:
            own_part(half, core, part)
            send_own(half, core, part)
        for i in range(step * local_chunks // steps, (step + 1) * local_chunks // steps):
            local_products(0, own, i * OWN_ROWS, OWN_ROWS)

    def own_products(h, c):
        @pl.loop(0, rows // OWN_ROWS)
        def _(i):
            at = pl.ds(pl.multiple_of(i * OWN_ROWS, OWN_ROWS), OWN_ROWS)
            both = product(0, at, 1, h, c)
            srq[0, c, at, lanes(h)] = both[:, :LANES]
            srkv[0, h, at, lanes(c)] = both[:, LANES:]
        for part in range(2):
            send_own(h, c, part)

    other_half = 1 - half
    from_partner = w.at[1, half, other_core]
    remote(from_partner, from_partner, wd_s.at[0], wd_r.at[0], partner).wait_recv()
    own_products(half, other_core)
    from_group = w.at[1, other_half, core]
    remote(from_group, from_group, wg_s, wg_r, group_peer).wait_recv()
    remote(from_group, from_group, wd_s.at[1], wd_r.at[1], partner).start()
    own_products(other_half, core)
    from_both = w.at[1, other_half, other_core]
    remote(from_both, from_both, wd_s.at[1], wd_r.at[1], partner).wait_recv()
    own_products(other_half, other_core)

    @pl.loop(0, chunks)
    def _(j):
        send_n(j).wait_recv()
        start = pl.multiple_of(j * CHUNK, CHUNK)
        at = pl.ds(start, CHUNK)
        out = pl.ds(pl.multiple_of(near + start, CHUNK), CHUNK)

        @pl.loop(0, 2)
        def _(h):
            for c in range(2):
                both = product(1, at, 1, h, c)
                srq[1, c, at, lanes(h)] = both[:, :LANES]
                srkv[1, h, at, lanes(c)] = both[:, LANES:]
        remote(srkv.at[1, :, at], okv.at[:, out], rkv_s, rkv_r.at[j], weight_peer).start()
        for c in range(2):
            remote(srq.at[1, c, at], oq.at[out], rq_s, rq_r.at[core], weight_core(c)).start()
        local_products(1, near, start, CHUNK)

    beside = pl.ds(block(core, weight_chip), rows)
    arrived = okv.at[:, beside]
    remote(arrived, arrived, okv_s, okv_r, weight_peer).wait_recv()
    remote(arrived, arrived, fk_s.at[0], fk_r.at[0], partner).start()
    far = block(core, far_chip)

    @pl.loop(0, chunks)
    def _(j):
        piece = okv.at[:, pl.ds(pl.multiple_of(far + j * CHUNK, CHUNK), CHUNK)]
        remote(piece, piece, rkv_s, rkv_r.at[j], weight_peer).wait_recv()
        remote(piece, piece, fk_s.at[1], fk_r.at[1], partner).start()

    def all_q(c, on_chip):
        return oq.at[pl.ds(block(c, on_chip), rows)]

    def all_kv(c, on_chip):
        return okv.at[:, pl.ds(block(c, on_chip), rows)]

    for c in range(2):
        remote(all_q(c, weight_chip), all_q(c, weight_chip), oq_s, oq_r.at[c], weight_peer).wait_recv()
        remote(all_q(c, far_chip), all_q(c, far_chip), rq_s, rq_r.at[c], weight_peer).wait_recv()
    for i, on_chip in enumerate((chip, token_chip)):
        remote(all_q(other_core, on_chip), all_q(other_core, on_chip), lq_s.at[i], lq_r.at[i], partner).wait_recv()
        remote(all_kv(other_core, on_chip), all_kv(other_core, on_chip), lkv_s.at[i], lkv_r.at[i], partner).wait_recv()
    for i, on_chip in enumerate((weight_chip, far_chip)):
        remote(all_kv(other_core, on_chip), all_kv(other_core, on_chip), fk_s.at[i], fk_r.at[i], partner).wait_recv()

    def sent(ref, sem):
        remote(ref, ref, sem, n_r.at[0], partner).wait_send()

    sent(own_w, wl_s)
    sent(w.at[1, 0, 0], wx_s)
    sent(w.at[1, 0, 0], wg_s)
    for i in range(2):
        sent(w.at[1, 0, 0], wd_s.at[i])
        sent(slq.at[i], lq_s.at[i])
        sent(srkv.at[0], lkv_s.at[i])
        sent(srkv.at[0], fk_s.at[i])
    sent(n.at[0], n_s)
    sent(srq.at[0], oq_s)
    sent(srkv.at[0], okv_s)
    sent(srq.at[1], rq_s)
    sent(srkv.at[1], rkv_s)


def place(oq, okv, q, k, v, sems):
    rows = oq.shape[0] // PLACE_BLOCKS
    copies = []
    for i in range(PLACE_BLOCKS):
        at = pl.ds(i * rows, rows)
        for a, (src, dst) in enumerate(((oq, q), (okv.at[0], k), (okv.at[1], v))):
            copies.append(pltpu.make_async_copy(src.at[at], dst.at[at], sems.at[i, a]))
    for copy in copies:
        copy.start()
    for copy in copies:
        copy.wait()


def solution(mesh):
    group_size = mesh.shape["tp"]
    chips = group_size // 2

    def local_step(x_rows, norm_gain, w_q, w_k, w_v):
        rows, depth = x_rows.shape
        head = w_q.shape[2]
        tokens = rows * group_size
        dtype = x_rows.dtype
        any_space = pl.BlockSpec(memory_space=pl.ANY)
        vmem = pl.BlockSpec(memory_space=pltpu.VMEM)
        dma = pltpu.SemaphoreType.DMA
        chunks = rows // CHUNK
        oq, okv = pl.pallas_call(
            functools.partial(exchange, chips),
            out_shape=(pltpu.VMEM((tokens, head), dtype), pltpu.VMEM((2, tokens, head), dtype)),
            in_specs=[any_space] * 5,
            out_specs=(vmem, vmem),
            scratch_shapes=[
                pltpu.VMEM((depth,), norm_gain.dtype),
                pltpu.VMEM((1, depth), norm_gain.dtype),
                pltpu.VMEM((2, rows, depth), dtype),
                pltpu.VMEM((2, 2, 2, depth, 2 * LANES), dtype),
                pltpu.VMEM((2, rows, head), dtype),
                pltpu.VMEM((2, 2, rows, head), dtype),
                pltpu.VMEM((2, 2, rows, head), dtype),
                dma, dma((chunks,)),
                dma((W_BLOCKS,)), dma((3,)), dma, dma,
                dma, dma((2, W_BLOCKS)),
                dma, dma,
                dma((2,)), dma((2,)),
                dma, dma((chunks,)),
                dma, dma((2,)), dma, dma,
                dma, dma((2,)), dma, dma((chunks,)),
                dma((2,)), dma((2,)), dma((2,)), dma((2,)),
                dma((2,)), dma((2,)),
            ],
            compiler_params=pltpu.CompilerParams(collective_id=0, has_side_effects=True, vmem_limit_bytes=46 * 1024 * 1024),
        )(x_rows, norm_gain, w_q.reshape(depth, head), w_k, w_v)
        out = jax.ShapeDtypeStruct((tokens, head), dtype)
        q, k, v = pl.pallas_call(
            place,
            out_shape=(out, out, out),
            in_specs=[vmem, vmem],
            out_specs=(any_space, any_space, any_space),
            scratch_shapes=[dma((PLACE_BLOCKS, 3))],
            compiler_params=pltpu.CompilerParams(vmem_limit_bytes=1024 * 1024),
        )(pltpu.with_memory_space_constraint(oq, pltpu.VMEM), pltpu.with_memory_space_constraint(okv, pltpu.VMEM))
        return q[:, None, :], k[:, None, :], v[:, None, :]

    return jax.shard_map(local_step, mesh=mesh, in_specs=(P(("dp", "tp"), None), P(None), P(None, "tp", None), P(None, "tp"), P(None, "tp")), out_specs=(P("dp", "tp", None), P("dp", "tp", None), P("dp", "tp", None)), check_vma=False)
```

```python
import functools

import jax
import jax.numpy as jnp
from jax import lax
from jax.experimental import pallas as pl
from jax.experimental.pallas import tpu as pltpu
from jax.sharding import PartitionSpec as P

EPSILON = 1e-6
LANES = 128
NORM_ROWS = 32
CHUNK = 128
OWN_ROWS = 256
PLACE_BLOCKS = 1
W_BLOCKS = 2
W_FIRST = 256
MESH = pl.DeviceIdType.MESH


def exchange(chips, x, gain, wq, wk, wv, oq, okv, gain_copy, gain_row, n, w, slq, srq, srkv, g_sem, x_sem, w0_sem, wl_sem, wl_s, wl_r, wx_s, wx_r, wg_s, wg_r, wd_s, wd_r, n_s, n_r,
             oq_s, oq_r, okv_s, okv_r, rq_s, rq_r, rkv_s, rkv_r, lq_s, lq_r, lkv_s, lkv_r, fk_s, fk_r):
    rows, depth = x.shape
    chunks = rows // CHUNK
    group = lax.axis_index("dp")
    device = lax.axis_index("tp")
    half = lax.rem(group, 2)
    core = lax.rem(device, 2)
    chip = lax.div(device, 2)
    token_chip = chips - 1 - chip
    weight_chip = chip + 1 - 2 * lax.rem(chip, 2)
    far_chip = chips - 1 - weight_chip
    other_core = 1 - core
    partner = {"tp": 2 * chip + other_core}
    token_peer = {"tp": 2 * token_chip + core}
    weight_peer = {"tp": 2 * weight_chip + core}
    group_peer = {"dp": group + 1 - 2 * half}

    def lanes(i):
        return pl.ds(pl.multiple_of(i * LANES, LANES), LANES)

    def weight_core(c):
        return {"tp": 2 * weight_chip + c}

    def remote(src, dst, send, recv, to):
        return pltpu.make_async_remote_copy(src_ref=src, dst_ref=dst, send_sem=send, recv_sem=recv, device_id=to, device_id_type=MESH)

    def block(c, on_chip):
        return pl.multiple_of((2 * on_chip + c) * rows, rows)

    def chunk_of(j):
        return pl.ds(pl.multiple_of(j * CHUNK, CHUNK), CHUNK)

    def load_x(j):
        return pltpu.make_async_copy(x.at[chunk_of(j)], n.at[0, chunk_of(j)], x_sem.at[j])

    q_half = [wq.at[:, pl.ds(h * LANES, LANES)] for h in range(2)]
    kv = [wk, wv]

    def own_w_part(h, part):
        return w.at[0, h, core, :, pl.ds(part * LANES, LANES)]

    cuts = ((0, W_FIRST, depth), (0, depth // 2, depth))

    def at_rows(ref, part, r):
        return ref.at[pl.ds(cuts[part][r], cuts[part][r + 1] - cuts[part][r])]

    barrier = pltpu.get_barrier_semaphore()

    def greet(peers):
        for peer in peers:
            pl.semaphore_signal(barrier, inc=1, device_id=peer, device_id_type=MESH)

    follows = lax.div(2 * chip, chips) + half
    first = own_w_part(half, 0)
    first_src = wq.at[:, pl.ds(pl.multiple_of(half * LANES, LANES), LANES)]
    for r in range(W_BLOCKS):
        pltpu.make_async_copy(at_rows(first_src, 0, r), at_rows(first, 0, r), w0_sem.at[r]).start()
    greet((partner, weight_peer, weight_core(other_core)))
    second = own_w_part(1 - half, 0)
    pltpu.make_async_copy(wq.at[:, pl.ds(pl.multiple_of((1 - half) * LANES, LANES), LANES)], second, wl_sem.at[0]).start()
    for h in range(2):
        pltpu.make_async_copy(kv[h], own_w_part(h, 1), wl_sem.at[1 + h]).start()
    gain_load = pltpu.make_async_copy(gain, gain_copy, g_sem)
    gain_load.start()
    for j in range(chunks):
        load_x(j).start()
    pl.semaphore_wait(barrier, 3 + follows)
    greet((token_peer, group_peer))

    w_parts = [w.at[1, half, core, :, pl.ds(part * LANES, LANES)] for part in range(2)]
    for r in range(W_BLOCKS):
        pltpu.make_async_copy(at_rows(first, 0, r), at_rows(first, 0, r), w0_sem.at[r]).wait()
        remote(at_rows(first, 0, r), at_rows(w_parts[0], 0, r), wx_s, wx_r.at[0, r], weight_peer).start()
    for h in range(2):
        @pl.when(half == h)
        def _():
            for r in range(W_BLOCKS):
                remote(at_rows(kv[h], 1, r), at_rows(w_parts[1], 1, r), wx_s, wx_r.at[1, r], weight_peer).start()
    for h in range(2):
        for part, src in enumerate((q_half[h], kv[h])):
            remote(src, own_w_part(h, part), wl_s, wl_r, partner).start()
    gain_load.wait()
    gain_row[...] = gain_copy[...].reshape(1, depth)

    def send_n(j):
        return remote(n.at[0, chunk_of(j)], n.at[1, chunk_of(j)], n_s, n_r.at[j], token_peer)

    @pl.loop(0, chunks)
    def _(j):
        load_x(j).wait()

        @pl.loop(0, CHUNK // NORM_ROWS)
        def _(i):
            at = pl.ds(pl.multiple_of(j * CHUNK + i * NORM_ROWS, NORM_ROWS), NORM_ROWS)
            wide = n[0, at, :].astype(jnp.float32)
            mean_sq = jnp.mean(wide * wide, axis=-1, keepdims=True)
            n[0, at, :] = (wide * lax.rsqrt(mean_sq + EPSILON) * gain_row[...]).astype(jnp.bfloat16)

        @pl.when(jnp.logical_and(j == 0, follows < 2))
        def _():
            pl.semaphore_wait(barrier, 2 - follows)

        send_n(j).start()

    def product(blk, at, side, h, c):
        return jnp.dot(n[blk, at, :], w[side, h, c], preferred_element_type=jnp.float32).astype(jnp.bfloat16)

    def local_products(blk, base, start, size):
        at = pl.ds(start, size)
        out = pl.ds(pl.multiple_of(base + start, size), size)

        @pl.loop(0, 2)
        def _(h):
            for b in range(2):
                c = lax.rem(core + b, 2)
                both = product(blk, at, 0, h, c)
                if b == 0:
                    oq[out, lanes(h)] = both[:, :LANES]
                else:
                    slq[blk, at, lanes(h)] = both[:, :LANES]
                okv[h, out, lanes(c)] = both[:, LANES:]
        remote(slq.at[blk, at], oq.at[out], lq_s.at[blk], lq_r.at[blk], partner).start()
        remote(okv.at[:, out], okv.at[:, out], lkv_s.at[blk], lkv_r.at[blk], partner).start()

    own = block(core, chip)
    near = block(core, token_chip)

    own_w = w.at[0, :, core]
    pltpu.make_async_copy(second, second, wl_sem.at[0]).wait()
    for h in range(2):
        pltpu.make_async_copy(kv[h], own_w_part(h, 1), wl_sem.at[1 + h]).wait()
    other_w = w.at[0, :, other_core]
    remote(other_w, other_w, wl_s, wl_r, partner).wait_recv()

    def own_part(h, c, part):
        @pl.loop(0, rows // OWN_ROWS)
        def _(i):
            at = pl.ds(pl.multiple_of(i * OWN_ROWS, OWN_ROWS), OWN_ROWS)
            piece = w[1, h, c, :, part * LANES:(part + 1) * LANES]
            value = jnp.dot(n[0, at, :], piece, preferred_element_type=jnp.float32).astype(jnp.bfloat16)
            if part == 0:
                srq[0, c, at, lanes(h)] = value
            else:
                srkv[0, h, at, lanes(c)] = value

    def send_own(h, c, part):
        out = pl.ds(own, rows)
        if part == 0:
            remote(srq.at[0, c, :, lanes(h)], oq.at[out, lanes(h)], oq_s, oq_r.at[core], weight_core(c)).start()
        else:
            remote(srkv.at[0, h, :, lanes(c)], okv.at[h, out, lanes(c)], okv_s, okv_r, weight_peer).start()

    local_chunks = rows // OWN_ROWS
    steps = 2 * W_BLOCKS
    for step in range(steps):
        part, r = divmod(step, W_BLOCKS)
        piece = at_rows(w_parts[part], part, r)
        remote(piece, piece, wx_s, wx_r.at[part, r], weight_peer).wait_recv()
        remote(piece, piece, wg_s, wg_r, group_peer).start()
        remote(piece, piece, wd_s.at[0], wd_r.at[0], partner).start()
        if r == W_BLOCKS - 1:
            own_part(half, core, part)
            send_own(half, core, part)
        for i in range(step * local_chunks // steps, (step + 1) * local_chunks // steps):
            local_products(0, own, i * OWN_ROWS, OWN_ROWS)

    def own_products(h, c):
        @pl.loop(0, rows // OWN_ROWS)
        def _(i):
            at = pl.ds(pl.multiple_of(i * OWN_ROWS, OWN_ROWS), OWN_ROWS)
            both = product(0, at, 1, h, c)
            srq[0, c, at, lanes(h)] = both[:, :LANES]
            srkv[0, h, at, lanes(c)] = both[:, LANES:]
        for part in range(2):
            send_own(h, c, part)

    other_half = 1 - half
    from_partner = w.at[1, half, other_core]
    remote(from_partner, from_partner, wd_s.at[0], wd_r.at[0], partner).wait_recv()
    own_products(half, other_core)
    from_group = w.at[1, other_half, core]
    remote(from_group, from_group, wg_s, wg_r, group_peer).wait_recv()
    remote(from_group, from_group, wd_s.at[1], wd_r.at[1], partner).start()
    own_products(other_half, core)
    from_both = w.at[1, other_half, other_core]
    remote(from_both, from_both, wd_s.at[1], wd_r.at[1], partner).wait_recv()
    own_products(other_half, other_core)

    @pl.loop(0, chunks)
    def _(j):
        send_n(j).wait_recv()
        start = pl.multiple_of(j * CHUNK, CHUNK)
        at = pl.ds(start, CHUNK)
        out = pl.ds(pl.multiple_of(near + start, CHUNK), CHUNK)

        @pl.loop(0, 2)
        def _(h):
            for c in range(2):
                both = product(1, at, 1, h, c)
                srq[1, c, at, lanes(h)] = both[:, :LANES]
                srkv[1, h, at, lanes(c)] = both[:, LANES:]
        remote(srkv.at[1, :, at], okv.at[:, out], rkv_s, rkv_r.at[j], weight_peer).start()
        for c in (1, 0):
            remote(srq.at[1, c, at], oq.at[out], rq_s, rq_r.at[core], weight_core(c)).start()
        local_products(1, near, start, CHUNK)

    def all_q(c, on_chip):
        return oq.at[pl.ds(block(c, on_chip), rows)]

    def all_kv(c, on_chip):
        return okv.at[:, pl.ds(block(c, on_chip), rows)]

    for c in range(2):
        remote(all_q(c, weight_chip), all_q(c, weight_chip), oq_s, oq_r.at[c], weight_peer).wait_recv()
    for i, on_chip in enumerate((chip, token_chip)):
        remote(all_q(other_core, on_chip), all_q(other_core, on_chip), lq_s.at[i], lq_r.at[i], partner).wait_recv()
        remote(all_kv(other_core, on_chip), all_kv(other_core, on_chip), lkv_s.at[i], lkv_r.at[i], partner).wait_recv()

    def sent(ref, sem):
        remote(ref, ref, sem, n_r.at[0], partner).wait_send()

    sent(own_w, wl_s)
    sent(w.at[1, 0, 0], wx_s)
    sent(w.at[1, 0, 0], wg_s)
    for i in range(2):
        sent(w.at[1, 0, 0], wd_s.at[i])
        sent(slq.at[i], lq_s.at[i])
        sent(srkv.at[0], lkv_s.at[i])
    sent(n.at[0], n_s)
    sent(srq.at[0], oq_s)
    sent(srkv.at[0], okv_s)

    beside = pl.ds(block(core, weight_chip), rows)
    arrived = okv.at[:, beside]
    remote(arrived, arrived, okv_s, okv_r, weight_peer).wait_recv()
    remote(arrived, arrived, fk_s.at[0], fk_r.at[0], partner).start()
    far = block(core, far_chip)

    @pl.loop(0, chunks)
    def _(j):
        piece = okv.at[:, pl.ds(pl.multiple_of(far + j * CHUNK, CHUNK), CHUNK)]
        remote(piece, piece, rkv_s, rkv_r.at[j], weight_peer).wait_recv()
        remote(piece, piece, fk_s.at[1], fk_r.at[1], partner).start()

    sent(srkv.at[1], rkv_s)
    for i, on_chip in enumerate((weight_chip, far_chip)):
        sent(srkv.at[0], fk_s.at[i])
        remote(all_kv(other_core, on_chip), all_kv(other_core, on_chip), fk_s.at[i], fk_r.at[i], partner).wait_recv()
    sent(srq.at[1], rq_s)
    for c in range(2):
        remote(all_q(c, far_chip), all_q(c, far_chip), rq_s, rq_r.at[c], weight_peer).wait_recv()


def place(oq, okv, q, k, v, sems):
    rows = oq.shape[0] // PLACE_BLOCKS
    copies = []
    for i in range(PLACE_BLOCKS):
        at = pl.ds(i * rows, rows)
        for a, (src, dst) in enumerate(((oq, q), (okv.at[0], k), (okv.at[1], v))):
            copies.append(pltpu.make_async_copy(src.at[at], dst.at[at], sems.at[i, a]))
    for copy in copies:
        copy.start()
    for copy in copies:
        copy.wait()


def solution(mesh):
    group_size = mesh.shape["tp"]
    chips = group_size // 2

    def local_step(x_rows, norm_gain, w_q, w_k, w_v):
        rows, depth = x_rows.shape
        head = w_q.shape[2]
        tokens = rows * group_size
        dtype = x_rows.dtype
        any_space = pl.BlockSpec(memory_space=pl.ANY)
        vmem = pl.BlockSpec(memory_space=pltpu.VMEM)
        dma = pltpu.SemaphoreType.DMA
        chunks = rows // CHUNK
        oq, okv = pl.pallas_call(
            functools.partial(exchange, chips),
            out_shape=(pltpu.VMEM((tokens, head), dtype), pltpu.VMEM((2, tokens, head), dtype)),
            in_specs=[any_space] * 5,
            out_specs=(vmem, vmem),
            scratch_shapes=[
                pltpu.VMEM((depth,), norm_gain.dtype),
                pltpu.VMEM((1, depth), norm_gain.dtype),
                pltpu.VMEM((2, rows, depth), dtype),
                pltpu.VMEM((2, 2, 2, depth, 2 * LANES), dtype),
                pltpu.VMEM((2, rows, head), dtype),
                pltpu.VMEM((2, 2, rows, head), dtype),
                pltpu.VMEM((2, 2, rows, head), dtype),
                dma, dma((chunks,)),
                dma((W_BLOCKS,)), dma((3,)), dma, dma,
                dma, dma((2, W_BLOCKS)),
                dma, dma,
                dma((2,)), dma((2,)),
                dma, dma((chunks,)),
                dma, dma((2,)), dma, dma,
                dma, dma((2,)), dma, dma((chunks,)),
                dma((2,)), dma((2,)), dma((2,)), dma((2,)),
                dma((2,)), dma((2,)),
            ],
            compiler_params=pltpu.CompilerParams(collective_id=0, has_side_effects=True, vmem_limit_bytes=46 * 1024 * 1024),
        )(x_rows, norm_gain, w_q.reshape(depth, head), w_k, w_v)
        out = jax.ShapeDtypeStruct((tokens, head), dtype)
        q, k, v = pl.pallas_call(
            place,
            out_shape=(out, out, out),
            in_specs=[vmem, vmem],
            out_specs=(any_space, any_space, any_space),
            scratch_shapes=[dma((PLACE_BLOCKS, 3))],
            compiler_params=pltpu.CompilerParams(vmem_limit_bytes=1024 * 1024),
        )(pltpu.with_memory_space_constraint(oq, pltpu.VMEM), pltpu.with_memory_space_constraint(okv, pltpu.VMEM))
        return q[:, None, :], k[:, None, :], v[:, None, :]

    return jax.shard_map(local_step, mesh=mesh, in_specs=(P(("dp", "tp"), None), P(None), P(None, "tp", None), P(None, "tp"), P(None, "tp")), out_specs=(P("dp", "tp", None), P("dp", "tp", None), P("dp", "tp", None)), check_vma=False)
```

```python
import functools

import jax
import jax.numpy as jnp
from jax import lax
from jax.experimental import pallas as pl
from jax.experimental.pallas import tpu as pltpu
from jax.sharding import PartitionSpec as P

EPSILON = 1e-6
LANES = 128
NORM_ROWS = 32
CHUNK = 128
OWN_ROWS = 256
W_BLOCKS = 2
W_FIRST = 256
MESH = pl.DeviceIdType.MESH


def exchange(chips, x, gain, wq, wk, wv, oq, okv, gain_copy, gain_row, n, w, slq, srq, srkv, g_sem, x_sem, w0_sem, wl_sem, wl_s, wl_r, wx_s, wx_r, wg_s, wg_r, wd_s, wd_r, n_s, n_r,
             oq_s, oq_r, okv_s, okv_r, rq_s, rq_r, rkv_s, rkv_r, lq_s, lq_r, lkv_s, lkv_r, fk_s, fk_r):
    rows, depth = x.shape
    chunks = rows // CHUNK
    group = lax.axis_index("dp")
    device = lax.axis_index("tp")
    half = lax.rem(group, 2)
    core = lax.rem(device, 2)
    chip = lax.div(device, 2)
    token_chip = chips - 1 - chip
    weight_chip = chip + 1 - 2 * lax.rem(chip, 2)
    far_chip = chips - 1 - weight_chip
    other_core = 1 - core
    partner = {"tp": 2 * chip + other_core}
    token_peer = {"tp": 2 * token_chip + core}
    weight_peer = {"tp": 2 * weight_chip + core}
    group_peer = {"dp": group + 1 - 2 * half}

    def lanes(i):
        return pl.ds(pl.multiple_of(i * LANES, LANES), LANES)

    def weight_core(c):
        return {"tp": 2 * weight_chip + c}

    def remote(src, dst, send, recv, to):
        return pltpu.make_async_remote_copy(src_ref=src, dst_ref=dst, send_sem=send, recv_sem=recv, device_id=to, device_id_type=MESH)

    def block(c, on_chip):
        return pl.multiple_of((2 * on_chip + c) * rows, rows)

    def chunk_of(j):
        return pl.ds(pl.multiple_of(j * CHUNK, CHUNK), CHUNK)

    def load_x(j):
        return pltpu.make_async_copy(x.at[chunk_of(j)], n.at[0, chunk_of(j)], x_sem.at[j])

    q_half = [wq.at[:, pl.ds(h * LANES, LANES)] for h in range(2)]
    kv = [wk, wv]

    def own_w_part(h, part):
        return w.at[0, h, core, :, pl.ds(part * LANES, LANES)]

    cuts = ((0, W_FIRST, depth), (0, depth // 2, depth))

    def at_rows(ref, part, r):
        return ref.at[pl.ds(cuts[part][r], cuts[part][r + 1] - cuts[part][r])]

    barrier = pltpu.get_barrier_semaphore()

    def greet(peers):
        for peer in peers:
            pl.semaphore_signal(barrier, inc=1, device_id=peer, device_id_type=MESH)

    follows = lax.div(2 * chip, chips) + half
    first = own_w_part(half, 0)
    first_src = wq.at[:, pl.ds(pl.multiple_of(half * LANES, LANES), LANES)]
    for r in range(W_BLOCKS):
        pltpu.make_async_copy(at_rows(first_src, 0, r), at_rows(first, 0, r), w0_sem.at[r]).start()
    greet((partner, weight_peer, weight_core(other_core)))
    second = own_w_part(1 - half, 0)
    pltpu.make_async_copy(wq.at[:, pl.ds(pl.multiple_of((1 - half) * LANES, LANES), LANES)], second, wl_sem.at[0]).start()
    for h in range(2):
        pltpu.make_async_copy(kv[h], own_w_part(h, 1), wl_sem.at[1 + h]).start()
    gain_load = pltpu.make_async_copy(gain, gain_copy, g_sem)
    gain_load.start()
    for j in range(chunks):
        load_x(j).start()
    pl.semaphore_wait(barrier, 3 + follows)
    greet((token_peer, group_peer))

    w_parts = [w.at[1, half, core, :, pl.ds(part * LANES, LANES)] for part in range(2)]
    for r in range(W_BLOCKS):
        pltpu.make_async_copy(at_rows(first, 0, r), at_rows(first, 0, r), w0_sem.at[r]).wait()
        remote(at_rows(first, 0, r), at_rows(w_parts[0], 0, r), wx_s, wx_r.at[0, r], weight_peer).start()
    for h in range(2):
        @pl.when(half == h)
        def _():
            for r in range(W_BLOCKS):
                remote(at_rows(kv[h], 1, r), at_rows(w_parts[1], 1, r), wx_s, wx_r.at[1, r], weight_peer).start()
    for h in range(2):
        for part, src in enumerate((q_half[h], kv[h])):
            remote(src, own_w_part(h, part), wl_s, wl_r, partner).start()
    gain_load.wait()
    gain_row[...] = gain_copy[...].reshape(1, depth)

    def send_n(j):
        return remote(n.at[0, chunk_of(j)], n.at[1, chunk_of(j)], n_s, n_r.at[j], token_peer)

    @pl.loop(0, chunks)
    def _(j):
        load_x(j).wait()

        @pl.loop(0, CHUNK // NORM_ROWS)
        def _(i):
            at = pl.ds(pl.multiple_of(j * CHUNK + i * NORM_ROWS, NORM_ROWS), NORM_ROWS)
            wide = n[0, at, :].astype(jnp.float32)
            mean_sq = jnp.mean(wide * wide, axis=-1, keepdims=True)
            n[0, at, :] = (wide * lax.rsqrt(mean_sq + EPSILON) * gain_row[...]).astype(jnp.bfloat16)

        @pl.when(jnp.logical_and(j == 0, follows < 2))
        def _():
            pl.semaphore_wait(barrier, 2 - follows)

        send_n(j).start()

    def product(blk, at, side, h, c):
        return jnp.dot(n[blk, at, :], w[side, h, c], preferred_element_type=jnp.float32).astype(jnp.bfloat16)

    def local_products(blk, base, start, size):
        at = pl.ds(start, size)
        out = pl.ds(pl.multiple_of(base + start, size), size)

        @pl.loop(0, 2)
        def _(h):
            for b in range(2):
                c = lax.rem(core + b, 2)
                both = product(blk, at, 0, h, c)
                if b == 0:
                    oq[out, lanes(h)] = both[:, :LANES]
                else:
                    slq[blk, at, lanes(h)] = both[:, :LANES]
                okv[h, out, lanes(c)] = both[:, LANES:]
        remote(slq.at[blk, at], oq.at[out], lq_s.at[blk], lq_r.at[blk], partner).start()
        remote(okv.at[:, out], okv.at[:, out], lkv_s.at[blk], lkv_r.at[blk], partner).start()

    own = block(core, chip)
    near = block(core, token_chip)

    own_w = w.at[0, :, core]
    pltpu.make_async_copy(second, second, wl_sem.at[0]).wait()
    for h in range(2):
        pltpu.make_async_copy(kv[h], own_w_part(h, 1), wl_sem.at[1 + h]).wait()
    other_w = w.at[0, :, other_core]
    remote(other_w, other_w, wl_s, wl_r, partner).wait_recv()

    def own_part(h, c, part):
        @pl.loop(0, rows // OWN_ROWS)
        def _(i):
            at = pl.ds(pl.multiple_of(i * OWN_ROWS, OWN_ROWS), OWN_ROWS)
            piece = w[1, h, c, :, part * LANES:(part + 1) * LANES]
            value = jnp.dot(n[0, at, :], piece, preferred_element_type=jnp.float32).astype(jnp.bfloat16)
            if part == 0:
                srq[0, c, at, lanes(h)] = value
            else:
                srkv[0, h, at, lanes(c)] = value

    def send_own(h, c, part):
        out = pl.ds(own, rows)
        if part == 0:
            remote(srq.at[0, c, :, lanes(h)], oq.at[out, lanes(h)], oq_s, oq_r.at[core], weight_core(c)).start()
        else:
            remote(srkv.at[0, h, :, lanes(c)], okv.at[h, out, lanes(c)], okv_s, okv_r, weight_peer).start()

    local_chunks = rows // OWN_ROWS
    steps = 2 * W_BLOCKS
    for step in range(steps):
        part, r = divmod(step, W_BLOCKS)
        piece = at_rows(w_parts[part], part, r)
        remote(piece, piece, wx_s, wx_r.at[part, r], weight_peer).wait_recv()
        remote(piece, piece, wg_s, wg_r, group_peer).start()
        remote(piece, piece, wd_s.at[0], wd_r.at[0], partner).start()
        if r == W_BLOCKS - 1:
            own_part(half, core, part)
            send_own(half, core, part)
        for i in range(step * local_chunks // steps, (step + 1) * local_chunks // steps):
            local_products(0, own, i * OWN_ROWS, OWN_ROWS)

    def own_products(h, c):
        @pl.loop(0, rows // OWN_ROWS)
        def _(i):
            at = pl.ds(pl.multiple_of(i * OWN_ROWS, OWN_ROWS), OWN_ROWS)
            both = product(0, at, 1, h, c)
            srq[0, c, at, lanes(h)] = both[:, :LANES]
            srkv[0, h, at, lanes(c)] = both[:, LANES:]
        for part in range(2):
            send_own(h, c, part)

    other_half = 1 - half
    from_partner = w.at[1, half, other_core]
    remote(from_partner, from_partner, wd_s.at[0], wd_r.at[0], partner).wait_recv()
    own_products(half, other_core)
    from_group = w.at[1, other_half, core]
    remote(from_group, from_group, wg_s, wg_r, group_peer).wait_recv()
    remote(from_group, from_group, wd_s.at[1], wd_r.at[1], partner).start()
    own_products(other_half, core)
    from_both = w.at[1, other_half, other_core]
    remote(from_both, from_both, wd_s.at[1], wd_r.at[1], partner).wait_recv()
    own_products(other_half, other_core)

    @pl.loop(0, chunks)
    def _(j):
        send_n(j).wait_recv()
        start = pl.multiple_of(j * CHUNK, CHUNK)
        at = pl.ds(start, CHUNK)
        out = pl.ds(pl.multiple_of(near + start, CHUNK), CHUNK)

        @pl.loop(0, 2)
        def _(h):
            for c in range(2):
                both = product(1, at, 1, h, c)
                srq[1, c, at, lanes(h)] = both[:, :LANES]
                srkv[1, h, at, lanes(c)] = both[:, LANES:]
        remote(srkv.at[1, :, at], okv.at[:, out], rkv_s, rkv_r.at[j], weight_peer).start()
        for c in (1, 0):
            remote(srq.at[1, c, at], oq.at[out], rq_s, rq_r.at[core], weight_core(c)).start()
        local_products(1, near, start, CHUNK)

    def all_q(c, on_chip):
        return oq.at[pl.ds(block(c, on_chip), rows)]

    def all_kv(c, on_chip):
        return okv.at[:, pl.ds(block(c, on_chip), rows)]

    for c in range(2):
        remote(all_q(c, weight_chip), all_q(c, weight_chip), oq_s, oq_r.at[c], weight_peer).wait_recv()
    for i, on_chip in enumerate((chip, token_chip)):
        remote(all_q(other_core, on_chip), all_q(other_core, on_chip), lq_s.at[i], lq_r.at[i], partner).wait_recv()
        remote(all_kv(other_core, on_chip), all_kv(other_core, on_chip), lkv_s.at[i], lkv_r.at[i], partner).wait_recv()

    def sent(ref, sem):
        remote(ref, ref, sem, n_r.at[0], partner).wait_send()

    sent(own_w, wl_s)
    sent(w.at[1, 0, 0], wx_s)
    sent(w.at[1, 0, 0], wg_s)
    for i in range(2):
        sent(w.at[1, 0, 0], wd_s.at[i])
        sent(slq.at[i], lq_s.at[i])
        sent(srkv.at[0], lkv_s.at[i])
    sent(n.at[0], n_s)
    sent(srq.at[0], oq_s)
    sent(srkv.at[0], okv_s)

    beside = pl.ds(block(core, weight_chip), rows)
    arrived = okv.at[:, beside]
    remote(arrived, arrived, okv_s, okv_r, weight_peer).wait_recv()
    remote(arrived, arrived, fk_s.at[0], fk_r.at[0], partner).start()
    far = block(core, far_chip)

    @pl.loop(0, chunks)
    def _(j):
        piece = okv.at[:, pl.ds(pl.multiple_of(far + j * CHUNK, CHUNK), CHUNK)]
        remote(piece, piece, rkv_s, rkv_r.at[j], weight_peer).wait_recv()
        remote(piece, piece, fk_s.at[1], fk_r.at[1], partner).start()

    sent(srkv.at[1], rkv_s)
    for i, on_chip in enumerate((weight_chip, far_chip)):
        sent(srkv.at[0], fk_s.at[i])
        remote(all_kv(other_core, on_chip), all_kv(other_core, on_chip), fk_s.at[i], fk_r.at[i], partner).wait_recv()
    sent(srq.at[1], rq_s)
    for c in range(2):
        remote(all_q(c, far_chip), all_q(c, far_chip), rq_s, rq_r.at[c], weight_peer).wait_recv()


def solution(mesh):
    group_size = mesh.shape["tp"]
    chips = group_size // 2

    def local_step(x_rows, norm_gain, w_q, w_k, w_v):
        rows, depth = x_rows.shape
        head = w_q.shape[2]
        tokens = rows * group_size
        dtype = x_rows.dtype
        any_space = pl.BlockSpec(memory_space=pl.ANY)
        vmem = pl.BlockSpec(memory_space=pltpu.VMEM)
        dma = pltpu.SemaphoreType.DMA
        chunks = rows // CHUNK
        oq, okv = pl.pallas_call(
            functools.partial(exchange, chips),
            out_shape=(pltpu.VMEM((tokens, head), dtype), pltpu.VMEM((2, tokens, head), dtype)),
            in_specs=[any_space] * 5,
            out_specs=(vmem, vmem),
            scratch_shapes=[
                pltpu.VMEM((depth,), norm_gain.dtype),
                pltpu.VMEM((1, depth), norm_gain.dtype),
                pltpu.VMEM((2, rows, depth), dtype),
                pltpu.VMEM((2, 2, 2, depth, 2 * LANES), dtype),
                pltpu.VMEM((2, rows, head), dtype),
                pltpu.VMEM((2, 2, rows, head), dtype),
                pltpu.VMEM((2, 2, rows, head), dtype),
                dma, dma((chunks,)),
                dma((W_BLOCKS,)), dma((3,)), dma, dma,
                dma, dma((2, W_BLOCKS)),
                dma, dma,
                dma((2,)), dma((2,)),
                dma, dma((chunks,)),
                dma, dma((2,)), dma, dma,
                dma, dma((2,)), dma, dma((chunks,)),
                dma((2,)), dma((2,)), dma((2,)), dma((2,)),
                dma((2,)), dma((2,)),
            ],
            compiler_params=pltpu.CompilerParams(collective_id=0, has_side_effects=True, vmem_limit_bytes=46 * 1024 * 1024),
        )(x_rows, norm_gain, w_q.reshape(depth, head), w_k, w_v)
        q, k, v = oq, okv[0], okv[1]
        return q[:, None, :], k[:, None, :], v[:, None, :]

    return jax.shard_map(local_step, mesh=mesh, in_specs=(P(("dp", "tp"), None), P(None), P(None, "tp", None), P(None, "tp"), P(None, "tp")), out_specs=(P("dp", "tp", None), P("dp", "tp", None), P("dp", "tp", None)), check_vma=False)
```

```python
import functools

import jax
import jax.numpy as jnp
from jax import lax
from jax.experimental import pallas as pl
from jax.experimental.pallas import tpu as pltpu
from jax.sharding import PartitionSpec as P

EPSILON = 1e-6
LANES = 128
NORM_ROWS = 32
CHUNK = 128
EARLY = 4
EARLY_SENDS = 5
OWN_ROWS = 256
W_BLOCKS = 2
W_FIRST = 256
MESH = pl.DeviceIdType.MESH


class Place:
    def __init__(self, chips, rows):
        self.rows = rows
        group = lax.axis_index("dp")
        device = lax.axis_index("tp")
        self.half = lax.rem(group, 2)
        self.core = lax.rem(device, 2)
        self.chip = lax.div(device, 2)
        self.token_chip = chips - 1 - self.chip
        self.weight_chip = self.chip + 1 - 2 * lax.rem(self.chip, 2)
        self.far_chip = chips - 1 - self.weight_chip
        self.other_core = 1 - self.core
        self.partner = {"tp": 2 * self.chip + self.other_core}
        self.token_peer = {"tp": 2 * self.token_chip + self.core}
        self.weight_peer = self.weight_core(self.core)
        self.group_peer = {"dp": group + 1 - 2 * self.half}
        self.follows = lax.div(2 * self.chip, chips) + self.half
        self.sends = EARLY_SENDS + 2 * self.core

    def weight_core(self, c):
        return {"tp": 2 * self.weight_chip + c}

    def block(self, c, on_chip):
        return pl.multiple_of((2 * on_chip + c) * self.rows, self.rows)


def remote(src, dst, send, recv, to):
    return pltpu.make_async_remote_copy(src_ref=src, dst_ref=dst, send_sem=send, recv_sem=recv, device_id=to, device_id_type=MESH)


def arrive(ref, sem, frm):
    remote(ref, ref, sem, sem, frm).wait_recv()


def sent(ref, sem, to):
    remote(ref, ref, sem, sem, to).wait_send()


def lanes(i):
    return pl.ds(pl.multiple_of(i * LANES, LANES), LANES)


def chunk_of(j):
    return pl.ds(pl.multiple_of(j * CHUNK, CHUNK), CHUNK)


def greet(barrier, peers):
    for peer in peers:
        pl.semaphore_signal(barrier, inc=1, device_id=peer, device_id_type=MESH)


def product(n, w, blk, at, side, h, c):
    return jnp.dot(n[blk, at, :], w[side, h, c], preferred_element_type=jnp.float32).astype(jnp.bfloat16)


def local_products(me, n, w, oq, okv, slq, blk, base, start, size, stage, q_sems, kv_sems):
    at = pl.ds(start, size)
    out = pl.ds(pl.multiple_of(base + start, size), size)

    @pl.loop(0, 2)
    def _(h):
        for b in range(2):
            c = lax.rem(me.core + b, 2)
            both = product(n, w, blk, at, 0, h, c)
            if b == 0:
                oq[out, lanes(h)] = both[:, :LANES]
            else:
                slq[stage, lanes(h)] = both[:, :LANES]
            okv[h, out, lanes(c)] = both[:, LANES:]
    remote(slq.at[stage], oq.at[out], *q_sems, me.partner).start()
    remote(okv.at[:, out], okv.at[:, out], *kv_sems, me.partner).start()


def remote_products(n, w, at, srq, srkv, stage):
    @pl.loop(0, 2)
    def _(h):
        for c in range(2):
            both = product(n, w, 1, at, 1, h, c)
            srq[c, at, lanes(h)] = both[:, :LANES]
            srkv[h, stage, lanes(c)] = both[:, LANES:]


def early_products(me, n, w, oq, okv, srq, srkv, ek_s, ek_r, eq_s, eq_r):
    near = me.block(me.core, me.token_chip)

    @pl.loop(0, EARLY)
    def _(j):
        at = chunk_of(j)
        out = pl.ds(pl.multiple_of(near + j * CHUNK, CHUNK), CHUNK)
        remote_products(n, w, at, srq, srkv, at)
        remote(srkv.at[:, at], okv.at[:, out], ek_s, ek_r, me.weight_peer).start()
        remote(srq.at[me.core, at], oq.at[out], eq_s, eq_r, me.weight_peer).start()


def finish_early(me, oq, okv, srq, srkv, ek_s, ek_r, eq_s, eq_r):
    at = pl.ds(0, EARLY * CHUNK)
    out = pl.ds(me.block(me.core, me.far_chip), EARLY * CHUNK)
    sent(srkv.at[:, at], ek_s, me.weight_peer)
    sent(srq.at[me.core, at], eq_s, me.weight_peer)
    arrive(okv.at[:, out], ek_r, me.weight_peer)
    arrive(oq.at[out], eq_r, me.weight_peer)


def first_exchange(chips, x, gain, wq, wk, wv, oq, okv, n, w, srq, gain_copy, gain_row, slq, srq0, srkv0, srkv, g_sem, x_sem, w0_sem, wl_sem, wl_s, wl_r,
                   wx_s, wx_r, wg_s, wg_r, wd_s, wd_r, n_s, n_r, oq_s, oq_r, okv_s, okv_r, lq_s, lq_r, lkv_s, lkv_r, fk_s, fk_r, ek_s, ek_r, eq_s, eq_r):
    rows, depth = x.shape
    chunks = rows // CHUNK
    me = Place(chips, rows)
    half, core, other_core = me.half, me.core, me.other_core
    partner, token_peer, weight_peer, group_peer = me.partner, me.token_peer, me.weight_peer, me.group_peer
    weight_core, follows, sends = me.weight_core, me.follows, me.sends

    def load_x(j):
        return pltpu.make_async_copy(x.at[chunk_of(j)], n.at[0, chunk_of(j)], x_sem.at[j])

    q_half = [wq.at[:, pl.ds(h * LANES, LANES)] for h in range(2)]
    kv = [wk, wv]

    def own_w_part(h, part):
        return w.at[0, h, core, :, pl.ds(part * LANES, LANES)]

    cuts = ((0, W_FIRST, depth), (0, depth // 2, depth))

    def at_rows(ref, part, r):
        return ref.at[pl.ds(cuts[part][r], cuts[part][r + 1] - cuts[part][r])]

    barrier = pltpu.get_barrier_semaphore()

    first = own_w_part(half, 0)
    first_src = wq.at[:, pl.ds(pl.multiple_of(half * LANES, LANES), LANES)]
    for r in range(W_BLOCKS):
        pltpu.make_async_copy(at_rows(first_src, 0, r), at_rows(first, 0, r), w0_sem.at[r]).start()
    greet(barrier, (partner, weight_peer, weight_core(other_core)))
    second = own_w_part(1 - half, 0)
    pltpu.make_async_copy(wq.at[:, pl.ds(pl.multiple_of((1 - half) * LANES, LANES), LANES)], second, wl_sem.at[0]).start()
    for h in range(2):
        pltpu.make_async_copy(kv[h], own_w_part(h, 1), wl_sem.at[1 + h]).start()
    gain_load = pltpu.make_async_copy(gain, gain_copy, g_sem)
    gain_load.start()
    for j in range(chunks):
        load_x(j).start()
    pl.semaphore_wait(barrier, 3 + follows)
    greet(barrier, (token_peer, group_peer))

    w_parts = [w.at[1, half, core, :, pl.ds(part * LANES, LANES)] for part in range(2)]
    for r in range(W_BLOCKS):
        pltpu.make_async_copy(at_rows(first, 0, r), at_rows(first, 0, r), w0_sem.at[r]).wait()
        remote(at_rows(first, 0, r), at_rows(w_parts[0], 0, r), wx_s, wx_r.at[0, r], weight_peer).start()
    for h in range(2):
        @pl.when(half == h)
        def _():
            for r in range(W_BLOCKS):
                remote(at_rows(kv[h], 1, r), at_rows(w_parts[1], 1, r), wx_s, wx_r.at[1, r], weight_peer).start()
    for h in range(2):
        for part, src in enumerate((q_half[h], kv[h])):
            remote(src, own_w_part(h, part), wl_s, wl_r, partner).start()
    gain_load.wait()
    gain_row[...] = gain_copy[...].reshape(1, depth)

    def send_n(j):
        return remote(n.at[0, chunk_of(j)], n.at[1, chunk_of(j)], n_s, n_r.at[j], token_peer)

    @pl.loop(0, chunks)
    def _(j):
        load_x(j).wait()

        @pl.loop(0, CHUNK // NORM_ROWS)
        def _(i):
            at = pl.ds(pl.multiple_of(j * CHUNK + i * NORM_ROWS, NORM_ROWS), NORM_ROWS)
            wide = n[0, at, :].astype(jnp.float32)
            mean_sq = jnp.mean(wide * wide, axis=-1, keepdims=True)
            n[0, at, :] = (wide * lax.rsqrt(mean_sq + EPSILON) * gain_row[...]).astype(jnp.bfloat16)

        @pl.when(jnp.logical_and(j == 0, follows < 2))
        def _():
            pl.semaphore_wait(barrier, 2 - follows)

        @pl.when(j < sends)
        def _():
            send_n(j).start()

    own = me.block(core, me.chip)
    near = me.block(core, me.token_chip)

    def own_rows(start, size, stage):
        local_products(me, n, w, oq, okv, slq, 0, own, start, size, stage, (lq_s.at[0], lq_r.at[0]), (lkv_s.at[0], lkv_r.at[0]))

    own_w = w.at[0, :, core]
    pltpu.make_async_copy(second, second, wl_sem.at[0]).wait()
    for h in range(2):
        pltpu.make_async_copy(kv[h], own_w_part(h, 1), wl_sem.at[1 + h]).wait()
    other_w = w.at[0, :, other_core]
    remote(other_w, other_w, wl_s, wl_r, partner).wait_recv()

    def own_part(h, c, part):
        @pl.loop(0, rows // OWN_ROWS)
        def _(i):
            at = pl.ds(pl.multiple_of(i * OWN_ROWS, OWN_ROWS), OWN_ROWS)
            piece = w[1, h, c, :, part * LANES:(part + 1) * LANES]
            value = jnp.dot(n[0, at, :], piece, preferred_element_type=jnp.float32).astype(jnp.bfloat16)
            if part == 0:
                srq0[c, at, lanes(h)] = value
            else:
                srkv0[h, at, lanes(c)] = value

    def send_own(h, c, part):
        out = pl.ds(own, rows)
        if part == 0:
            remote(srq0.at[c, :, lanes(h)], oq.at[out, lanes(h)], oq_s, oq_r.at[core], weight_core(c)).start()
        else:
            remote(srkv0.at[h, :, lanes(c)], okv.at[h, out, lanes(c)], okv_s, okv_r, weight_peer).start()

    local_chunks = rows // OWN_ROWS
    steps = 2 * W_BLOCKS
    for step in range(steps):
        part, r = divmod(step, W_BLOCKS)
        piece = at_rows(w_parts[part], part, r)
        remote(piece, piece, wx_s, wx_r.at[part, r], weight_peer).wait_recv()
        remote(piece, piece, wg_s, wg_r, group_peer).start()
        remote(piece, piece, wd_s.at[0], wd_r.at[0], partner).start()
        if r == W_BLOCKS - 1:
            own_part(half, core, part)
            send_own(half, core, part)
        for i in range(step * local_chunks // steps, (step + 1) * local_chunks // steps):
            own_rows(i * OWN_ROWS, OWN_ROWS, pl.ds(i * OWN_ROWS, OWN_ROWS))

    def own_products(h, c):
        @pl.loop(0, rows // OWN_ROWS)
        def _(i):
            at = pl.ds(pl.multiple_of(i * OWN_ROWS, OWN_ROWS), OWN_ROWS)
            both = product(n, w, 0, at, 1, h, c)
            srq0[c, at, lanes(h)] = both[:, :LANES]
            srkv0[h, at, lanes(c)] = both[:, LANES:]
        for part in range(2):
            send_own(h, c, part)

    other_half = 1 - half
    from_partner = w.at[1, half, other_core]
    remote(from_partner, from_partner, wd_s.at[0], wd_r.at[0], partner).wait_recv()
    own_products(half, other_core)
    from_group = w.at[1, other_half, core]
    remote(from_group, from_group, wg_s, wg_r, group_peer).wait_recv()
    remote(from_group, from_group, wd_s.at[1], wd_r.at[1], partner).start()
    own_products(other_half, core)
    from_both = w.at[1, other_half, other_core]
    remote(from_both, from_both, wd_s.at[1], wd_r.at[1], partner).wait_recv()
    own_products(other_half, other_core)

    @pl.loop(0, EARLY)
    def _(j):
        send_n(j).wait_recv()
        start = pl.multiple_of(j * CHUNK, CHUNK)
        stage = pl.ds(pl.multiple_of(rows + start, CHUNK), CHUNK)
        local_products(me, n, w, oq, okv, slq, 1, near, start, CHUNK, stage, (lq_s.at[1], lq_r.at[1]), (lkv_s.at[1], lkv_r.at[1]))

    @pl.when(core == 1)
    def _():
        early_products(me, n, w, oq, okv, srq, srkv, ek_s, ek_r, eq_s, eq_r)

    @pl.loop(EARLY, sends)
    def _(j):
        send_n(j).wait_recv()

    for c in range(2):
        arrive(oq.at[pl.ds(me.block(c, me.weight_chip), rows)], oq_r.at[c], weight_peer)
    beside = okv.at[:, pl.ds(me.block(core, me.weight_chip), rows)]
    arrive(beside, okv_r, weight_peer)
    remote(beside, beside, fk_s, fk_r, partner).start()
    for i, (on_chip, size) in enumerate(((me.chip, rows), (me.token_chip, EARLY * CHUNK))):
        theirs = pl.ds(me.block(other_core, on_chip), size)
        mine = pl.ds(0, size)
        arrive(oq.at[theirs], lq_r.at[i], partner)
        arrive(okv.at[:, theirs], lkv_r.at[i], partner)
        sent(slq.at[mine], lq_s.at[i], partner)
        sent(okv.at[:, mine], lkv_s.at[i], partner)
    for i in range(2):
        @pl.when(core == i)
        def _():
            sent(n.at[0, pl.ds(0, (EARLY_SENDS + 2 * i) * CHUNK)], n_s, token_peer)
    sent(own_w, wl_s, partner)
    sent(w.at[1, 0, 0], wx_s, weight_peer)
    sent(w.at[1, 0, 0], wg_s, group_peer)
    for i in range(2):
        sent(w.at[1, 0, 0], wd_s.at[i], partner)
    sent(srq0, oq_s, weight_peer)
    sent(srkv0, okv_s, weight_peer)

    @pl.when(core == 1)
    def _():
        finish_early(me, oq, okv, srq, srkv, ek_s, ek_r, eq_s, eq_r)

    sent(beside, fk_s, partner)
    arrive(okv.at[:, pl.ds(me.block(other_core, me.weight_chip), rows)], fk_r, partner)


def second_exchange(chips, w, written, oq_in, okv_in, n_in, srq_in, oq, okv, n, srq, srkv, slq, n_s, n_r, ek_s, ek_r, eq_s, eq_r, xb_s, xb_r, rq_s, rq_r, rkv_s, rkv_r,
                    lq_s, lq_r, lkv_s, lkv_r, fe_s, fe_r, fk_s, fk_r):
    rows = n.shape[1]
    chunks = rows // CHUNK
    early = EARLY * CHUNK
    late = rows - early
    me = Place(chips, rows)
    core, other_core, partner, weight_peer = me.core, me.other_core, me.partner, me.weight_peer
    near = me.block(core, me.token_chip)
    far = me.block(core, me.far_chip)

    barrier = pltpu.get_barrier_semaphore()
    greet(barrier, (weight_peer, me.token_peer))
    pl.semaphore_wait(barrier, 2 + 2 * core)
    greet(barrier, (partner, me.weight_core(other_core)))

    def send_n(j):
        return remote(n.at[0, chunk_of(j)], n.at[1, chunk_of(j)], n_s, n_r.at[j], me.token_peer)

    @pl.loop(me.sends, chunks)
    def _(j):
        send_n(j).start()

    @pl.when(core == 0)
    def _():
        early_products(me, n, w, oq, okv, srq, srkv, ek_s, ek_r, eq_s, eq_r)
        pl.semaphore_wait(barrier, 2)

    remote(srq.at[other_core, pl.ds(0, early)], oq.at[pl.ds(near, early)], xb_s, xb_r, me.weight_core(other_core)).start()

    @pl.loop(EARLY, chunks)
    def _(j):
        @pl.when(j >= me.sends)
        def _():
            send_n(j).wait_recv()

        start = pl.multiple_of(j * CHUNK, CHUNK)
        at = pl.ds(start, CHUNK)
        out = pl.ds(pl.multiple_of(near + start, CHUNK), CHUNK)
        remote_products(n, w, at, srq, srkv, at)
        remote(srkv.at[:, at], okv.at[:, out], rkv_s, rkv_r.at[j - EARLY], weight_peer).start()
        for c in (1, 0):
            remote(srq.at[c, at], oq.at[out], rq_s, rq_r.at[core], me.weight_core(c)).start()
        stage = pl.ds(pl.multiple_of(start - early, CHUNK), CHUNK)
        local_products(me, n, w, oq, okv, slq, 1, near, start, CHUNK, stage, (lq_s, lq_r), (lkv_s, lkv_r))

    @pl.when(core == 0)
    def _():
        finish_early(me, oq, okv, srq, srkv, ek_s, ek_r, eq_s, eq_r)

    far_early = okv.at[:, pl.ds(far, early)]
    remote(far_early, far_early, fe_s, fe_r, partner).start()
    theirs = pl.ds(pl.multiple_of(me.block(other_core, me.token_chip) + early, CHUNK), late)
    arrive(oq.at[theirs], lq_r, partner)
    arrive(okv.at[:, theirs], lkv_r, partner)
    sent(slq, lq_s, partner)
    sent(okv.at[:, theirs], lkv_s, partner)
    arrive(oq.at[pl.ds(me.block(other_core, me.far_chip), early)], xb_r, weight_peer)
    sent(srq.at[other_core, pl.ds(0, early)], xb_s, weight_peer)
    for i in range(2):
        @pl.when(core == i)
        def _():
            sent(n.at[0, pl.ds((EARLY_SENDS + 2 * i) * CHUNK, rows - (EARLY_SENDS + 2 * i) * CHUNK)], n_s, me.token_peer)

    @pl.loop(EARLY, chunks)
    def _(j):
        piece = okv.at[:, pl.ds(pl.multiple_of(far + j * CHUNK, CHUNK), CHUNK)]
        remote(piece, piece, rkv_s, rkv_r.at[j - EARLY], weight_peer).wait_recv()
        remote(piece, piece, fk_s, fk_r, partner).start()

    tail = pl.ds(early, late)
    sent(srkv.at[:, tail], rkv_s, weight_peer)
    sent(far_early, fe_s, partner)
    sent(srkv.at[:, tail], fk_s, partner)
    arrive(okv.at[:, pl.ds(me.block(other_core, me.far_chip), early)], fe_r, partner)
    arrive(okv.at[:, pl.ds(pl.multiple_of(me.block(other_core, me.far_chip) + early, CHUNK), late)], fk_r, partner)
    sent(srq.at[:, tail], rq_s, weight_peer)
    for c in range(2):
        arrive(oq.at[pl.ds(pl.multiple_of(me.block(c, me.far_chip) + early, CHUNK), late)], rq_r.at[c], weight_peer)


def write_rows(blocks, oq, okv, q, k, v, sems):
    copies = []
    for i, (start, size) in enumerate(blocks):
        at = pl.ds(start, size)
        for a, (src, dst) in enumerate(((oq, q), (okv.at[0], k), (okv.at[1], v))):
            copies.append(pltpu.make_async_copy(src.at[at], dst.at[at], sems.at[i, a]))
    for copy in copies:
        copy.start()
    for copy in copies:
        copy.wait()


def first_write(chips, rows, oq, okv, q, k, v, written, sems):
    me = Place(chips, rows)
    written[...] = jnp.zeros_like(written)
    blocks = [(me.block(0, me.chip), 2 * rows), (me.block(0, me.weight_chip), 2 * rows)]
    blocks += [(me.block(c, me.token_chip), EARLY * CHUNK) for c in range(2)]
    write_rows(blocks, oq, okv, q, k, v, sems)


def last_write(chips, rows, oq, okv, q_in, k_in, v_in, q, k, v, sems):
    me = Place(chips, rows)
    early = EARLY * CHUNK
    blocks = [(me.block(0, me.far_chip), 2 * rows)]
    blocks += [(pl.multiple_of(me.block(c, me.token_chip) + early, CHUNK), rows - early) for c in range(2)]
    write_rows(blocks, oq, okv, q, k, v, sems)


def solution(mesh):
    group_size = mesh.shape["tp"]
    chips = group_size // 2

    def local_step(x_rows, norm_gain, w_q, w_k, w_v):
        rows, depth = x_rows.shape
        head = w_q.shape[2]
        tokens = rows * group_size
        dtype = x_rows.dtype
        any_space = pl.BlockSpec(memory_space=pl.ANY)
        vmem = pl.BlockSpec(memory_space=pltpu.VMEM)
        dma = pltpu.SemaphoreType.DMA
        chunks = rows // CHUNK
        early = EARLY * CHUNK
        oq_type, okv_type = pltpu.VMEM((tokens, head), dtype), pltpu.VMEM((2, tokens, head), dtype)
        n_type, srq_type = pltpu.VMEM((2, rows, depth), dtype), pltpu.VMEM((2, rows, head), dtype)

        def held(*arrays):
            return [pltpu.with_memory_space_constraint(a, pltpu.VMEM) for a in arrays]

        oq, okv, n, w, srq = pl.pallas_call(
            functools.partial(first_exchange, chips),
            out_shape=(oq_type, okv_type, n_type, pltpu.VMEM((2, 2, 2, depth, 2 * LANES), dtype), srq_type),
            in_specs=[any_space] * 5,
            out_specs=(vmem,) * 5,
            scratch_shapes=[
                pltpu.VMEM((depth,), norm_gain.dtype),
                pltpu.VMEM((1, depth), norm_gain.dtype),
                pltpu.VMEM((rows + early, head), dtype),
                pltpu.VMEM((2, rows, head), dtype),
                pltpu.VMEM((2, rows, head), dtype),
                pltpu.VMEM((2, early, head), dtype),
                dma, dma((chunks,)),
                dma((W_BLOCKS,)), dma((3,)), dma, dma,
                dma, dma((2, W_BLOCKS)),
                dma, dma,
                dma((2,)), dma((2,)),
                dma, dma((chunks,)),
                dma, dma((2,)), dma, dma,
                dma((2,)), dma((2,)), dma((2,)), dma((2,)),
                dma, dma, dma, dma, dma, dma,
            ],
            compiler_params=pltpu.CompilerParams(collective_id=0, has_side_effects=True, vmem_limit_bytes=16 * 1024 * 1024),
        )(*[pltpu.with_memory_space_constraint(a, pltpu.HBM) for a in (x_rows, norm_gain, w_q.reshape(depth, head), w_k, w_v)])
        out = jax.ShapeDtypeStruct((tokens, head), dtype)
        q, k, v, written = pl.pallas_call(
            functools.partial(first_write, chips, rows),
            out_shape=(out, out, out, jax.ShapeDtypeStruct((8, LANES), jnp.float32)),
            in_specs=[vmem, vmem],
            out_specs=(any_space, any_space, any_space, vmem),
            scratch_shapes=[dma((4, 3))],
            compiler_params=pltpu.CompilerParams(vmem_limit_bytes=1024 * 1024),
        )(*held(oq, okv))
        oq, okv, _, _ = pl.pallas_call(
            functools.partial(second_exchange, chips),
            out_shape=(oq_type, okv_type, n_type, srq_type),
            in_specs=[vmem, any_space, vmem, vmem, vmem, vmem],
            out_specs=(vmem,) * 4,
            input_output_aliases={2: 0, 3: 1, 4: 2, 5: 3},
            scratch_shapes=[
                pltpu.VMEM((2, rows, head), dtype),
                pltpu.VMEM((rows - early, head), dtype),
                dma, dma((chunks,)),
                dma, dma, dma, dma, dma, dma,
                dma, dma((2,)), dma, dma((chunks - EARLY,)),
                dma, dma, dma, dma,
                dma, dma, dma, dma,
            ],
            compiler_params=pltpu.CompilerParams(collective_id=1, has_side_effects=True, vmem_limit_bytes=16 * 1024 * 1024),
        )(*held(w), written, *held(oq, okv, n, srq))
        q, k, v = pl.pallas_call(
            functools.partial(last_write, chips, rows),
            out_shape=(out, out, out),
            in_specs=[vmem, vmem, any_space, any_space, any_space],
            out_specs=(any_space, any_space, any_space),
            input_output_aliases={2: 0, 3: 1, 4: 2},
            scratch_shapes=[dma((3, 3))],
            compiler_params=pltpu.CompilerParams(vmem_limit_bytes=1024 * 1024),
        )(*held(oq, okv), q, k, v)
        return q[:, None, :], k[:, None, :], v[:, None, :]

    return jax.shard_map(local_step, mesh=mesh, in_specs=(P(("dp", "tp"), None), P(None), P(None, "tp", None), P(None, "tp"), P(None, "tp")), out_specs=(P("dp", "tp", None), P("dp", "tp", None), P("dp", "tp", None)), check_vma=False)
```

```python
import functools

import jax
import jax.numpy as jnp
from jax import lax
from jax.experimental import pallas as pl
from jax.experimental.pallas import tpu as pltpu
from jax.sharding import PartitionSpec as P

EPSILON = 1e-6
LANES = 128
NORM_ROWS = 32
CHUNK = 128
EARLY = 4
EARLY_SENDS = 5
OWN_ROWS = 256
W_BLOCKS = 2
W_FIRST = 256
MESH = pl.DeviceIdType.MESH


class Place:
    def __init__(self, chips, rows):
        self.rows = rows
        group = lax.axis_index("dp")
        device = lax.axis_index("tp")
        self.half = lax.rem(group, 2)
        self.core = lax.rem(device, 2)
        self.chip = lax.div(device, 2)
        self.token_chip = chips - 1 - self.chip
        self.weight_chip = self.chip + 1 - 2 * lax.rem(self.chip, 2)
        self.far_chip = chips - 1 - self.weight_chip
        self.other_core = 1 - self.core
        self.partner = {"tp": 2 * self.chip + self.other_core}
        self.token_peer = {"tp": 2 * self.token_chip + self.core}
        self.weight_peer = self.weight_core(self.core)
        self.group_peer = {"dp": group + 1 - 2 * self.half}
        self.follows = lax.div(2 * self.chip, chips) + self.half
        self.sends = EARLY_SENDS + 2 * self.core

    def weight_core(self, c):
        return {"tp": 2 * self.weight_chip + c}

    def block(self, c, on_chip):
        return pl.multiple_of((2 * on_chip + c) * self.rows, self.rows)


def remote(src, dst, send, recv, to):
    return pltpu.make_async_remote_copy(src_ref=src, dst_ref=dst, send_sem=send, recv_sem=recv, device_id=to, device_id_type=MESH)


def arrive(ref, sem, frm):
    remote(ref, ref, sem, sem, frm).wait_recv()


def sent(ref, sem, to):
    remote(ref, ref, sem, sem, to).wait_send()


def lanes(i):
    return pl.ds(pl.multiple_of(i * LANES, LANES), LANES)


def chunk_of(j):
    return pl.ds(pl.multiple_of(j * CHUNK, CHUNK), CHUNK)


def greet(barrier, peers):
    for peer in peers:
        pl.semaphore_signal(barrier, inc=1, device_id=peer, device_id_type=MESH)


def product(n, w, blk, at, side, h, c):
    return jnp.dot(n[blk, at, :], w[side, h, c], preferred_element_type=jnp.float32).astype(jnp.bfloat16)


def local_products(me, n, w, oq, okv, slq, blk, base, start, size, stage, q_sems, kv_sems):
    at = pl.ds(start, size)
    out = pl.ds(pl.multiple_of(base + start, size), size)

    @pl.loop(0, 2)
    def _(h):
        for b in range(2):
            c = lax.rem(me.core + b, 2)
            both = product(n, w, blk, at, 0, h, c)
            if b == 0:
                oq[out, lanes(h)] = both[:, :LANES]
            else:
                slq[stage, lanes(h)] = both[:, :LANES]
            okv[h, out, lanes(c)] = both[:, LANES:]
    remote(slq.at[stage], oq.at[out], *q_sems, me.partner).start()
    remote(okv.at[:, out], okv.at[:, out], *kv_sems, me.partner).start()


def remote_products(n, w, at, srq, srkv, stage):
    @pl.loop(0, 2)
    def _(h):
        for c in range(2):
            both = product(n, w, 1, at, 1, h, c)
            srq[c, at, lanes(h)] = both[:, :LANES]
            srkv[h, stage, lanes(c)] = both[:, LANES:]


def early_products(me, n, w, oq, okv, srq, srkv, ek_s, ek_r, eq_s, eq_r):
    near = me.block(me.core, me.token_chip)

    @pl.loop(0, EARLY)
    def _(j):
        at = chunk_of(j)
        out = pl.ds(pl.multiple_of(near + j * CHUNK, CHUNK), CHUNK)
        remote_products(n, w, at, srq, srkv, at)
        remote(srkv.at[:, at], okv.at[:, out], ek_s, ek_r, me.weight_peer).start()
        remote(srq.at[me.core, at], oq.at[out], eq_s, eq_r, me.weight_peer).start()


def finish_early(me, oq, okv, srq, srkv, ek_s, ek_r, eq_s, eq_r):
    at = pl.ds(0, EARLY * CHUNK)
    out = pl.ds(me.block(me.core, me.far_chip), EARLY * CHUNK)
    sent(srkv.at[:, at], ek_s, me.weight_peer)
    sent(srq.at[me.core, at], eq_s, me.weight_peer)
    arrive(okv.at[:, out], ek_r, me.weight_peer)
    arrive(oq.at[out], eq_r, me.weight_peer)


def first_exchange(chips, x, gain, wq, wk, wv, oq, okv, n, w, srq, gain_copy, gain_row, slq, srq0, srkv0, srkv, g_sem, x_sem, w0_sem, wl_sem, wl_s, wl_r,
                   wx_s, wx_r, wg_s, wg_r, wd_s, wd_r, n_s, n_r, oq_s, oq_r, okv_s, okv_r, lq_s, lq_r, lkv_s, lkv_r, fk_s, fk_r, ek_s, ek_r, eq_s, eq_r):
    rows, depth = x.shape
    chunks = rows // CHUNK
    me = Place(chips, rows)
    half, core, other_core = me.half, me.core, me.other_core
    partner, token_peer, weight_peer, group_peer = me.partner, me.token_peer, me.weight_peer, me.group_peer
    weight_core, follows, sends = me.weight_core, me.follows, me.sends

    def load_x(j):
        return pltpu.make_async_copy(x.at[chunk_of(j)], n.at[0, chunk_of(j)], x_sem.at[j])

    q_half = [wq.at[:, pl.ds(h * LANES, LANES)] for h in range(2)]
    kv = [wk, wv]

    def own_w_part(h, part):
        return w.at[0, h, core, :, pl.ds(part * LANES, LANES)]

    cuts = ((0, W_FIRST, depth), (0, depth // 2, depth))

    def at_rows(ref, part, r):
        return ref.at[pl.ds(cuts[part][r], cuts[part][r + 1] - cuts[part][r])]

    barrier = pltpu.get_barrier_semaphore()

    first = own_w_part(half, 0)
    first_src = wq.at[:, pl.ds(pl.multiple_of(half * LANES, LANES), LANES)]
    for r in range(W_BLOCKS):
        pltpu.make_async_copy(at_rows(first_src, 0, r), at_rows(first, 0, r), w0_sem.at[r]).start()
    greet(barrier, (partner, weight_peer, weight_core(other_core)))
    second = own_w_part(1 - half, 0)
    pltpu.make_async_copy(wq.at[:, pl.ds(pl.multiple_of((1 - half) * LANES, LANES), LANES)], second, wl_sem.at[0]).start()
    for h in range(2):
        pltpu.make_async_copy(kv[h], own_w_part(h, 1), wl_sem.at[1 + h]).start()
    gain_load = pltpu.make_async_copy(gain, gain_copy, g_sem)
    gain_load.start()
    for j in range(chunks):
        load_x(j).start()
    pl.semaphore_wait(barrier, 3 + follows)
    greet(barrier, (token_peer, group_peer))

    w_parts = [w.at[1, half, core, :, pl.ds(part * LANES, LANES)] for part in range(2)]
    for r in range(W_BLOCKS):
        pltpu.make_async_copy(at_rows(first, 0, r), at_rows(first, 0, r), w0_sem.at[r]).wait()
        remote(at_rows(first, 0, r), at_rows(w_parts[0], 0, r), wx_s, wx_r.at[0, r], weight_peer).start()
    for h in range(2):
        @pl.when(half == h)
        def _():
            for r in range(W_BLOCKS):
                remote(at_rows(kv[h], 1, r), at_rows(w_parts[1], 1, r), wx_s, wx_r.at[1, r], weight_peer).start()
    for h in range(2):
        for part, src in enumerate((q_half[h], kv[h])):
            remote(src, own_w_part(h, part), wl_s, wl_r, partner).start()
    gain_load.wait()
    gain_row[...] = gain_copy[...].reshape(1, depth)

    def send_n(j):
        return remote(n.at[0, chunk_of(j)], n.at[1, chunk_of(j)], n_s, n_r.at[j], token_peer)

    @pl.loop(0, chunks)
    def _(j):
        load_x(j).wait()

        @pl.loop(0, CHUNK // NORM_ROWS)
        def _(i):
            at = pl.ds(pl.multiple_of(j * CHUNK + i * NORM_ROWS, NORM_ROWS), NORM_ROWS)
            wide = n[0, at, :].astype(jnp.float32)
            mean_sq = jnp.mean(wide * wide, axis=-1, keepdims=True)
            n[0, at, :] = (wide * lax.rsqrt(mean_sq + EPSILON) * gain_row[...]).astype(jnp.bfloat16)

        @pl.when(jnp.logical_and(j == 0, follows < 2))
        def _():
            pl.semaphore_wait(barrier, 2 - follows)

        @pl.when(j < sends)
        def _():
            send_n(j).start()

    own = me.block(core, me.chip)
    near = me.block(core, me.token_chip)

    def own_rows(start, size, stage):
        local_products(me, n, w, oq, okv, slq, 0, own, start, size, stage, (lq_s.at[0], lq_r.at[0]), (lkv_s.at[0], lkv_r.at[0]))

    own_w = w.at[0, :, core]
    pltpu.make_async_copy(second, second, wl_sem.at[0]).wait()
    for h in range(2):
        pltpu.make_async_copy(kv[h], own_w_part(h, 1), wl_sem.at[1 + h]).wait()
    other_w = w.at[0, :, other_core]
    remote(other_w, other_w, wl_s, wl_r, partner).wait_recv()

    def own_part(h, c, part):
        @pl.loop(0, rows // OWN_ROWS)
        def _(i):
            at = pl.ds(pl.multiple_of(i * OWN_ROWS, OWN_ROWS), OWN_ROWS)
            piece = w[1, h, c, :, part * LANES:(part + 1) * LANES]
            value = jnp.dot(n[0, at, :], piece, preferred_element_type=jnp.float32).astype(jnp.bfloat16)
            if part == 0:
                srq0[c, at, lanes(h)] = value
            else:
                srkv0[h, at, lanes(c)] = value

    def send_own(h, c, part):
        out = pl.ds(own, rows)
        if part == 0:
            remote(srq0.at[c, :, lanes(h)], oq.at[out, lanes(h)], oq_s, oq_r.at[core], weight_core(c)).start()
        else:
            remote(srkv0.at[h, :, lanes(c)], okv.at[h, out, lanes(c)], okv_s, okv_r, weight_peer).start()

    local_chunks = rows // OWN_ROWS
    steps = 2 * W_BLOCKS
    for step in range(steps):
        part, r = divmod(step, W_BLOCKS)
        piece = at_rows(w_parts[part], part, r)
        remote(piece, piece, wx_s, wx_r.at[part, r], weight_peer).wait_recv()
        remote(piece, piece, wg_s, wg_r, group_peer).start()
        remote(piece, piece, wd_s.at[0], wd_r.at[0], partner).start()
        if r == W_BLOCKS - 1:
            own_part(half, core, part)
            send_own(half, core, part)
        for i in range(step * local_chunks // steps, (step + 1) * local_chunks // steps):
            own_rows(i * OWN_ROWS, OWN_ROWS, pl.ds(i * OWN_ROWS, OWN_ROWS))

    def own_products(h, c):
        @pl.loop(0, rows // OWN_ROWS)
        def _(i):
            at = pl.ds(pl.multiple_of(i * OWN_ROWS, OWN_ROWS), OWN_ROWS)
            both = product(n, w, 0, at, 1, h, c)
            srq0[c, at, lanes(h)] = both[:, :LANES]
            srkv0[h, at, lanes(c)] = both[:, LANES:]
        for part in range(2):
            send_own(h, c, part)

    other_half = 1 - half
    from_partner = w.at[1, half, other_core]
    remote(from_partner, from_partner, wd_s.at[0], wd_r.at[0], partner).wait_recv()
    own_products(half, other_core)
    from_group = w.at[1, other_half, core]
    remote(from_group, from_group, wg_s, wg_r, group_peer).wait_recv()
    remote(from_group, from_group, wd_s.at[1], wd_r.at[1], partner).start()
    own_products(other_half, core)
    from_both = w.at[1, other_half, other_core]
    remote(from_both, from_both, wd_s.at[1], wd_r.at[1], partner).wait_recv()
    own_products(other_half, other_core)

    @pl.loop(0, EARLY)
    def _(j):
        send_n(j).wait_recv()
        start = pl.multiple_of(j * CHUNK, CHUNK)
        stage = pl.ds(pl.multiple_of(rows + start, CHUNK), CHUNK)
        local_products(me, n, w, oq, okv, slq, 1, near, start, CHUNK, stage, (lq_s.at[1], lq_r.at[1]), (lkv_s.at[1], lkv_r.at[1]))

    @pl.when(core == 1)
    def _():
        early_products(me, n, w, oq, okv, srq, srkv, ek_s, ek_r, eq_s, eq_r)

    for c in range(2):
        arrive(oq.at[pl.ds(me.block(c, me.weight_chip), rows)], oq_r.at[c], weight_peer)
    beside = okv.at[:, pl.ds(me.block(core, me.weight_chip), rows)]
    arrive(beside, okv_r, weight_peer)
    remote(beside, beside, fk_s, fk_r, partner).start()
    for i, (on_chip, size) in enumerate(((me.chip, rows), (me.token_chip, EARLY * CHUNK))):
        theirs = pl.ds(me.block(other_core, on_chip), size)
        mine = pl.ds(0, size)
        arrive(oq.at[theirs], lq_r.at[i], partner)
        arrive(okv.at[:, theirs], lkv_r.at[i], partner)
        sent(slq.at[mine], lq_s.at[i], partner)
        sent(okv.at[:, mine], lkv_s.at[i], partner)
    @pl.loop(EARLY, sends)
    def _(j):
        send_n(j).wait_recv()

    for i in range(2):
        @pl.when(core == i)
        def _():
            sent(n.at[0, pl.ds(0, (EARLY_SENDS + 2 * i) * CHUNK)], n_s, token_peer)
    sent(own_w, wl_s, partner)
    sent(w.at[1, 0, 0], wx_s, weight_peer)
    sent(w.at[1, 0, 0], wg_s, group_peer)
    for i in range(2):
        sent(w.at[1, 0, 0], wd_s.at[i], partner)
    sent(srq0, oq_s, weight_peer)
    sent(srkv0, okv_s, weight_peer)

    @pl.when(core == 1)
    def _():
        finish_early(me, oq, okv, srq, srkv, ek_s, ek_r, eq_s, eq_r)

    sent(beside, fk_s, partner)
    arrive(okv.at[:, pl.ds(me.block(other_core, me.weight_chip), rows)], fk_r, partner)


def second_exchange(chips, w, written, oq_in, okv_in, n_in, srq_in, oq, okv, n, srq, srkv, slq, n_s, n_r, ek_s, ek_r, eq_s, eq_r, xb_s, xb_r, rq_s, rq_r, rkv_s, rkv_r,
                    lq_s, lq_r, lkv_s, lkv_r, fe_s, fe_r, fk_s, fk_r):
    rows = n.shape[1]
    chunks = rows // CHUNK
    early = EARLY * CHUNK
    late = rows - early
    me = Place(chips, rows)
    core, other_core, partner, weight_peer = me.core, me.other_core, me.partner, me.weight_peer
    near = me.block(core, me.token_chip)
    far = me.block(core, me.far_chip)

    barrier = pltpu.get_barrier_semaphore()
    greet(barrier, (weight_peer, me.token_peer))
    pl.semaphore_wait(barrier, 2 + 2 * core)
    greet(barrier, (partner, me.weight_core(other_core)))

    def send_n(j):
        return remote(n.at[0, chunk_of(j)], n.at[1, chunk_of(j)], n_s, n_r.at[j], me.token_peer)

    @pl.loop(me.sends, chunks)
    def _(j):
        send_n(j).start()

    @pl.when(core == 0)
    def _():
        early_products(me, n, w, oq, okv, srq, srkv, ek_s, ek_r, eq_s, eq_r)
        pl.semaphore_wait(barrier, 2)

    remote(srq.at[other_core, pl.ds(0, early)], oq.at[pl.ds(near, early)], xb_s, xb_r, me.weight_core(other_core)).start()

    @pl.loop(EARLY, chunks)
    def _(j):
        @pl.when(j >= me.sends)
        def _():
            send_n(j).wait_recv()

        start = pl.multiple_of(j * CHUNK, CHUNK)
        at = pl.ds(start, CHUNK)
        out = pl.ds(pl.multiple_of(near + start, CHUNK), CHUNK)
        remote_products(n, w, at, srq, srkv, at)
        remote(srkv.at[:, at], okv.at[:, out], rkv_s, rkv_r.at[j - EARLY], weight_peer).start()
        for c in (1, 0):
            remote(srq.at[c, at], oq.at[out], rq_s, rq_r.at[core], me.weight_core(c)).start()
        stage = pl.ds(pl.multiple_of(start - early, CHUNK), CHUNK)
        local_products(me, n, w, oq, okv, slq, 1, near, start, CHUNK, stage, (lq_s, lq_r), (lkv_s, lkv_r))

    @pl.when(core == 0)
    def _():
        finish_early(me, oq, okv, srq, srkv, ek_s, ek_r, eq_s, eq_r)

    far_early = okv.at[:, pl.ds(far, early)]
    remote(far_early, far_early, fe_s, fe_r, partner).start()
    theirs = pl.ds(pl.multiple_of(me.block(other_core, me.token_chip) + early, CHUNK), late)
    arrive(oq.at[theirs], lq_r, partner)
    arrive(okv.at[:, theirs], lkv_r, partner)
    sent(slq, lq_s, partner)
    sent(okv.at[:, theirs], lkv_s, partner)
    arrive(oq.at[pl.ds(me.block(other_core, me.far_chip), early)], xb_r, weight_peer)
    sent(srq.at[other_core, pl.ds(0, early)], xb_s, weight_peer)
    for i in range(2):
        @pl.when(core == i)
        def _():
            sent(n.at[0, pl.ds((EARLY_SENDS + 2 * i) * CHUNK, rows - (EARLY_SENDS + 2 * i) * CHUNK)], n_s, me.token_peer)

    @pl.loop(EARLY, chunks)
    def _(j):
        piece = okv.at[:, pl.ds(pl.multiple_of(far + j * CHUNK, CHUNK), CHUNK)]
        remote(piece, piece, rkv_s, rkv_r.at[j - EARLY], weight_peer).wait_recv()
        remote(piece, piece, fk_s, fk_r, partner).start()

    tail = pl.ds(early, late)
    sent(srkv.at[:, tail], rkv_s, weight_peer)
    sent(far_early, fe_s, partner)
    sent(srkv.at[:, tail], fk_s, partner)
    arrive(okv.at[:, pl.ds(me.block(other_core, me.far_chip), early)], fe_r, partner)
    arrive(okv.at[:, pl.ds(pl.multiple_of(me.block(other_core, me.far_chip) + early, CHUNK), late)], fk_r, partner)
    sent(srq.at[:, tail], rq_s, weight_peer)
    for c in range(2):
        arrive(oq.at[pl.ds(pl.multiple_of(me.block(c, me.far_chip) + early, CHUNK), late)], rq_r.at[c], weight_peer)


def write_rows(blocks, oq, okv, q, k, v, sems):
    copies = []
    for i, (start, size) in enumerate(blocks):
        at = pl.ds(start, size)
        for a, (src, dst) in enumerate(((oq, q), (okv.at[0], k), (okv.at[1], v))):
            copies.append(pltpu.make_async_copy(src.at[at], dst.at[at], sems.at[i, a]))
    for copy in copies:
        copy.start()
    for copy in copies:
        copy.wait()


def first_write(chips, rows, oq, okv, q, k, v, written, sems):
    me = Place(chips, rows)
    written[...] = jnp.zeros_like(written)
    blocks = [(me.block(0, me.chip), 2 * rows), (me.block(0, me.weight_chip), 2 * rows)]
    blocks += [(me.block(c, me.token_chip), EARLY * CHUNK) for c in range(2)]
    write_rows(blocks, oq, okv, q, k, v, sems)


def last_write(chips, rows, oq, okv, q_in, k_in, v_in, q, k, v, sems):
    me = Place(chips, rows)
    early = EARLY * CHUNK
    blocks = [(me.block(0, me.far_chip), 2 * rows)]
    blocks += [(pl.multiple_of(me.block(c, me.token_chip) + early, CHUNK), rows - early) for c in range(2)]
    write_rows(blocks, oq, okv, q, k, v, sems)


def solution(mesh):
    group_size = mesh.shape["tp"]
    chips = group_size // 2

    def local_step(x_rows, norm_gain, w_q, w_k, w_v):
        rows, depth = x_rows.shape
        head = w_q.shape[2]
        tokens = rows * group_size
        dtype = x_rows.dtype
        any_space = pl.BlockSpec(memory_space=pl.ANY)
        vmem = pl.BlockSpec(memory_space=pltpu.VMEM)
        dma = pltpu.SemaphoreType.DMA
        chunks = rows // CHUNK
        early = EARLY * CHUNK
        oq_type, okv_type = pltpu.VMEM((tokens, head), dtype), pltpu.VMEM((2, tokens, head), dtype)
        n_type, srq_type = pltpu.VMEM((2, rows, depth), dtype), pltpu.VMEM((2, rows, head), dtype)

        def held(*arrays):
            return [pltpu.with_memory_space_constraint(a, pltpu.VMEM) for a in arrays]

        oq, okv, n, w, srq = pl.pallas_call(
            functools.partial(first_exchange, chips),
            out_shape=(oq_type, okv_type, n_type, pltpu.VMEM((2, 2, 2, depth, 2 * LANES), dtype), srq_type),
            in_specs=[any_space] * 5,
            out_specs=(vmem,) * 5,
            scratch_shapes=[
                pltpu.VMEM((depth,), norm_gain.dtype),
                pltpu.VMEM((1, depth), norm_gain.dtype),
                pltpu.VMEM((rows + early, head), dtype),
                pltpu.VMEM((2, rows, head), dtype),
                pltpu.VMEM((2, rows, head), dtype),
                pltpu.VMEM((2, early, head), dtype),
                dma, dma((chunks,)),
                dma((W_BLOCKS,)), dma((3,)), dma, dma,
                dma, dma((2, W_BLOCKS)),
                dma, dma,
                dma((2,)), dma((2,)),
                dma, dma((chunks,)),
                dma, dma((2,)), dma, dma,
                dma((2,)), dma((2,)), dma((2,)), dma((2,)),
                dma, dma, dma, dma, dma, dma,
            ],
            compiler_params=pltpu.CompilerParams(collective_id=0, has_side_effects=True, vmem_limit_bytes=16 * 1024 * 1024),
        )(*[pltpu.with_memory_space_constraint(a, pltpu.HBM) for a in (x_rows, norm_gain, w_q.reshape(depth, head), w_k, w_v)])
        out = jax.ShapeDtypeStruct((tokens, head), dtype)
        q, k, v, written = pl.pallas_call(
            functools.partial(first_write, chips, rows),
            out_shape=(out, out, out, jax.ShapeDtypeStruct((8, LANES), jnp.float32)),
            in_specs=[vmem, vmem],
            out_specs=(any_space, any_space, any_space, vmem),
            scratch_shapes=[dma((4, 3))],
            compiler_params=pltpu.CompilerParams(vmem_limit_bytes=1024 * 1024),
        )(*held(oq, okv))
        oq, okv, _, _ = pl.pallas_call(
            functools.partial(second_exchange, chips),
            out_shape=(oq_type, okv_type, n_type, srq_type),
            in_specs=[vmem, any_space, vmem, vmem, vmem, vmem],
            out_specs=(vmem,) * 4,
            input_output_aliases={2: 0, 3: 1, 4: 2, 5: 3},
            scratch_shapes=[
                pltpu.VMEM((2, rows, head), dtype),
                pltpu.VMEM((rows - early, head), dtype),
                dma, dma((chunks,)),
                dma, dma, dma, dma, dma, dma,
                dma, dma((2,)), dma, dma((chunks - EARLY,)),
                dma, dma, dma, dma,
                dma, dma, dma, dma,
            ],
            compiler_params=pltpu.CompilerParams(collective_id=1, has_side_effects=True, vmem_limit_bytes=16 * 1024 * 1024),
        )(*held(w), written, *held(oq, okv, n, srq))
        q, k, v = pl.pallas_call(
            functools.partial(last_write, chips, rows),
            out_shape=(out, out, out),
            in_specs=[vmem, vmem, any_space, any_space, any_space],
            out_specs=(any_space, any_space, any_space),
            input_output_aliases={2: 0, 3: 1, 4: 2},
            scratch_shapes=[dma((3, 3))],
            compiler_params=pltpu.CompilerParams(vmem_limit_bytes=1024 * 1024),
        )(*held(oq, okv), q, k, v)
        return q[:, None, :], k[:, None, :], v[:, None, :]

    return jax.shard_map(local_step, mesh=mesh, in_specs=(P(("dp", "tp"), None), P(None), P(None, "tp", None), P(None, "tp"), P(None, "tp")), out_specs=(P("dp", "tp", None), P("dp", "tp", None), P("dp", "tp", None)), check_vma=False)
```

```python
import functools

import jax
import jax.numpy as jnp
from jax import lax
from jax.experimental import pallas as pl
from jax.experimental.pallas import tpu as pltpu
from jax.sharding import PartitionSpec as P

EPSILON = 1e-6
LANES = 128
NORM_ROWS = 32
CHUNK = 128
EARLY = 5
EARLY_SENDS = 5
OWN_ROWS = 256
W_BLOCKS = 2
W_FIRST = 256
MESH = pl.DeviceIdType.MESH


class Place:
    def __init__(self, chips, rows):
        self.rows = rows
        group = lax.axis_index("dp")
        device = lax.axis_index("tp")
        self.half = lax.rem(group, 2)
        self.core = lax.rem(device, 2)
        self.chip = lax.div(device, 2)
        self.token_chip = chips - 1 - self.chip
        self.weight_chip = self.chip + 1 - 2 * lax.rem(self.chip, 2)
        self.far_chip = chips - 1 - self.weight_chip
        self.other_core = 1 - self.core
        self.partner = {"tp": 2 * self.chip + self.other_core}
        self.token_peer = {"tp": 2 * self.token_chip + self.core}
        self.weight_peer = self.weight_core(self.core)
        self.group_peer = {"dp": group + 1 - 2 * self.half}
        self.follows = lax.div(2 * self.chip, chips) + self.half
        self.sends = EARLY_SENDS + 2 * self.core

    def weight_core(self, c):
        return {"tp": 2 * self.weight_chip + c}

    def block(self, c, on_chip):
        return pl.multiple_of((2 * on_chip + c) * self.rows, self.rows)


def remote(src, dst, send, recv, to):
    return pltpu.make_async_remote_copy(src_ref=src, dst_ref=dst, send_sem=send, recv_sem=recv, device_id=to, device_id_type=MESH)


def arrive(ref, sem, frm):
    remote(ref, ref, sem, sem, frm).wait_recv()


def sent(ref, sem, to):
    remote(ref, ref, sem, sem, to).wait_send()


def lanes(i):
    return pl.ds(pl.multiple_of(i * LANES, LANES), LANES)


def chunk_of(j):
    return pl.ds(pl.multiple_of(j * CHUNK, CHUNK), CHUNK)


def greet(barrier, peers):
    for peer in peers:
        pl.semaphore_signal(barrier, inc=1, device_id=peer, device_id_type=MESH)


def product(n, w, blk, at, side, h, c):
    return jnp.dot(n[blk, at, :], w[side, h, c], preferred_element_type=jnp.float32).astype(jnp.bfloat16)


def local_products(me, n, w, oq, okv, slq, blk, base, start, size, stage, q_sems, kv_sems):
    at = pl.ds(start, size)
    out = pl.ds(pl.multiple_of(base + start, size), size)

    @pl.loop(0, 2)
    def _(h):
        for b in range(2):
            c = lax.rem(me.core + b, 2)
            both = product(n, w, blk, at, 0, h, c)
            if b == 0:
                oq[out, lanes(h)] = both[:, :LANES]
            else:
                slq[stage, lanes(h)] = both[:, :LANES]
            okv[h, out, lanes(c)] = both[:, LANES:]
    remote(slq.at[stage], oq.at[out], *q_sems, me.partner).start()
    remote(okv.at[:, out], okv.at[:, out], *kv_sems, me.partner).start()


def remote_products(n, w, at, srq, srkv, stage):
    @pl.loop(0, 2)
    def _(h):
        for c in range(2):
            both = product(n, w, 1, at, 1, h, c)
            srq[c, at, lanes(h)] = both[:, :LANES]
            srkv[h, stage, lanes(c)] = both[:, LANES:]


def send_early(me, at, oq, okv, srq, srkv, ek_s, ek_r, eq_s, eq_r):
    out = pl.ds(pl.multiple_of(me.block(me.core, me.token_chip) + at.start, CHUNK), at.size)
    remote(srkv.at[:, at], okv.at[:, out], ek_s, ek_r, me.weight_peer).start()
    remote(srq.at[me.core, at], oq.at[out], eq_s, eq_r, me.weight_peer).start()


def finish_early(me, oq, okv, srq, srkv, ek_s, ek_r, eq_s, eq_r):
    at = pl.ds(0, EARLY * CHUNK)
    out = pl.ds(me.block(me.core, me.far_chip), EARLY * CHUNK)
    sent(srkv.at[:, at], ek_s, me.weight_peer)
    sent(srq.at[me.core, at], eq_s, me.weight_peer)
    arrive(okv.at[:, out], ek_r, me.weight_peer)
    arrive(oq.at[out], eq_r, me.weight_peer)


def first_exchange(chips, x, gain, wq, wk, wv, oq, okv, n, w, srq, srkv, gain_copy, gain_row, slq, srq0, srkv0, g_sem, x_sem, w0_sem, wl_sem, wl_s, wl_r,
                   wx_s, wx_r, wg_s, wg_r, wd_s, wd_r, n_s, n_r, oq_s, oq_r, okv_s, okv_r, lq_s, lq_r, lkv_s, lkv_r, fk_s, fk_r, ek_s, ek_r, eq_s, eq_r):
    rows, depth = x.shape
    chunks = rows // CHUNK
    me = Place(chips, rows)
    half, core, other_core = me.half, me.core, me.other_core
    partner, token_peer, weight_peer, group_peer = me.partner, me.token_peer, me.weight_peer, me.group_peer
    weight_core, follows, sends = me.weight_core, me.follows, me.sends

    def load_x(j):
        return pltpu.make_async_copy(x.at[chunk_of(j)], n.at[0, chunk_of(j)], x_sem.at[j])

    q_half = [wq.at[:, pl.ds(h * LANES, LANES)] for h in range(2)]
    kv = [wk, wv]

    def own_w_part(h, part):
        return w.at[0, h, core, :, pl.ds(part * LANES, LANES)]

    cuts = ((0, W_FIRST, depth), (0, depth // 2, depth))

    def at_rows(ref, part, r):
        return ref.at[pl.ds(cuts[part][r], cuts[part][r + 1] - cuts[part][r])]

    barrier = pltpu.get_barrier_semaphore()

    first = own_w_part(half, 0)
    first_src = wq.at[:, pl.ds(pl.multiple_of(half * LANES, LANES), LANES)]
    for r in range(W_BLOCKS):
        pltpu.make_async_copy(at_rows(first_src, 0, r), at_rows(first, 0, r), w0_sem.at[r]).start()
    greet(barrier, (partner, weight_peer, weight_core(other_core)))
    second = own_w_part(1 - half, 0)
    pltpu.make_async_copy(wq.at[:, pl.ds(pl.multiple_of((1 - half) * LANES, LANES), LANES)], second, wl_sem.at[0]).start()
    for h in range(2):
        pltpu.make_async_copy(kv[h], own_w_part(h, 1), wl_sem.at[1 + h]).start()
    gain_load = pltpu.make_async_copy(gain, gain_copy, g_sem)
    gain_load.start()
    for j in range(chunks):
        load_x(j).start()
    pl.semaphore_wait(barrier, 3 + follows)
    greet(barrier, (token_peer, group_peer))

    w_parts = [w.at[1, half, core, :, pl.ds(part * LANES, LANES)] for part in range(2)]
    for r in range(W_BLOCKS):
        pltpu.make_async_copy(at_rows(first, 0, r), at_rows(first, 0, r), w0_sem.at[r]).wait()
        remote(at_rows(first, 0, r), at_rows(w_parts[0], 0, r), wx_s, wx_r.at[0, r], weight_peer).start()
    for h in range(2):
        @pl.when(half == h)
        def _():
            for r in range(W_BLOCKS):
                remote(at_rows(kv[h], 1, r), at_rows(w_parts[1], 1, r), wx_s, wx_r.at[1, r], weight_peer).start()
    for h in range(2):
        for part, src in enumerate((q_half[h], kv[h])):
            remote(src, own_w_part(h, part), wl_s, wl_r, partner).start()
    gain_load.wait()
    gain_row[...] = gain_copy[...].reshape(1, depth)

    def send_n(j):
        return remote(n.at[0, chunk_of(j)], n.at[1, chunk_of(j)], n_s, n_r.at[j], token_peer)

    @pl.loop(0, chunks)
    def _(j):
        load_x(j).wait()

        @pl.loop(0, CHUNK // NORM_ROWS)
        def _(i):
            at = pl.ds(pl.multiple_of(j * CHUNK + i * NORM_ROWS, NORM_ROWS), NORM_ROWS)
            wide = n[0, at, :].astype(jnp.float32)
            mean_sq = jnp.mean(wide * wide, axis=-1, keepdims=True)
            n[0, at, :] = (wide * lax.rsqrt(mean_sq + EPSILON) * gain_row[...]).astype(jnp.bfloat16)

        @pl.when(jnp.logical_and(j == 0, follows < 2))
        def _():
            pl.semaphore_wait(barrier, 2 - follows)

        @pl.when(j < sends)
        def _():
            send_n(j).start()

    own = me.block(core, me.chip)
    near = me.block(core, me.token_chip)

    def own_rows(start, size, stage):
        local_products(me, n, w, oq, okv, slq, 0, own, start, size, stage, (lq_s.at[0], lq_r.at[0]), (lkv_s.at[0], lkv_r.at[0]))

    own_w = w.at[0, :, core]
    pltpu.make_async_copy(second, second, wl_sem.at[0]).wait()
    for h in range(2):
        pltpu.make_async_copy(kv[h], own_w_part(h, 1), wl_sem.at[1 + h]).wait()
    other_w = w.at[0, :, other_core]
    remote(other_w, other_w, wl_s, wl_r, partner).wait_recv()

    def own_part(h, c, part):
        @pl.loop(0, rows // OWN_ROWS)
        def _(i):
            at = pl.ds(pl.multiple_of(i * OWN_ROWS, OWN_ROWS), OWN_ROWS)
            piece = w[1, h, c, :, part * LANES:(part + 1) * LANES]
            value = jnp.dot(n[0, at, :], piece, preferred_element_type=jnp.float32).astype(jnp.bfloat16)
            if part == 0:
                srq0[c, at, lanes(h)] = value
            else:
                srkv0[h, at, lanes(c)] = value

    def send_own(h, c, part):
        out = pl.ds(own, rows)
        if part == 0:
            remote(srq0.at[c, :, lanes(h)], oq.at[out, lanes(h)], oq_s, oq_r.at[core], weight_core(c)).start()
        else:
            remote(srkv0.at[h, :, lanes(c)], okv.at[h, out, lanes(c)], okv_s, okv_r, weight_peer).start()

    local_chunks = rows // OWN_ROWS
    steps = 2 * W_BLOCKS
    for step in range(steps):
        part, r = divmod(step, W_BLOCKS)
        piece = at_rows(w_parts[part], part, r)
        remote(piece, piece, wx_s, wx_r.at[part, r], weight_peer).wait_recv()
        remote(piece, piece, wg_s, wg_r, group_peer).start()
        remote(piece, piece, wd_s.at[0], wd_r.at[0], partner).start()
        if r == W_BLOCKS - 1:
            own_part(half, core, part)
            send_own(half, core, part)
        for i in range(step * local_chunks // steps, (step + 1) * local_chunks // steps):
            own_rows(i * OWN_ROWS, OWN_ROWS, pl.ds(i * OWN_ROWS, OWN_ROWS))

    def own_products(h, c):
        @pl.loop(0, rows // OWN_ROWS)
        def _(i):
            at = pl.ds(pl.multiple_of(i * OWN_ROWS, OWN_ROWS), OWN_ROWS)
            both = product(n, w, 0, at, 1, h, c)
            srq0[c, at, lanes(h)] = both[:, :LANES]
            srkv0[h, at, lanes(c)] = both[:, LANES:]
        for part in range(2):
            send_own(h, c, part)

    other_half = 1 - half
    from_partner = w.at[1, half, other_core]
    remote(from_partner, from_partner, wd_s.at[0], wd_r.at[0], partner).wait_recv()
    own_products(half, other_core)
    from_group = w.at[1, other_half, core]
    remote(from_group, from_group, wg_s, wg_r, group_peer).wait_recv()
    remote(from_group, from_group, wd_s.at[1], wd_r.at[1], partner).start()
    own_products(other_half, core)
    from_both = w.at[1, other_half, other_core]
    remote(from_both, from_both, wd_s.at[1], wd_r.at[1], partner).wait_recv()
    own_products(other_half, other_core)

    @pl.loop(0, EARLY)
    def _(j):
        send_n(j).wait_recv()
        start = pl.multiple_of(j * CHUNK, CHUNK)
        stage = pl.ds(pl.multiple_of(rows + start, CHUNK), CHUNK)
        at = chunk_of(j)
        remote_products(n, w, at, srq, srkv, at)

        @pl.when(core == 1)
        def _():
            send_early(me, at, oq, okv, srq, srkv, ek_s, ek_r, eq_s, eq_r)

        local_products(me, n, w, oq, okv, slq, 1, near, start, CHUNK, stage, (lq_s.at[1], lq_r.at[1]), (lkv_s.at[1], lkv_r.at[1]))

    for c in range(2):
        arrive(oq.at[pl.ds(me.block(c, me.weight_chip), rows)], oq_r.at[c], weight_peer)
    beside = okv.at[:, pl.ds(me.block(core, me.weight_chip), rows)]
    arrive(beside, okv_r, weight_peer)
    remote(beside, beside, fk_s, fk_r, partner).start()
    for i, (on_chip, size) in enumerate(((me.chip, rows), (me.token_chip, EARLY * CHUNK))):
        theirs = pl.ds(me.block(other_core, on_chip), size)
        mine = pl.ds(0, size)
        arrive(oq.at[theirs], lq_r.at[i], partner)
        arrive(okv.at[:, theirs], lkv_r.at[i], partner)
        sent(slq.at[mine], lq_s.at[i], partner)
        sent(okv.at[:, mine], lkv_s.at[i], partner)
    @pl.loop(EARLY, sends)
    def _(j):
        send_n(j).wait_recv()

    for i in range(2):
        @pl.when(core == i)
        def _():
            sent(n.at[0, pl.ds(0, (EARLY_SENDS + 2 * i) * CHUNK)], n_s, token_peer)
    sent(own_w, wl_s, partner)
    sent(w.at[1, 0, 0], wx_s, weight_peer)
    sent(w.at[1, 0, 0], wg_s, group_peer)
    for i in range(2):
        sent(w.at[1, 0, 0], wd_s.at[i], partner)
    sent(srq0, oq_s, weight_peer)
    sent(srkv0, okv_s, weight_peer)

    @pl.when(core == 1)
    def _():
        finish_early(me, oq, okv, srq, srkv, ek_s, ek_r, eq_s, eq_r)

    sent(beside, fk_s, partner)
    arrive(okv.at[:, pl.ds(me.block(other_core, me.weight_chip), rows)], fk_r, partner)


def second_exchange(chips, w, srkv_early, written, oq_in, okv_in, n_in, srq_in, oq, okv, n, srq, srkv, slq, n_s, n_r, ek_s, ek_r, eq_s, eq_r, xb_s, xb_r, rq_s, rq_r, rkv_s, rkv_r,
                    lq_s, lq_r, lkv_s, lkv_r, fe_s, fe_r, fk_s, fk_r):
    rows = n.shape[1]
    chunks = rows // CHUNK
    early = EARLY * CHUNK
    late = rows - early
    me = Place(chips, rows)
    core, other_core, partner, weight_peer = me.core, me.other_core, me.partner, me.weight_peer
    near = me.block(core, me.token_chip)
    far = me.block(core, me.far_chip)

    barrier = pltpu.get_barrier_semaphore()
    greet(barrier, (weight_peer, me.token_peer))
    pl.semaphore_wait(barrier, 2 + 2 * core)
    greet(barrier, (partner, me.weight_core(other_core)))

    def send_n(j):
        return remote(n.at[0, chunk_of(j)], n.at[1, chunk_of(j)], n_s, n_r.at[j], me.token_peer)

    @pl.loop(me.sends, chunks)
    def _(j):
        send_n(j).start()

    @pl.when(core == 0)
    def _():
        send_early(me, pl.ds(0, early), oq, okv, srq, srkv_early, ek_s, ek_r, eq_s, eq_r)
        pl.semaphore_wait(barrier, 2)

    remote(srq.at[other_core, pl.ds(0, early)], oq.at[pl.ds(near, early)], xb_s, xb_r, me.weight_core(other_core)).start()

    @pl.loop(EARLY, chunks)
    def _(j):
        @pl.when(j >= me.sends)
        def _():
            send_n(j).wait_recv()

        start = pl.multiple_of(j * CHUNK, CHUNK)
        at = pl.ds(start, CHUNK)
        out = pl.ds(pl.multiple_of(near + start, CHUNK), CHUNK)
        remote_products(n, w, at, srq, srkv, at)
        remote(srkv.at[:, at], okv.at[:, out], rkv_s, rkv_r.at[j - EARLY], weight_peer).start()
        for c in (1, 0):
            remote(srq.at[c, at], oq.at[out], rq_s, rq_r.at[core], me.weight_core(c)).start()
        stage = pl.ds(pl.multiple_of(start - early, CHUNK), CHUNK)
        local_products(me, n, w, oq, okv, slq, 1, near, start, CHUNK, stage, (lq_s, lq_r), (lkv_s, lkv_r))

    @pl.when(core == 0)
    def _():
        finish_early(me, oq, okv, srq, srkv_early, ek_s, ek_r, eq_s, eq_r)

    far_early = okv.at[:, pl.ds(far, early)]
    remote(far_early, far_early, fe_s, fe_r, partner).start()
    theirs = pl.ds(pl.multiple_of(me.block(other_core, me.token_chip) + early, CHUNK), late)
    arrive(oq.at[theirs], lq_r, partner)
    arrive(okv.at[:, theirs], lkv_r, partner)
    sent(slq, lq_s, partner)
    sent(okv.at[:, theirs], lkv_s, partner)
    arrive(oq.at[pl.ds(me.block(other_core, me.far_chip), early)], xb_r, weight_peer)
    sent(srq.at[other_core, pl.ds(0, early)], xb_s, weight_peer)
    for i in range(2):
        @pl.when(core == i)
        def _():
            sent(n.at[0, pl.ds((EARLY_SENDS + 2 * i) * CHUNK, rows - (EARLY_SENDS + 2 * i) * CHUNK)], n_s, me.token_peer)

    @pl.loop(EARLY, chunks)
    def _(j):
        piece = okv.at[:, pl.ds(pl.multiple_of(far + j * CHUNK, CHUNK), CHUNK)]
        remote(piece, piece, rkv_s, rkv_r.at[j - EARLY], weight_peer).wait_recv()
        remote(piece, piece, fk_s, fk_r, partner).start()

    tail = pl.ds(early, late)
    sent(srkv.at[:, tail], rkv_s, weight_peer)
    sent(far_early, fe_s, partner)
    sent(srkv.at[:, tail], fk_s, partner)
    arrive(okv.at[:, pl.ds(me.block(other_core, me.far_chip), early)], fe_r, partner)
    arrive(okv.at[:, pl.ds(pl.multiple_of(me.block(other_core, me.far_chip) + early, CHUNK), late)], fk_r, partner)
    sent(srq.at[:, tail], rq_s, weight_peer)
    for c in range(2):
        arrive(oq.at[pl.ds(pl.multiple_of(me.block(c, me.far_chip) + early, CHUNK), late)], rq_r.at[c], weight_peer)


def write_rows(blocks, oq, okv, q, k, v, sems):
    copies = []
    for i, (start, size) in enumerate(blocks):
        at = pl.ds(start, size)
        for a, (src, dst) in enumerate(((oq, q), (okv.at[0], k), (okv.at[1], v))):
            copies.append(pltpu.make_async_copy(src.at[at], dst.at[at], sems.at[i, a]))
    for copy in copies:
        copy.start()
    for copy in copies:
        copy.wait()


def first_write(chips, rows, oq, okv, q, k, v, written, sems):
    me = Place(chips, rows)
    written[...] = jnp.zeros_like(written)
    blocks = [(me.block(0, me.chip), 2 * rows), (me.block(0, me.weight_chip), 2 * rows)]
    blocks += [(me.block(c, me.token_chip), EARLY * CHUNK) for c in range(2)]
    write_rows(blocks, oq, okv, q, k, v, sems)


def last_write(chips, rows, oq, okv, q_in, k_in, v_in, q, k, v, sems):
    me = Place(chips, rows)
    early = EARLY * CHUNK
    blocks = [(me.block(0, me.far_chip), 2 * rows)]
    blocks += [(pl.multiple_of(me.block(c, me.token_chip) + early, CHUNK), rows - early) for c in range(2)]
    write_rows(blocks, oq, okv, q, k, v, sems)


def solution(mesh):
    group_size = mesh.shape["tp"]
    chips = group_size // 2

    def local_step(x_rows, norm_gain, w_q, w_k, w_v):
        rows, depth = x_rows.shape
        head = w_q.shape[2]
        tokens = rows * group_size
        dtype = x_rows.dtype
        any_space = pl.BlockSpec(memory_space=pl.ANY)
        vmem = pl.BlockSpec(memory_space=pltpu.VMEM)
        dma = pltpu.SemaphoreType.DMA
        chunks = rows // CHUNK
        early = EARLY * CHUNK
        oq_type, okv_type = pltpu.VMEM((tokens, head), dtype), pltpu.VMEM((2, tokens, head), dtype)
        n_type, srq_type = pltpu.VMEM((2, rows, depth), dtype), pltpu.VMEM((2, rows, head), dtype)

        def held(*arrays):
            return [pltpu.with_memory_space_constraint(a, pltpu.VMEM) for a in arrays]

        oq, okv, n, w, srq, srkv = pl.pallas_call(
            functools.partial(first_exchange, chips),
            out_shape=(oq_type, okv_type, n_type, pltpu.VMEM((2, 2, 2, depth, 2 * LANES), dtype), srq_type, pltpu.VMEM((2, early, head), dtype)),
            in_specs=[any_space] * 5,
            out_specs=(vmem,) * 6,
            scratch_shapes=[
                pltpu.VMEM((depth,), norm_gain.dtype),
                pltpu.VMEM((1, depth), norm_gain.dtype),
                pltpu.VMEM((rows + early, head), dtype),
                pltpu.VMEM((2, rows, head), dtype),
                pltpu.VMEM((2, rows, head), dtype),
                dma, dma((chunks,)),
                dma((W_BLOCKS,)), dma((3,)), dma, dma,
                dma, dma((2, W_BLOCKS)),
                dma, dma,
                dma((2,)), dma((2,)),
                dma, dma((chunks,)),
                dma, dma((2,)), dma, dma,
                dma((2,)), dma((2,)), dma((2,)), dma((2,)),
                dma, dma, dma, dma, dma, dma,
            ],
            compiler_params=pltpu.CompilerParams(collective_id=0, has_side_effects=True, vmem_limit_bytes=16 * 1024 * 1024),
        )(*[pltpu.with_memory_space_constraint(a, pltpu.HBM) for a in (x_rows, norm_gain, w_q.reshape(depth, head), w_k, w_v)])
        out = jax.ShapeDtypeStruct((tokens, head), dtype)
        q, k, v, written = pl.pallas_call(
            functools.partial(first_write, chips, rows),
            out_shape=(out, out, out, jax.ShapeDtypeStruct((8, LANES), jnp.float32)),
            in_specs=[vmem, vmem],
            out_specs=(any_space, any_space, any_space, vmem),
            scratch_shapes=[dma((4, 3))],
            compiler_params=pltpu.CompilerParams(vmem_limit_bytes=1024 * 1024),
        )(*held(oq, okv))
        oq, okv, _, _ = pl.pallas_call(
            functools.partial(second_exchange, chips),
            out_shape=(oq_type, okv_type, n_type, srq_type),
            in_specs=[vmem, vmem, any_space, vmem, vmem, vmem, vmem],
            out_specs=(vmem,) * 4,
            input_output_aliases={3: 0, 4: 1, 5: 2, 6: 3},
            scratch_shapes=[
                pltpu.VMEM((2, rows, head), dtype),
                pltpu.VMEM((rows - early, head), dtype),
                dma, dma((chunks,)),
                dma, dma, dma, dma, dma, dma,
                dma, dma((2,)), dma, dma((chunks - EARLY,)),
                dma, dma, dma, dma,
                dma, dma, dma, dma,
            ],
            compiler_params=pltpu.CompilerParams(collective_id=1, has_side_effects=True, vmem_limit_bytes=16 * 1024 * 1024),
        )(*held(w, srkv), written, *held(oq, okv, n, srq))
        q, k, v = pl.pallas_call(
            functools.partial(last_write, chips, rows),
            out_shape=(out, out, out),
            in_specs=[vmem, vmem, any_space, any_space, any_space],
            out_specs=(any_space, any_space, any_space),
            input_output_aliases={2: 0, 3: 1, 4: 2},
            scratch_shapes=[dma((3, 3))],
            compiler_params=pltpu.CompilerParams(vmem_limit_bytes=1024 * 1024),
        )(*held(oq, okv), q, k, v)
        return q[:, None, :], k[:, None, :], v[:, None, :]

    return jax.shard_map(local_step, mesh=mesh, in_specs=(P(("dp", "tp"), None), P(None), P(None, "tp", None), P(None, "tp"), P(None, "tp")), out_specs=(P("dp", "tp", None), P("dp", "tp", None), P("dp", "tp", None)), check_vma=False)
```

```python
import functools

import jax
import jax.numpy as jnp
from jax import lax
from jax.experimental import pallas as pl
from jax.experimental.pallas import tpu as pltpu
from jax.sharding import PartitionSpec as P

EPSILON = 1e-6
LANES = 128
NORM_ROWS = 32
CHUNK = 128
EARLY = 5
EARLY_SENDS = 5
MORE_SENDS = 3
OWN_ROWS = 256
W_BLOCKS = 2
W_FIRST = 256
MESH = pl.DeviceIdType.MESH


class Place:
    def __init__(self, chips, rows):
        self.rows = rows
        group = lax.axis_index("dp")
        device = lax.axis_index("tp")
        self.half = lax.rem(group, 2)
        self.core = lax.rem(device, 2)
        self.chip = lax.div(device, 2)
        self.token_chip = chips - 1 - self.chip
        self.weight_chip = self.chip + 1 - 2 * lax.rem(self.chip, 2)
        self.far_chip = chips - 1 - self.weight_chip
        self.other_core = 1 - self.core
        self.partner = {"tp": 2 * self.chip + self.other_core}
        self.token_peer = {"tp": 2 * self.token_chip + self.core}
        self.weight_peer = self.weight_core(self.core)
        self.group_peer = {"dp": group + 1 - 2 * self.half}
        self.follows = lax.div(2 * self.chip, chips) + self.half
        self.sends = EARLY_SENDS + MORE_SENDS * self.core

    def weight_core(self, c):
        return {"tp": 2 * self.weight_chip + c}

    def block(self, c, on_chip):
        return pl.multiple_of((2 * on_chip + c) * self.rows, self.rows)


def remote(src, dst, send, recv, to):
    return pltpu.make_async_remote_copy(src_ref=src, dst_ref=dst, send_sem=send, recv_sem=recv, device_id=to, device_id_type=MESH)


def arrive(ref, sem, frm):
    remote(ref, ref, sem, sem, frm).wait_recv()


def sent(ref, sem, to):
    remote(ref, ref, sem, sem, to).wait_send()


def lanes(i):
    return pl.ds(pl.multiple_of(i * LANES, LANES), LANES)


def chunk_of(j):
    return pl.ds(pl.multiple_of(j * CHUNK, CHUNK), CHUNK)


def greet(barrier, peers):
    for peer in peers:
        pl.semaphore_signal(barrier, inc=1, device_id=peer, device_id_type=MESH)


def product(n, w, blk, at, side, h, c):
    return jnp.dot(n[blk, at, :], w[side, h, c], preferred_element_type=jnp.float32).astype(jnp.bfloat16)


def local_products(me, n, w, oq, okv, slq, blk, base, start, size, stage, q_sems, kv_sems):
    at = pl.ds(start, size)
    out = pl.ds(pl.multiple_of(base + start, size), size)

    @pl.loop(0, 2)
    def _(h):
        for b in range(2):
            c = lax.rem(me.core + b, 2)
            both = product(n, w, blk, at, 0, h, c)
            if b == 0:
                oq[out, lanes(h)] = both[:, :LANES]
            else:
                slq[stage, lanes(h)] = both[:, :LANES]
            okv[h, out, lanes(c)] = both[:, LANES:]
    remote(slq.at[stage], oq.at[out], *q_sems, me.partner).start()
    remote(okv.at[:, out], okv.at[:, out], *kv_sems, me.partner).start()


def remote_products(n, w, at, srq, srkv, stage):
    @pl.loop(0, 2)
    def _(h):
        for c in range(2):
            both = product(n, w, 1, at, 1, h, c)
            srq[c, at, lanes(h)] = both[:, :LANES]
            srkv[h, stage, lanes(c)] = both[:, LANES:]


def send_early(me, at, oq, okv, srq, srkv, ek_s, ek_r, eq_s, eq_r):
    out = pl.ds(pl.multiple_of(me.block(me.core, me.token_chip) + at.start, CHUNK), at.size)
    remote(srkv.at[:, at], okv.at[:, out], ek_s, ek_r, me.weight_peer).start()
    remote(srq.at[me.core, at], oq.at[out], eq_s, eq_r, me.weight_peer).start()


def finish_early(me, oq, okv, srq, srkv, ek_s, ek_r, eq_s, eq_r):
    at = pl.ds(0, EARLY * CHUNK)
    out = pl.ds(me.block(me.core, me.far_chip), EARLY * CHUNK)
    sent(srkv.at[:, at], ek_s, me.weight_peer)
    sent(srq.at[me.core, at], eq_s, me.weight_peer)
    arrive(okv.at[:, out], ek_r, me.weight_peer)
    arrive(oq.at[out], eq_r, me.weight_peer)


def first_exchange(chips, x, gain, wq, wk, wv, oq, okv, n, w, srq, srkv, gain_copy, gain_row, slq, srq0, srkv0, g_sem, x_sem, w0_sem, wl_sem, wl_s, wl_r,
                   wx_s, wx_r, wg_s, wg_r, wd_s, wd_r, n_s, n_r, oq_s, oq_r, okv_s, okv_r, lq_s, lq_r, lkv_s, lkv_r, fk_s, fk_r, ek_s, ek_r, eq_s, eq_r):
    rows, depth = x.shape
    chunks = rows // CHUNK
    me = Place(chips, rows)
    half, core, other_core = me.half, me.core, me.other_core
    partner, token_peer, weight_peer, group_peer = me.partner, me.token_peer, me.weight_peer, me.group_peer
    weight_core, follows, sends = me.weight_core, me.follows, me.sends

    def load_x(j):
        return pltpu.make_async_copy(x.at[chunk_of(j)], n.at[0, chunk_of(j)], x_sem.at[j])

    q_half = [wq.at[:, pl.ds(h * LANES, LANES)] for h in range(2)]
    kv = [wk, wv]

    def own_w_part(h, part):
        return w.at[0, h, core, :, pl.ds(part * LANES, LANES)]

    cuts = ((0, W_FIRST, depth), (0, depth // 2, depth))

    def at_rows(ref, part, r):
        return ref.at[pl.ds(cuts[part][r], cuts[part][r + 1] - cuts[part][r])]

    barrier = pltpu.get_barrier_semaphore()

    first = own_w_part(half, 0)
    first_src = wq.at[:, pl.ds(pl.multiple_of(half * LANES, LANES), LANES)]
    for r in range(W_BLOCKS):
        pltpu.make_async_copy(at_rows(first_src, 0, r), at_rows(first, 0, r), w0_sem.at[r]).start()
    greet(barrier, (partner, weight_peer, weight_core(other_core)))
    second = own_w_part(1 - half, 0)
    pltpu.make_async_copy(wq.at[:, pl.ds(pl.multiple_of((1 - half) * LANES, LANES), LANES)], second, wl_sem.at[0]).start()
    for h in range(2):
        pltpu.make_async_copy(kv[h], own_w_part(h, 1), wl_sem.at[1 + h]).start()
    gain_load = pltpu.make_async_copy(gain, gain_copy, g_sem)
    gain_load.start()
    for j in range(chunks):
        load_x(j).start()
    pl.semaphore_wait(barrier, 3 + follows)
    greet(barrier, (token_peer, group_peer))

    w_parts = [w.at[1, half, core, :, pl.ds(part * LANES, LANES)] for part in range(2)]
    for r in range(W_BLOCKS):
        pltpu.make_async_copy(at_rows(first, 0, r), at_rows(first, 0, r), w0_sem.at[r]).wait()
        remote(at_rows(first, 0, r), at_rows(w_parts[0], 0, r), wx_s, wx_r.at[0, r], weight_peer).start()
    for h in range(2):
        @pl.when(half == h)
        def _():
            for r in range(W_BLOCKS):
                remote(at_rows(kv[h], 1, r), at_rows(w_parts[1], 1, r), wx_s, wx_r.at[1, r], weight_peer).start()
    for h in range(2):
        for part, src in enumerate((q_half[h], kv[h])):
            remote(src, own_w_part(h, part), wl_s, wl_r, partner).start()
    gain_load.wait()
    gain_row[...] = gain_copy[...].reshape(1, depth)

    def send_n(j):
        return remote(n.at[0, chunk_of(j)], n.at[1, chunk_of(j)], n_s, n_r.at[j], token_peer)

    @pl.loop(0, chunks)
    def _(j):
        load_x(j).wait()

        @pl.loop(0, CHUNK // NORM_ROWS)
        def _(i):
            at = pl.ds(pl.multiple_of(j * CHUNK + i * NORM_ROWS, NORM_ROWS), NORM_ROWS)
            wide = n[0, at, :].astype(jnp.float32)
            mean_sq = jnp.mean(wide * wide, axis=-1, keepdims=True)
            n[0, at, :] = (wide * lax.rsqrt(mean_sq + EPSILON) * gain_row[...]).astype(jnp.bfloat16)

        @pl.when(jnp.logical_and(j == 0, follows < 2))
        def _():
            pl.semaphore_wait(barrier, 2 - follows)

        @pl.when(j < sends)
        def _():
            send_n(j).start()

    own = me.block(core, me.chip)
    near = me.block(core, me.token_chip)

    def own_rows(start, size, stage):
        local_products(me, n, w, oq, okv, slq, 0, own, start, size, stage, (lq_s.at[0], lq_r.at[0]), (lkv_s.at[0], lkv_r.at[0]))

    own_w = w.at[0, :, core]
    pltpu.make_async_copy(second, second, wl_sem.at[0]).wait()
    for h in range(2):
        pltpu.make_async_copy(kv[h], own_w_part(h, 1), wl_sem.at[1 + h]).wait()
    other_w = w.at[0, :, other_core]
    remote(other_w, other_w, wl_s, wl_r, partner).wait_recv()

    def own_part(h, c, part):
        @pl.loop(0, rows // OWN_ROWS)
        def _(i):
            at = pl.ds(pl.multiple_of(i * OWN_ROWS, OWN_ROWS), OWN_ROWS)
            piece = w[1, h, c, :, part * LANES:(part + 1) * LANES]
            value = jnp.dot(n[0, at, :], piece, preferred_element_type=jnp.float32).astype(jnp.bfloat16)
            if part == 0:
                srq0[c, at, lanes(h)] = value
            else:
                srkv0[h, at, lanes(c)] = value

    def send_own(h, c, part):
        out = pl.ds(own, rows)
        if part == 0:
            remote(srq0.at[c, :, lanes(h)], oq.at[out, lanes(h)], oq_s, oq_r.at[core], weight_core(c)).start()
        else:
            remote(srkv0.at[h, :, lanes(c)], okv.at[h, out, lanes(c)], okv_s, okv_r, weight_peer).start()

    local_chunks = rows // OWN_ROWS
    steps = 2 * W_BLOCKS
    for step in range(steps):
        part, r = divmod(step, W_BLOCKS)
        piece = at_rows(w_parts[part], part, r)
        remote(piece, piece, wx_s, wx_r.at[part, r], weight_peer).wait_recv()
        remote(piece, piece, wg_s, wg_r, group_peer).start()
        remote(piece, piece, wd_s.at[0], wd_r.at[0], partner).start()
        if r == W_BLOCKS - 1:
            own_part(half, core, part)
            send_own(half, core, part)
        for i in range(step * local_chunks // steps, (step + 1) * local_chunks // steps):
            own_rows(i * OWN_ROWS, OWN_ROWS, pl.ds(i * OWN_ROWS, OWN_ROWS))

    def own_products(h, c):
        @pl.loop(0, rows // OWN_ROWS)
        def _(i):
            at = pl.ds(pl.multiple_of(i * OWN_ROWS, OWN_ROWS), OWN_ROWS)
            both = product(n, w, 0, at, 1, h, c)
            srq0[c, at, lanes(h)] = both[:, :LANES]
            srkv0[h, at, lanes(c)] = both[:, LANES:]
        for part in range(2):
            send_own(h, c, part)

    other_half = 1 - half
    from_partner = w.at[1, half, other_core]
    remote(from_partner, from_partner, wd_s.at[0], wd_r.at[0], partner).wait_recv()
    own_products(half, other_core)
    from_group = w.at[1, other_half, core]
    remote(from_group, from_group, wg_s, wg_r, group_peer).wait_recv()
    remote(from_group, from_group, wd_s.at[1], wd_r.at[1], partner).start()
    own_products(other_half, core)
    from_both = w.at[1, other_half, other_core]
    remote(from_both, from_both, wd_s.at[1], wd_r.at[1], partner).wait_recv()
    own_products(other_half, other_core)

    @pl.loop(0, EARLY)
    def _(j):
        send_n(j).wait_recv()
        start = pl.multiple_of(j * CHUNK, CHUNK)
        stage = pl.ds(pl.multiple_of(rows + start, CHUNK), CHUNK)
        at = chunk_of(j)
        remote_products(n, w, at, srq, srkv, at)

        @pl.when(core == 1)
        def _():
            send_early(me, at, oq, okv, srq, srkv, ek_s, ek_r, eq_s, eq_r)

        local_products(me, n, w, oq, okv, slq, 1, near, start, CHUNK, stage, (lq_s.at[1], lq_r.at[1]), (lkv_s.at[1], lkv_r.at[1]))

    for c in range(2):
        arrive(oq.at[pl.ds(me.block(c, me.weight_chip), rows)], oq_r.at[c], weight_peer)
    beside = okv.at[:, pl.ds(me.block(core, me.weight_chip), rows)]
    arrive(beside, okv_r, weight_peer)
    remote(beside, beside, fk_s, fk_r, partner).start()
    for i, (on_chip, size) in enumerate(((me.chip, rows), (me.token_chip, EARLY * CHUNK))):
        theirs = pl.ds(me.block(other_core, on_chip), size)
        mine = pl.ds(0, size)
        arrive(oq.at[theirs], lq_r.at[i], partner)
        arrive(okv.at[:, theirs], lkv_r.at[i], partner)
        sent(slq.at[mine], lq_s.at[i], partner)
        sent(okv.at[:, mine], lkv_s.at[i], partner)
    @pl.loop(EARLY, sends)
    def _(j):
        send_n(j).wait_recv()

    for i in range(2):
        @pl.when(core == i)
        def _():
            sent(n.at[0, pl.ds(0, (EARLY_SENDS + MORE_SENDS * i) * CHUNK)], n_s, token_peer)
    sent(own_w, wl_s, partner)
    sent(w.at[1, 0, 0], wx_s, weight_peer)
    sent(w.at[1, 0, 0], wg_s, group_peer)
    for i in range(2):
        sent(w.at[1, 0, 0], wd_s.at[i], partner)
    sent(srq0, oq_s, weight_peer)
    sent(srkv0, okv_s, weight_peer)

    @pl.when(core == 1)
    def _():
        finish_early(me, oq, okv, srq, srkv, ek_s, ek_r, eq_s, eq_r)

    sent(beside, fk_s, partner)
    arrive(okv.at[:, pl.ds(me.block(other_core, me.weight_chip), rows)], fk_r, partner)


def second_exchange(chips, w, srkv_early, written, oq_in, okv_in, n_in, srq_in, oq, okv, n, srq, srkv, slq, n_s, n_r, ek_s, ek_r, eq_s, eq_r, xb_s, xb_r, rq_s, rq_r, rkv_s, rkv_r,
                    lq_s, lq_r, lkv_s, lkv_r, fe_s, fe_r, fk_s, fk_r):
    rows = n.shape[1]
    chunks = rows // CHUNK
    early = EARLY * CHUNK
    late = rows - early
    me = Place(chips, rows)
    core, other_core, partner, weight_peer = me.core, me.other_core, me.partner, me.weight_peer
    near = me.block(core, me.token_chip)
    far = me.block(core, me.far_chip)

    barrier = pltpu.get_barrier_semaphore()
    greet(barrier, (weight_peer, me.token_peer))
    pl.semaphore_wait(barrier, 2 + 2 * core)
    greet(barrier, (partner, me.weight_core(other_core)))

    def send_n(j):
        return remote(n.at[0, chunk_of(j)], n.at[1, chunk_of(j)], n_s, n_r.at[j], me.token_peer)

    @pl.loop(me.sends, chunks)
    def _(j):
        send_n(j).start()

    @pl.when(core == 0)
    def _():
        send_early(me, pl.ds(0, early), oq, okv, srq, srkv_early, ek_s, ek_r, eq_s, eq_r)
        pl.semaphore_wait(barrier, 2)

    remote(srq.at[other_core, pl.ds(0, early)], oq.at[pl.ds(near, early)], xb_s, xb_r, me.weight_core(other_core)).start()

    @pl.loop(EARLY, chunks)
    def _(j):
        @pl.when(j >= me.sends)
        def _():
            send_n(j).wait_recv()

        start = pl.multiple_of(j * CHUNK, CHUNK)
        at = pl.ds(start, CHUNK)
        out = pl.ds(pl.multiple_of(near + start, CHUNK), CHUNK)
        remote_products(n, w, at, srq, srkv, at)
        remote(srkv.at[:, at], okv.at[:, out], rkv_s, rkv_r.at[j - EARLY], weight_peer).start()
        for c in (1, 0):
            remote(srq.at[c, at], oq.at[out], rq_s, rq_r.at[core], me.weight_core(c)).start()
        stage = pl.ds(pl.multiple_of(start - early, CHUNK), CHUNK)
        local_products(me, n, w, oq, okv, slq, 1, near, start, CHUNK, stage, (lq_s, lq_r), (lkv_s, lkv_r))

    @pl.when(core == 0)
    def _():
        finish_early(me, oq, okv, srq, srkv_early, ek_s, ek_r, eq_s, eq_r)

    far_early = okv.at[:, pl.ds(far, early)]
    remote(far_early, far_early, fe_s, fe_r, partner).start()
    theirs = pl.ds(pl.multiple_of(me.block(other_core, me.token_chip) + early, CHUNK), late)
    arrive(oq.at[theirs], lq_r, partner)
    arrive(okv.at[:, theirs], lkv_r, partner)
    sent(slq, lq_s, partner)
    sent(okv.at[:, theirs], lkv_s, partner)
    arrive(oq.at[pl.ds(me.block(other_core, me.far_chip), early)], xb_r, weight_peer)
    sent(srq.at[other_core, pl.ds(0, early)], xb_s, weight_peer)
    for i in range(2):
        gone = (EARLY_SENDS + MORE_SENDS * i) * CHUNK
        if gone < rows:
            @pl.when(core == i)
            def _():
                sent(n.at[0, pl.ds(gone, rows - gone)], n_s, me.token_peer)

    @pl.loop(EARLY, chunks)
    def _(j):
        piece = okv.at[:, pl.ds(pl.multiple_of(far + j * CHUNK, CHUNK), CHUNK)]
        remote(piece, piece, rkv_s, rkv_r.at[j - EARLY], weight_peer).wait_recv()
        remote(piece, piece, fk_s, fk_r, partner).start()

    tail = pl.ds(early, late)
    sent(srkv.at[:, tail], rkv_s, weight_peer)
    sent(far_early, fe_s, partner)
    sent(srkv.at[:, tail], fk_s, partner)
    arrive(okv.at[:, pl.ds(me.block(other_core, me.far_chip), early)], fe_r, partner)
    arrive(okv.at[:, pl.ds(pl.multiple_of(me.block(other_core, me.far_chip) + early, CHUNK), late)], fk_r, partner)
    sent(srq.at[:, tail], rq_s, weight_peer)
    for c in range(2):
        arrive(oq.at[pl.ds(pl.multiple_of(me.block(c, me.far_chip) + early, CHUNK), late)], rq_r.at[c], weight_peer)


def write_rows(blocks, oq, okv, q, k, v, sems):
    copies = []
    for i, (start, size) in enumerate(blocks):
        at = pl.ds(start, size)
        for a, (src, dst) in enumerate(((oq, q), (okv.at[0], k), (okv.at[1], v))):
            copies.append(pltpu.make_async_copy(src.at[at], dst.at[at], sems.at[i, a]))
    for copy in copies:
        copy.start()
    for copy in copies:
        copy.wait()


def first_write(chips, rows, oq, okv, q, k, v, written, sems):
    me = Place(chips, rows)
    written[...] = jnp.zeros_like(written)
    blocks = [(me.block(0, me.chip), 2 * rows), (me.block(0, me.weight_chip), 2 * rows)]
    blocks += [(me.block(c, me.token_chip), EARLY * CHUNK) for c in range(2)]
    write_rows(blocks, oq, okv, q, k, v, sems)


def last_write(chips, rows, oq, okv, q_in, k_in, v_in, q, k, v, sems):
    me = Place(chips, rows)
    early = EARLY * CHUNK
    blocks = [(me.block(0, me.far_chip), 2 * rows)]
    blocks += [(pl.multiple_of(me.block(c, me.token_chip) + early, CHUNK), rows - early) for c in range(2)]
    write_rows(blocks, oq, okv, q, k, v, sems)


def solution(mesh):
    group_size = mesh.shape["tp"]
    chips = group_size // 2

    def local_step(x_rows, norm_gain, w_q, w_k, w_v):
        rows, depth = x_rows.shape
        head = w_q.shape[2]
        tokens = rows * group_size
        dtype = x_rows.dtype
        any_space = pl.BlockSpec(memory_space=pl.ANY)
        vmem = pl.BlockSpec(memory_space=pltpu.VMEM)
        dma = pltpu.SemaphoreType.DMA
        chunks = rows // CHUNK
        early = EARLY * CHUNK
        oq_type, okv_type = pltpu.VMEM((tokens, head), dtype), pltpu.VMEM((2, tokens, head), dtype)
        n_type, srq_type = pltpu.VMEM((2, rows, depth), dtype), pltpu.VMEM((2, rows, head), dtype)

        def held(*arrays):
            return [pltpu.with_memory_space_constraint(a, pltpu.VMEM) for a in arrays]

        oq, okv, n, w, srq, srkv = pl.pallas_call(
            functools.partial(first_exchange, chips),
            out_shape=(oq_type, okv_type, n_type, pltpu.VMEM((2, 2, 2, depth, 2 * LANES), dtype), srq_type, pltpu.VMEM((2, early, head), dtype)),
            in_specs=[any_space] * 5,
            out_specs=(vmem,) * 6,
            scratch_shapes=[
                pltpu.VMEM((depth,), norm_gain.dtype),
                pltpu.VMEM((1, depth), norm_gain.dtype),
                pltpu.VMEM((rows + early, head), dtype),
                pltpu.VMEM((2, rows, head), dtype),
                pltpu.VMEM((2, rows, head), dtype),
                dma, dma((chunks,)),
                dma((W_BLOCKS,)), dma((3,)), dma, dma,
                dma, dma((2, W_BLOCKS)),
                dma, dma,
                dma((2,)), dma((2,)),
                dma, dma((chunks,)),
                dma, dma((2,)), dma, dma,
                dma((2,)), dma((2,)), dma((2,)), dma((2,)),
                dma, dma, dma, dma, dma, dma,
            ],
            compiler_params=pltpu.CompilerParams(collective_id=0, has_side_effects=True, vmem_limit_bytes=16 * 1024 * 1024),
        )(*[pltpu.with_memory_space_constraint(a, pltpu.HBM) for a in (x_rows, norm_gain, w_q.reshape(depth, head), w_k, w_v)])
        out = jax.ShapeDtypeStruct((tokens, head), dtype)
        q, k, v, written = pl.pallas_call(
            functools.partial(first_write, chips, rows),
            out_shape=(out, out, out, jax.ShapeDtypeStruct((8, LANES), jnp.float32)),
            in_specs=[vmem, vmem],
            out_specs=(any_space, any_space, any_space, vmem),
            scratch_shapes=[dma((4, 3))],
            compiler_params=pltpu.CompilerParams(vmem_limit_bytes=1024 * 1024),
        )(*held(oq, okv))
        oq, okv, _, _ = pl.pallas_call(
            functools.partial(second_exchange, chips),
            out_shape=(oq_type, okv_type, n_type, srq_type),
            in_specs=[vmem, vmem, any_space, vmem, vmem, vmem, vmem],
            out_specs=(vmem,) * 4,
            input_output_aliases={3: 0, 4: 1, 5: 2, 6: 3},
            scratch_shapes=[
                pltpu.VMEM((2, rows, head), dtype),
                pltpu.VMEM((rows - early, head), dtype),
                dma, dma((chunks,)),
                dma, dma, dma, dma, dma, dma,
                dma, dma((2,)), dma, dma((chunks - EARLY,)),
                dma, dma, dma, dma,
                dma, dma, dma, dma,
            ],
            compiler_params=pltpu.CompilerParams(collective_id=1, has_side_effects=True, vmem_limit_bytes=16 * 1024 * 1024),
        )(*held(w, srkv), written, *held(oq, okv, n, srq))
        q, k, v = pl.pallas_call(
            functools.partial(last_write, chips, rows),
            out_shape=(out, out, out),
            in_specs=[vmem, vmem, any_space, any_space, any_space],
            out_specs=(any_space, any_space, any_space),
            input_output_aliases={2: 0, 3: 1, 4: 2},
            scratch_shapes=[dma((3, 3))],
            compiler_params=pltpu.CompilerParams(vmem_limit_bytes=1024 * 1024),
        )(*held(oq, okv), q, k, v)
        return q[:, None, :], k[:, None, :], v[:, None, :]

    return jax.shard_map(local_step, mesh=mesh, in_specs=(P(("dp", "tp"), None), P(None), P(None, "tp", None), P(None, "tp"), P(None, "tp")), out_specs=(P("dp", "tp", None), P("dp", "tp", None), P("dp", "tp", None)), check_vma=False)
```

```python
import functools

import jax
import jax.numpy as jnp
from jax import lax
from jax.experimental import pallas as pl
from jax.experimental.pallas import tpu as pltpu
from jax.sharding import PartitionSpec as P

EPSILON = 1e-6
LANES = 128
NORM_ROWS = 32
CHUNK = 128
EARLY = 5
SEND_ROWS = 64
EARLY_SENDS = 10
MORE_SENDS = 5
OWN_ROWS = 256
W_BLOCKS = 2
W_FIRST = 256
MESH = pl.DeviceIdType.MESH


class Place:
    def __init__(self, chips, rows):
        self.rows = rows
        group = lax.axis_index("dp")
        device = lax.axis_index("tp")
        self.half = lax.rem(group, 2)
        self.core = lax.rem(device, 2)
        self.chip = lax.div(device, 2)
        self.token_chip = chips - 1 - self.chip
        self.weight_chip = self.chip + 1 - 2 * lax.rem(self.chip, 2)
        self.far_chip = chips - 1 - self.weight_chip
        self.other_core = 1 - self.core
        self.partner = {"tp": 2 * self.chip + self.other_core}
        self.token_peer = {"tp": 2 * self.token_chip + self.core}
        self.weight_peer = self.weight_core(self.core)
        self.group_peer = {"dp": group + 1 - 2 * self.half}
        self.follows = lax.div(2 * self.chip, chips) + self.half
        self.sends = EARLY_SENDS + MORE_SENDS * self.core

    def weight_core(self, c):
        return {"tp": 2 * self.weight_chip + c}

    def block(self, c, on_chip):
        return pl.multiple_of((2 * on_chip + c) * self.rows, self.rows)


def remote(src, dst, send, recv, to):
    return pltpu.make_async_remote_copy(src_ref=src, dst_ref=dst, send_sem=send, recv_sem=recv, device_id=to, device_id_type=MESH)


def arrive(ref, sem, frm):
    remote(ref, ref, sem, sem, frm).wait_recv()


def sent(ref, sem, to):
    remote(ref, ref, sem, sem, to).wait_send()


def lanes(i):
    return pl.ds(pl.multiple_of(i * LANES, LANES), LANES)


def chunk_of(j):
    return pl.ds(pl.multiple_of(j * CHUNK, CHUNK), CHUNK)


def sends_of(j):
    return [j * (CHUNK // SEND_ROWS) + i for i in range(CHUNK // SEND_ROWS)]


def send_of(u):
    return pl.ds(pl.multiple_of(u * SEND_ROWS, SEND_ROWS), SEND_ROWS)


def greet(barrier, peers):
    for peer in peers:
        pl.semaphore_signal(barrier, inc=1, device_id=peer, device_id_type=MESH)


def product(n, w, blk, at, side, h, c):
    return jnp.dot(n[blk, at, :], w[side, h, c], preferred_element_type=jnp.float32).astype(jnp.bfloat16)


def local_products(me, n, w, oq, okv, slq, blk, base, start, size, stage, q_sems, kv_sems):
    at = pl.ds(start, size)
    out = pl.ds(pl.multiple_of(base + start, size), size)

    @pl.loop(0, 2)
    def _(h):
        for b in range(2):
            c = lax.rem(me.core + b, 2)
            both = product(n, w, blk, at, 0, h, c)
            if b == 0:
                oq[out, lanes(h)] = both[:, :LANES]
            else:
                slq[stage, lanes(h)] = both[:, :LANES]
            okv[h, out, lanes(c)] = both[:, LANES:]
    remote(slq.at[stage], oq.at[out], *q_sems, me.partner).start()
    remote(okv.at[:, out], okv.at[:, out], *kv_sems, me.partner).start()


def remote_products(n, w, at, srq, srkv, stage):
    @pl.loop(0, 2)
    def _(h):
        for c in range(2):
            both = product(n, w, 1, at, 1, h, c)
            srq[c, at, lanes(h)] = both[:, :LANES]
            srkv[h, stage, lanes(c)] = both[:, LANES:]


def send_early(me, at, oq, okv, srq, srkv, ek_s, ek_r, eq_s, eq_r):
    out = pl.ds(pl.multiple_of(me.block(me.core, me.token_chip) + at.start, CHUNK), at.size)
    remote(srkv.at[:, at], okv.at[:, out], ek_s, ek_r, me.weight_peer).start()
    remote(srq.at[me.core, at], oq.at[out], eq_s, eq_r, me.weight_peer).start()


def finish_early(me, oq, okv, srq, srkv, ek_s, ek_r, eq_s, eq_r):
    at = pl.ds(0, EARLY * CHUNK)
    out = pl.ds(me.block(me.core, me.far_chip), EARLY * CHUNK)
    sent(srkv.at[:, at], ek_s, me.weight_peer)
    sent(srq.at[me.core, at], eq_s, me.weight_peer)
    arrive(okv.at[:, out], ek_r, me.weight_peer)
    arrive(oq.at[out], eq_r, me.weight_peer)


def first_exchange(chips, x, gain, wq, wk, wv, oq, okv, n, w, srq, srkv, gain_copy, gain_row, slq, srq0, srkv0, g_sem, x_sem, w0_sem, wl_sem, wl_s, wl_r,
                   wx_s, wx_r, wg_s, wg_r, wd_s, wd_r, n_s, n_r, oq_s, oq_r, okv_s, okv_r, lq_s, lq_r, lkv_s, lkv_r, fk_s, fk_r, ek_s, ek_r, eq_s, eq_r):
    rows, depth = x.shape
    chunks = rows // CHUNK
    me = Place(chips, rows)
    half, core, other_core = me.half, me.core, me.other_core
    partner, token_peer, weight_peer, group_peer = me.partner, me.token_peer, me.weight_peer, me.group_peer
    weight_core, follows, sends = me.weight_core, me.follows, me.sends

    def load_x(j):
        return pltpu.make_async_copy(x.at[chunk_of(j)], n.at[0, chunk_of(j)], x_sem.at[j])

    q_half = [wq.at[:, pl.ds(h * LANES, LANES)] for h in range(2)]
    kv = [wk, wv]

    def own_w_part(h, part):
        return w.at[0, h, core, :, pl.ds(part * LANES, LANES)]

    cuts = ((0, W_FIRST, depth), (0, depth // 2, depth))

    def at_rows(ref, part, r):
        return ref.at[pl.ds(cuts[part][r], cuts[part][r + 1] - cuts[part][r])]

    barrier = pltpu.get_barrier_semaphore()

    first = own_w_part(half, 0)
    first_src = wq.at[:, pl.ds(pl.multiple_of(half * LANES, LANES), LANES)]
    for r in range(W_BLOCKS):
        pltpu.make_async_copy(at_rows(first_src, 0, r), at_rows(first, 0, r), w0_sem.at[r]).start()
    greet(barrier, (partner, weight_peer, weight_core(other_core)))
    second = own_w_part(1 - half, 0)
    pltpu.make_async_copy(wq.at[:, pl.ds(pl.multiple_of((1 - half) * LANES, LANES), LANES)], second, wl_sem.at[0]).start()
    for h in range(2):
        pltpu.make_async_copy(kv[h], own_w_part(h, 1), wl_sem.at[1 + h]).start()
    gain_load = pltpu.make_async_copy(gain, gain_copy, g_sem)
    gain_load.start()
    for j in range(chunks):
        load_x(j).start()
    pl.semaphore_wait(barrier, 3 + follows)
    greet(barrier, (token_peer, group_peer))

    w_parts = [w.at[1, half, core, :, pl.ds(part * LANES, LANES)] for part in range(2)]
    for r in range(W_BLOCKS):
        pltpu.make_async_copy(at_rows(first, 0, r), at_rows(first, 0, r), w0_sem.at[r]).wait()
        remote(at_rows(first, 0, r), at_rows(w_parts[0], 0, r), wx_s, wx_r.at[0, r], weight_peer).start()
    for h in range(2):
        @pl.when(half == h)
        def _():
            for r in range(W_BLOCKS):
                remote(at_rows(kv[h], 1, r), at_rows(w_parts[1], 1, r), wx_s, wx_r.at[1, r], weight_peer).start()
    for h in range(2):
        for part, src in enumerate((q_half[h], kv[h])):
            remote(src, own_w_part(h, part), wl_s, wl_r, partner).start()
    gain_load.wait()
    gain_row[...] = gain_copy[...].reshape(1, depth)

    def send_n(u):
        return remote(n.at[0, send_of(u)], n.at[1, send_of(u)], n_s, n_r.at[u], token_peer)

    @pl.loop(0, chunks)
    def _(j):
        load_x(j).wait()

        @pl.loop(0, CHUNK // NORM_ROWS)
        def _(i):
            at = pl.ds(pl.multiple_of(j * CHUNK + i * NORM_ROWS, NORM_ROWS), NORM_ROWS)
            wide = n[0, at, :].astype(jnp.float32)
            mean_sq = jnp.mean(wide * wide, axis=-1, keepdims=True)
            n[0, at, :] = (wide * lax.rsqrt(mean_sq + EPSILON) * gain_row[...]).astype(jnp.bfloat16)

        @pl.when(jnp.logical_and(j == 0, follows < 2))
        def _():
            pl.semaphore_wait(barrier, 2 - follows)

        for u in sends_of(j):
            @pl.when(u < sends)
            def _():
                send_n(u).start()

    own = me.block(core, me.chip)
    near = me.block(core, me.token_chip)

    def own_rows(start, size, stage):
        local_products(me, n, w, oq, okv, slq, 0, own, start, size, stage, (lq_s.at[0], lq_r.at[0]), (lkv_s.at[0], lkv_r.at[0]))

    own_w = w.at[0, :, core]
    pltpu.make_async_copy(second, second, wl_sem.at[0]).wait()
    for h in range(2):
        pltpu.make_async_copy(kv[h], own_w_part(h, 1), wl_sem.at[1 + h]).wait()
    other_w = w.at[0, :, other_core]
    remote(other_w, other_w, wl_s, wl_r, partner).wait_recv()

    def own_part(h, c, part):
        @pl.loop(0, rows // OWN_ROWS)
        def _(i):
            at = pl.ds(pl.multiple_of(i * OWN_ROWS, OWN_ROWS), OWN_ROWS)
            piece = w[1, h, c, :, part * LANES:(part + 1) * LANES]
            value = jnp.dot(n[0, at, :], piece, preferred_element_type=jnp.float32).astype(jnp.bfloat16)
            if part == 0:
                srq0[c, at, lanes(h)] = value
            else:
                srkv0[h, at, lanes(c)] = value

    def send_own(h, c, part):
        out = pl.ds(own, rows)
        if part == 0:
            remote(srq0.at[c, :, lanes(h)], oq.at[out, lanes(h)], oq_s, oq_r.at[core], weight_core(c)).start()
        else:
            remote(srkv0.at[h, :, lanes(c)], okv.at[h, out, lanes(c)], okv_s, okv_r, weight_peer).start()

    local_chunks = rows // OWN_ROWS
    steps = 2 * W_BLOCKS
    for step in range(steps):
        part, r = divmod(step, W_BLOCKS)
        piece = at_rows(w_parts[part], part, r)
        remote(piece, piece, wx_s, wx_r.at[part, r], weight_peer).wait_recv()
        remote(piece, piece, wg_s, wg_r, group_peer).start()
        remote(piece, piece, wd_s.at[0], wd_r.at[0], partner).start()
        if r == W_BLOCKS - 1:
            own_part(half, core, part)
            send_own(half, core, part)
        for i in range(step * local_chunks // steps, (step + 1) * local_chunks // steps):
            own_rows(i * OWN_ROWS, OWN_ROWS, pl.ds(i * OWN_ROWS, OWN_ROWS))

    def own_products(h, c):
        @pl.loop(0, rows // OWN_ROWS)
        def _(i):
            at = pl.ds(pl.multiple_of(i * OWN_ROWS, OWN_ROWS), OWN_ROWS)
            both = product(n, w, 0, at, 1, h, c)
            srq0[c, at, lanes(h)] = both[:, :LANES]
            srkv0[h, at, lanes(c)] = both[:, LANES:]
        for part in range(2):
            send_own(h, c, part)

    other_half = 1 - half
    from_partner = w.at[1, half, other_core]
    remote(from_partner, from_partner, wd_s.at[0], wd_r.at[0], partner).wait_recv()
    own_products(half, other_core)
    from_group = w.at[1, other_half, core]
    remote(from_group, from_group, wg_s, wg_r, group_peer).wait_recv()
    remote(from_group, from_group, wd_s.at[1], wd_r.at[1], partner).start()
    own_products(other_half, core)
    from_both = w.at[1, other_half, other_core]
    remote(from_both, from_both, wd_s.at[1], wd_r.at[1], partner).wait_recv()
    own_products(other_half, other_core)

    @pl.loop(0, EARLY)
    def _(j):
        for u in sends_of(j):
            send_n(u).wait_recv()
        start = pl.multiple_of(j * CHUNK, CHUNK)
        stage = pl.ds(pl.multiple_of(rows + start, CHUNK), CHUNK)
        at = chunk_of(j)
        remote_products(n, w, at, srq, srkv, at)

        @pl.when(core == 1)
        def _():
            send_early(me, at, oq, okv, srq, srkv, ek_s, ek_r, eq_s, eq_r)

        local_products(me, n, w, oq, okv, slq, 1, near, start, CHUNK, stage, (lq_s.at[1], lq_r.at[1]), (lkv_s.at[1], lkv_r.at[1]))

    for c in range(2):
        arrive(oq.at[pl.ds(me.block(c, me.weight_chip), rows)], oq_r.at[c], weight_peer)
    beside = okv.at[:, pl.ds(me.block(core, me.weight_chip), rows)]
    arrive(beside, okv_r, weight_peer)
    remote(beside, beside, fk_s, fk_r, partner).start()
    for i, (on_chip, size) in enumerate(((me.chip, rows), (me.token_chip, EARLY * CHUNK))):
        theirs = pl.ds(me.block(other_core, on_chip), size)
        mine = pl.ds(0, size)
        arrive(oq.at[theirs], lq_r.at[i], partner)
        arrive(okv.at[:, theirs], lkv_r.at[i], partner)
        sent(slq.at[mine], lq_s.at[i], partner)
        sent(okv.at[:, mine], lkv_s.at[i], partner)
    @pl.loop(EARLY_SENDS, sends)
    def _(u):
        send_n(u).wait_recv()

    for i in range(2):
        @pl.when(core == i)
        def _():
            sent(n.at[0, pl.ds(0, (EARLY_SENDS + MORE_SENDS * i) * SEND_ROWS)], n_s, token_peer)
    sent(own_w, wl_s, partner)
    sent(w.at[1, 0, 0], wx_s, weight_peer)
    sent(w.at[1, 0, 0], wg_s, group_peer)
    for i in range(2):
        sent(w.at[1, 0, 0], wd_s.at[i], partner)
    sent(srq0, oq_s, weight_peer)
    sent(srkv0, okv_s, weight_peer)

    @pl.when(core == 1)
    def _():
        finish_early(me, oq, okv, srq, srkv, ek_s, ek_r, eq_s, eq_r)

    sent(beside, fk_s, partner)
    arrive(okv.at[:, pl.ds(me.block(other_core, me.weight_chip), rows)], fk_r, partner)


def second_exchange(chips, w, srkv_early, written, oq_in, okv_in, n_in, srq_in, oq, okv, n, srq, srkv, slq, n_s, n_r, ek_s, ek_r, eq_s, eq_r, xb_s, xb_r, rq_s, rq_r, rkv_s, rkv_r,
                    lq_s, lq_r, lkv_s, lkv_r, fe_s, fe_r, fk_s, fk_r):
    rows = n.shape[1]
    chunks = rows // CHUNK
    early = EARLY * CHUNK
    late = rows - early
    me = Place(chips, rows)
    core, other_core, partner, weight_peer = me.core, me.other_core, me.partner, me.weight_peer
    near = me.block(core, me.token_chip)
    far = me.block(core, me.far_chip)

    barrier = pltpu.get_barrier_semaphore()
    greet(barrier, (weight_peer, me.token_peer))
    pl.semaphore_wait(barrier, 2 + 2 * core)
    greet(barrier, (partner, me.weight_core(other_core)))

    def send_n(u):
        return remote(n.at[0, send_of(u)], n.at[1, send_of(u)], n_s, n_r.at[u], me.token_peer)

    @pl.loop(me.sends, rows // SEND_ROWS)
    def _(u):
        send_n(u).start()

    @pl.when(core == 0)
    def _():
        send_early(me, pl.ds(0, early), oq, okv, srq, srkv_early, ek_s, ek_r, eq_s, eq_r)
        pl.semaphore_wait(barrier, 2)

    remote(srq.at[other_core, pl.ds(0, early)], oq.at[pl.ds(near, early)], xb_s, xb_r, me.weight_core(other_core)).start()

    @pl.loop(EARLY, chunks)
    def _(j):
        for u in sends_of(j):
            @pl.when(u >= me.sends)
            def _():
                send_n(u).wait_recv()

        start = pl.multiple_of(j * CHUNK, CHUNK)
        at = pl.ds(start, CHUNK)
        out = pl.ds(pl.multiple_of(near + start, CHUNK), CHUNK)
        remote_products(n, w, at, srq, srkv, at)
        remote(srkv.at[:, at], okv.at[:, out], rkv_s, rkv_r.at[j - EARLY], weight_peer).start()
        for c in (1, 0):
            remote(srq.at[c, at], oq.at[out], rq_s, rq_r.at[core], me.weight_core(c)).start()
        stage = pl.ds(pl.multiple_of(start - early, CHUNK), CHUNK)
        local_products(me, n, w, oq, okv, slq, 1, near, start, CHUNK, stage, (lq_s, lq_r), (lkv_s, lkv_r))

    @pl.when(core == 0)
    def _():
        finish_early(me, oq, okv, srq, srkv_early, ek_s, ek_r, eq_s, eq_r)

    far_early = okv.at[:, pl.ds(far, early)]
    remote(far_early, far_early, fe_s, fe_r, partner).start()
    theirs = pl.ds(pl.multiple_of(me.block(other_core, me.token_chip) + early, CHUNK), late)
    arrive(oq.at[theirs], lq_r, partner)
    arrive(okv.at[:, theirs], lkv_r, partner)
    sent(slq, lq_s, partner)
    sent(okv.at[:, theirs], lkv_s, partner)
    arrive(oq.at[pl.ds(me.block(other_core, me.far_chip), early)], xb_r, weight_peer)
    sent(srq.at[other_core, pl.ds(0, early)], xb_s, weight_peer)
    for i in range(2):
        @pl.when(core == i)
        def _():
            gone = (EARLY_SENDS + MORE_SENDS * i) * SEND_ROWS
            sent(n.at[0, pl.ds(gone, rows - gone)], n_s, me.token_peer)

    @pl.loop(EARLY, chunks)
    def _(j):
        piece = okv.at[:, pl.ds(pl.multiple_of(far + j * CHUNK, CHUNK), CHUNK)]
        remote(piece, piece, rkv_s, rkv_r.at[j - EARLY], weight_peer).wait_recv()
        remote(piece, piece, fk_s, fk_r, partner).start()

    tail = pl.ds(early, late)
    sent(srkv.at[:, tail], rkv_s, weight_peer)
    sent(far_early, fe_s, partner)
    sent(srkv.at[:, tail], fk_s, partner)
    arrive(okv.at[:, pl.ds(me.block(other_core, me.far_chip), early)], fe_r, partner)
    arrive(okv.at[:, pl.ds(pl.multiple_of(me.block(other_core, me.far_chip) + early, CHUNK), late)], fk_r, partner)
    sent(srq.at[:, tail], rq_s, weight_peer)
    for c in range(2):
        arrive(oq.at[pl.ds(pl.multiple_of(me.block(c, me.far_chip) + early, CHUNK), late)], rq_r.at[c], weight_peer)


def write_rows(blocks, oq, okv, q, k, v, sems):
    copies = []
    for i, (start, size) in enumerate(blocks):
        at = pl.ds(start, size)
        for a, (src, dst) in enumerate(((oq, q), (okv.at[0], k), (okv.at[1], v))):
            copies.append(pltpu.make_async_copy(src.at[at], dst.at[at], sems.at[i, a]))
    for copy in copies:
        copy.start()
    for copy in copies:
        copy.wait()


def first_write(chips, rows, oq, okv, q, k, v, written, sems):
    me = Place(chips, rows)
    written[...] = jnp.zeros_like(written)
    blocks = [(me.block(0, me.chip), 2 * rows), (me.block(0, me.weight_chip), 2 * rows)]
    blocks += [(me.block(c, me.token_chip), EARLY * CHUNK) for c in range(2)]
    write_rows(blocks, oq, okv, q, k, v, sems)


def last_write(chips, rows, oq, okv, q_in, k_in, v_in, q, k, v, sems):
    me = Place(chips, rows)
    early = EARLY * CHUNK
    blocks = [(me.block(0, me.far_chip), 2 * rows)]
    blocks += [(pl.multiple_of(me.block(c, me.token_chip) + early, CHUNK), rows - early) for c in range(2)]
    write_rows(blocks, oq, okv, q, k, v, sems)


def solution(mesh):
    group_size = mesh.shape["tp"]
    chips = group_size // 2

    def local_step(x_rows, norm_gain, w_q, w_k, w_v):
        rows, depth = x_rows.shape
        head = w_q.shape[2]
        tokens = rows * group_size
        dtype = x_rows.dtype
        any_space = pl.BlockSpec(memory_space=pl.ANY)
        vmem = pl.BlockSpec(memory_space=pltpu.VMEM)
        dma = pltpu.SemaphoreType.DMA
        chunks = rows // CHUNK
        early = EARLY * CHUNK
        oq_type, okv_type = pltpu.VMEM((tokens, head), dtype), pltpu.VMEM((2, tokens, head), dtype)
        n_type, srq_type = pltpu.VMEM((2, rows, depth), dtype), pltpu.VMEM((2, rows, head), dtype)

        def held(*arrays):
            return [pltpu.with_memory_space_constraint(a, pltpu.VMEM) for a in arrays]

        oq, okv, n, w, srq, srkv = pl.pallas_call(
            functools.partial(first_exchange, chips),
            out_shape=(oq_type, okv_type, n_type, pltpu.VMEM((2, 2, 2, depth, 2 * LANES), dtype), srq_type, pltpu.VMEM((2, early, head), dtype)),
            in_specs=[any_space] * 5,
            out_specs=(vmem,) * 6,
            scratch_shapes=[
                pltpu.VMEM((depth,), norm_gain.dtype),
                pltpu.VMEM((1, depth), norm_gain.dtype),
                pltpu.VMEM((rows + early, head), dtype),
                pltpu.VMEM((2, rows, head), dtype),
                pltpu.VMEM((2, rows, head), dtype),
                dma, dma((chunks,)),
                dma((W_BLOCKS,)), dma((3,)), dma, dma,
                dma, dma((2, W_BLOCKS)),
                dma, dma,
                dma((2,)), dma((2,)),
                dma, dma((rows // SEND_ROWS,)),
                dma, dma((2,)), dma, dma,
                dma((2,)), dma((2,)), dma((2,)), dma((2,)),
                dma, dma, dma, dma, dma, dma,
            ],
            compiler_params=pltpu.CompilerParams(collective_id=0, has_side_effects=True, vmem_limit_bytes=16 * 1024 * 1024),
        )(*[pltpu.with_memory_space_constraint(a, pltpu.HBM) for a in (x_rows, norm_gain, w_q.reshape(depth, head), w_k, w_v)])
        out = jax.ShapeDtypeStruct((tokens, head), dtype)
        q, k, v, written = pl.pallas_call(
            functools.partial(first_write, chips, rows),
            out_shape=(out, out, out, jax.ShapeDtypeStruct((8, LANES), jnp.float32)),
            in_specs=[vmem, vmem],
            out_specs=(any_space, any_space, any_space, vmem),
            scratch_shapes=[dma((4, 3))],
            compiler_params=pltpu.CompilerParams(vmem_limit_bytes=1024 * 1024),
        )(*held(oq, okv))
        oq, okv, _, _ = pl.pallas_call(
            functools.partial(second_exchange, chips),
            out_shape=(oq_type, okv_type, n_type, srq_type),
            in_specs=[vmem, vmem, any_space, vmem, vmem, vmem, vmem],
            out_specs=(vmem,) * 4,
            input_output_aliases={3: 0, 4: 1, 5: 2, 6: 3},
            scratch_shapes=[
                pltpu.VMEM((2, rows, head), dtype),
                pltpu.VMEM((rows - early, head), dtype),
                dma, dma((rows // SEND_ROWS,)),
                dma, dma, dma, dma, dma, dma,
                dma, dma((2,)), dma, dma((chunks - EARLY,)),
                dma, dma, dma, dma,
                dma, dma, dma, dma,
            ],
            compiler_params=pltpu.CompilerParams(collective_id=1, has_side_effects=True, vmem_limit_bytes=16 * 1024 * 1024),
        )(*held(w, srkv), written, *held(oq, okv, n, srq))
        q, k, v = pl.pallas_call(
            functools.partial(last_write, chips, rows),
            out_shape=(out, out, out),
            in_specs=[vmem, vmem, any_space, any_space, any_space],
            out_specs=(any_space, any_space, any_space),
            input_output_aliases={2: 0, 3: 1, 4: 2},
            scratch_shapes=[dma((3, 3))],
            compiler_params=pltpu.CompilerParams(vmem_limit_bytes=1024 * 1024),
        )(*held(oq, okv), q, k, v)
        return q[:, None, :], k[:, None, :], v[:, None, :]

    return jax.shard_map(local_step, mesh=mesh, in_specs=(P(("dp", "tp"), None), P(None), P(None, "tp", None), P(None, "tp"), P(None, "tp")), out_specs=(P("dp", "tp", None), P("dp", "tp", None), P("dp", "tp", None)), check_vma=False)
```
